32 devices in a mesh: train: 4 (over z), serve: 8 (over y, x, core).
Axes of the slice: x: 2, y: 2, z: 4, core: 2. Of those that a mesh axis runs over, the one named last changes fastest.
Arguments:
- train_weights: bfloat16 [16, 7424, 2112], P(None, 'train', 'serve'), may hold values from -6 to 6
- row_offset: int32 [16, 5], replicated, may hold values from 0 to 7168, as said below
- block_group: int32 [16, 224, 1], P(None, 'train'), may hold values from 0 to 7; in each aligned block of 56 rows (0 to 55, 56 to 111, ..., all dimensions but the last counted through in order) at most 8 rows name the same one
Outputs:
- quant_codes: bfloat16 [16, 8, 4, 8, 32, 2112], P(None, 'serve', 'train')
- block_scales: float32 [16, 8, 4, 8, 2112], P(None, 'serve', 'train')
The draws below stay inside these ranges and needn't reach their ends.
Inputs may be any that keep to these rules, and one draw needn't show every extreme that they name: For every layer l: row_offset[l, 0] = 0 and row_offset[l, 4] = 7168; every other row_offset[l, t] lies 1 to 32 rows above or below t * 1792, never on it; in every layer one entry lies exactly 32 rows above and another exactly 32 rows below; layer 1 has the opposite sign of layer 0 at every such entry. `block_group`: within each aligned block of 56 entries (one training device's blocks of one layer), no group is named more than 8 times; some group reaches 8 in some of them.
All inputs are finite; a program needn't handle non-finite values.
Results may differ from the reference program's by a relative error of at most 0.001.
Values may be sent and summed in bfloat16 or wider, within the bound.
A program may use at most 128 MiB of HBM per device.

```python
import math
import jax
import jax.numpy as jnp
import numpy as np
from jax import lax

MODEL_DIM = 7168
LAYERS = 16
BLOCK = 32
SHIFT = 32
FEAT = 2112
ROWS_DEV = 1792
SLOT = 1856
BLOCKS = 224
BLOCKS_DEV = 56
SLOTS = 8
N_TRAIN = 4
N_SERVE = 8


def draw_train_weights(key, part):
    base_key = jax.random.fold_in(key, 23)
    value_key, quiet_key, scale_key = jax.random.split(base_key, 3)
    full_shape = (LAYERS, N_TRAIN * SLOT, FEAT)
    values = jnp.clip(jax.random.normal(value_key, full_shape, jnp.float32), -6.0, 6.0)
    quiet_mask = jax.random.randint(quiet_key, (LAYERS, MODEL_DIM // BLOCK, FEAT), 0, 8, dtype=jnp.int32) == 0
    buffer_row = jnp.arange(N_TRAIN * SLOT, dtype=jnp.int32)
    owner_dev = buffer_row // SLOT
    global_row = jnp.clip(owner_dev * ROWS_DEV + buffer_row % SLOT - SHIFT, 0, MODEL_DIM - 1).astype(jnp.int32)
    block_of_row = (global_row // BLOCK).astype(jnp.int32)
    quiet_rows = jnp.take(quiet_mask, block_of_row, axis=1)
    damping = jnp.where(quiet_rows, 0.02, 1.0).astype(jnp.float32)
    return (values * damping).astype(jnp.bfloat16)


def draw_row_offset(key, part):
    base_key = jax.random.fold_in(key, 11)
    size_key, sign_key, pick_key = jax.random.split(base_key, 3)
    magnitude = jax.random.randint(size_key, (LAYERS, N_TRAIN - 1), 1, SHIFT + 1, dtype=jnp.int32)
    signs = jax.random.randint(sign_key, (LAYERS, N_TRAIN - 1), 0, 2, dtype=jnp.int32) * 2 - 1
    inner = (magnitude * signs).astype(jnp.int32)
    pick_keys = jax.random.split(pick_key, LAYERS)
    picked = jax.vmap(lambda one_key: jax.random.permutation(one_key, N_TRAIN - 1))(pick_keys)
    column_ids = jnp.arange(N_TRAIN - 1, dtype=jnp.int32)[None, :]
    inner = jnp.where(column_ids == picked[:, 0:1], SHIFT, inner)
    inner = jnp.where(column_ids == picked[:, 1:2], -SHIFT, inner)
    layer_ids = jnp.arange(LAYERS, dtype=jnp.int32)[:, None]
    inner = jnp.where(layer_ids == 1, -inner[0:1], inner).astype(jnp.int32)
    middle = jnp.arange(1, N_TRAIN, dtype=jnp.int32)[None, :] * ROWS_DEV + inner
    start = jnp.zeros((LAYERS, 1), jnp.int32)
    finish = jnp.full((LAYERS, 1), N_TRAIN * ROWS_DEV, jnp.int32)
    return jnp.concatenate([start, middle, finish], axis=1).astype(jnp.int32)


def routed_block(key, own, number, rows, number_of, top, most, slope):
    order = jax.random.permutation(key, number_of)
    crowded, ordinary = shares(number_of, rows * top, most, slope, True), shares(number_of, rows * top, most, slope, False)
    places = jnp.arange(number_of)

    def named(lengths, rotation):
        used = int((lengths > 0).sum())
        fixed = max(1, used // 4)
        moved = fixed + (places - fixed + rotation * (used - fixed)) % max(1, number_of - fixed)
        return jnp.zeros((number_of,), jnp.int32).at[order[jnp.where(places < fixed, places, moved)]].set(jnp.asarray(lengths, jnp.int32))

    lengths = jnp.where(number % 4 == 0, named(crowded, number // 4), named(ordinary, number - number // 4 - 1))
    mixed = jax.random.permutation(jax.random.fold_in(own, 3), number_of)
    donor, sink = mixed[0:number_of // 2 * 2:2], mixed[1:number_of // 2 * 2:2]
    slack = jnp.minimum(lengths[donor] - 1, most - lengths[sink]) // 2
    slack = jnp.where((donor == order[0]) | (sink == order[0]) | (lengths[sink] == 0), 0, jnp.maximum(slack, 0))
    moved = jax.random.randint(jax.random.fold_in(own, 4), (number_of // 2,), 0, 1 << 20) % (slack + 1)
    lengths = lengths.at[donor].add(-moved).at[sink].add(moved)
    labels = jnp.searchsorted(jnp.cumsum(lengths), jnp.arange(rows * top), side="right").astype(jnp.int32)
    listing = labels.reshape(top, rows).T
    listing = listing[jax.random.permutation(jax.random.fold_in(own, 1), rows)]
    rotation = jax.random.randint(jax.random.fold_in(own, 2), (rows, 1), 0, top)
    return jnp.take_along_axis(listing, (jnp.arange(top)[None, :] + rotation) % top, axis=1)


def shares(number_of, total, bound, skew, full):
    portions = [(1 << 20) // math.isqrt(grade ** skew) + 1 for grade in range(1, number_of + 1)]
    largest = bound if full else min(bound, max(-(-total // number_of), total * portions[0] // sum(portions)))
    least = 1 if total - largest >= number_of - 1 else 0
    given, rest = [largest] + [least] * (number_of - 1), total - largest - least * (number_of - 1)
    while rest > 0:
        movable = [i for i in range(1, number_of) if given[i] < largest] or [i for i in range(1, number_of) if given[i] < bound]
        pool, budget = sum([portions[i] for i in movable]), rest
        for i in movable:
            extra = min(bound - given[i], max(1, budget * portions[i] // pool), rest)
            given[i] = given[i] + extra
            rest = rest - extra
    return np.array(given)


def setup_inputs(seed: int = 0) -> dict:
    splits = jax.random.split(jax.random.key(seed), 4)
    train_weights = draw_train_weights(jax.random.fold_in(splits[3], 71), 0)
    row_offset = draw_row_offset(jax.random.fold_in(splits[3], 71), 0)
    block_group_keys = jax.random.split(jax.random.fold_in(splits[2], 1), LAYERS * BLOCKS // BLOCKS_DEV)
    block_group_turns = jax.random.permutation(jax.random.fold_in(splits[2], 3), LAYERS * BLOCKS // BLOCKS_DEV)
    block_group = jax.vmap(lambda own, number: routed_block(jax.random.fold_in(splits[2], 2), own, number, BLOCKS_DEV, N_SERVE, 1, SLOTS, 0))(block_group_keys, block_group_turns).reshape((LAYERS, BLOCKS, 1))
    return {"train_weights": train_weights, "row_offset": row_offset, "block_group": block_group}


def reference(train_weights, row_offset, block_group):
    row_ids = jnp.arange(MODEL_DIM, dtype=jnp.int32)
    block_owner = (jnp.arange(BLOCKS, dtype=jnp.int32) // BLOCKS_DEV).astype(jnp.int32)
    position = jnp.arange(BLOCKS_DEV, dtype=jnp.int32)
    earlier = position[None, :] < position[:, None]

    def one_layer(inputs):
        weights, groups, offsets = inputs
        owner_dev = jnp.sum((row_ids[:, None] >= offsets[None, 1:N_TRAIN]).astype(jnp.int32), axis=1).astype(jnp.int32)
        source = (owner_dev * SLOT + row_ids - owner_dev * ROWS_DEV + SHIFT).astype(jnp.int32)
        gathered = jnp.take(weights, source, axis=0)
        blocks = gathered.reshape(BLOCKS, BLOCK, FEAT).astype(jnp.float32)
        absmax = jnp.max(jnp.abs(blocks), axis=1)
        divisor = jnp.maximum(absmax, 0.25)
        coded = (blocks / divisor[:, None, :]).astype(jnp.bfloat16)
        group_ids = groups[:, 0].astype(jnp.int32)
        per_dev = group_ids.reshape(N_TRAIN, BLOCKS_DEV)
        same_group = per_dev[:, :, None] == per_dev[:, None, :]
        order_in = jnp.sum((same_group & earlier[None]).astype(jnp.int32), axis=2).reshape(BLOCKS).astype(jnp.int32)
        flat_slot = ((group_ids * N_TRAIN + block_owner) * SLOTS + order_in).astype(jnp.int32)
        out_codes = jnp.zeros((N_SERVE * N_TRAIN * SLOTS, BLOCK, FEAT), jnp.bfloat16).at[flat_slot].set(coded)
        out_scales = jnp.zeros((N_SERVE * N_TRAIN * SLOTS, FEAT), jnp.float32).at[flat_slot].set(divisor)
        return (out_codes.reshape(N_SERVE, N_TRAIN, SLOTS, BLOCK, FEAT),
                out_scales.reshape(N_SERVE, N_TRAIN, SLOTS, FEAT))

    quant_codes, block_scales = lax.map(one_layer, (train_weights, block_group, row_offset))
    return quant_codes, block_scales
```

```python
import functools

import jax
import jax.numpy as jnp
from jax import lax
from jax.experimental import pallas as pl
from jax.experimental.pallas import tpu as pltpu
from jax.sharding import PartitionSpec as P

BLOCK = 32
SHIFT = 32
LANES = 128
PAIR = 2
MESH = pl.DeviceIdType.MESH
MIB = 1024 * 1024


def turned(values):
    return jnp.transpose(values.astype(jnp.float32))


def partner(me, mask, count):
    out, bit = 0, 1
    while bit < count:
        out = out + ((me // bit + mask // bit) % 2) * bit
        bit *= 2
    return out


def scaled(values):
    values = values.astype(jnp.float32)
    divisor = jnp.maximum(jnp.max(jnp.abs(values), axis=0, keepdims=True), 0.25)
    return values * (1.0 / divisor), divisor


def unpack_pair(dims, recv, rem_code, rem_scale, rows, put_code, put_scale):
    slots, full, rem, columns, sources = dims
    width = columns * sources
    tiles = -(-width // LANES)
    lane = lax.broadcasted_iota(jnp.int32, (BLOCK, LANES), 1)
    lane_row = lax.broadcasted_iota(jnp.int32, (1, LANES), 1)
    if rem:
        for s in range(sources):
            rem_code[s], rem_scale[s] = scaled(recv(s, PAIR * slots * full))

    def slot(i, carry):
        parts = [None] * tiles

        def put(tile, low, code, scale):
            if tile >= tiles:
                return
            if parts[tile] is None:
                parts[tile] = (code, scale)
            else:
                before = parts[tile]
                parts[tile] = (jnp.where(lane >= low, code, before[0]), jnp.where(lane_row >= low, scale, before[1]))

        def flush(below):
            for tile in range(below):
                if parts[tile] is not None:
                    code, scale = parts[tile]
                    end = min(width, (tile + 1) * LANES)
                    size = end - tile * LANES
                    put_code(i, tile * LANES, end, code[:, :size])
                    rows[i, :, tile * LANES : end] = scale[:, :size]
                    parts[tile] = None

        for s in range(sources):
            for t in range(full + (1 if rem else 0)):
                start = s * columns + t * LANES
                size = LANES if t < full else rem
                low = start % LANES
                if t < full:
                    code, scale = scaled(recv(s, i * full + t))
                    if low:
                        code, scale = pltpu.roll(code, low, 1), pltpu.roll(scale, low, 1)
                else:
                    turn = lax.rem(low + LANES - i * rem, LANES)
                    code, scale = pltpu.roll(rem_code[s], turn, 1), pltpu.roll(rem_scale[s], turn, 1)
                tile = start // LANES
                put(tile, low, code, scale)
                if low + size > LANES:
                    put(tile + 1, 0, code, scale)
                flush((start + size) // LANES)
        flush(tiles)
        return carry

    lax.fori_loop(0, PAIR * slots, slot, 0)
    for i in range(PAIR * slots):
        put_scale(i // slots, i % slots, rows[i])


def move_kernel(
    dims,
    table_ref,
    offset_ref,
    wt_ref,
    codes_ref,
    scale_ref,
    recv_ref,
    send_ref,
    in_ref,
    w_ref,
    rem_ref,
    edge_ref,
    halo_ref,
    rem_code,
    rem_scale,
    rows,
    in_sem,
    send_sem,
    recv_sem,
    halo_send,
    halo_recv,
):
    slots, full, rem, columns, groups = dims
    pairs = recv_ref.shape[1]
    layers = pairs * PAIR
    blocks = w_ref.shape[0]
    buffer_len = blocks * BLOCK
    rows_dev = buffer_len - 2 * SHIFT
    me = lax.axis_index("serve")
    part = lax.axis_index("train")
    parts_n = lax.axis_size("train")
    half = slots * full
    rest = half + (1 if rem else 0)

    def fetch(layer, sub):
        return pltpu.make_async_copy(wt_ref.at[layer], in_ref.at[sub], in_sem.at[sub])

    def message(mask, pair, sub):
        peer = partner(me, mask, groups)
        span = pl.ds(sub * half, rest if sub == PAIR - 1 else half)
        return pltpu.make_async_remote_copy(
            send_ref.at[peer, pair, span],
            recv_ref.at[me, pair, span],
            send_sem.at[mask, pair, sub],
            recv_sem.at[mask, pair, sub],
            device_id={"serve": peer},
            device_id_type=MESH,
        )

    def arrival(mask, pair, sub):
        peer = partner(me, mask, groups)
        span = pl.ds(sub * half, rest if sub == PAIR - 1 else half)
        return pltpu.make_async_remote_copy(
            recv_ref.at[peer, pair, span],
            recv_ref.at[peer, pair, span],
            send_sem.at[mask, pair, sub],
            recv_sem.at[mask, pair, sub],
            device_id={"serve": peer},
            device_id_type=MESH,
        )

    def edge(layer, side):
        to = part + 1 if side == 0 else part - 1
        return pltpu.make_async_remote_copy(
            edge_ref.at[layer, side],
            halo_ref.at[layer, side],
            halo_send.at[layer, side],
            halo_recv.at[layer, side],
            device_id={"train": to},
            device_id_type=MESH,
        )

    for sub in range(PAIR):
        fetch(sub, sub).start()

    barrier = pltpu.get_barrier_semaphore()

    def greet(mask, carry):
        pl.semaphore_signal(barrier, inc=1, device_id={"serve": partner(me, mask, groups)}, device_id_type=MESH)
        return carry

    lax.fori_loop(1, groups, greet, 0)

    @pl.when(part > 0)
    def _():
        pl.semaphore_signal(barrier, inc=1, device_id={"train": part - 1}, device_id_type=MESH)

    @pl.when(part < parts_n - 1)
    def _():
        pl.semaphore_signal(barrier, inc=1, device_id={"train": part + 1}, device_id_type=MESH)

    below = (part + parts_n - 1) // parts_n
    above = (2 * parts_n - 2 - part) // parts_n
    pl.semaphore_wait(barrier, groups - 1 + below + above)

    row = lax.broadcasted_iota(jnp.int32, (BLOCK, columns), 0)
    lane = lax.broadcasted_iota(jnp.int32, (BLOCK, LANES), 1)
    last = rows_dev - BLOCK

    def transpose_tile(sub, low):
        high = min(low + LANES, buffer_len)
        rows_of = turned(in_ref[sub, :, low:high]).astype(w_ref.dtype)
        w_ref[low // BLOCK : high // BLOCK] = rows_of.reshape((high - low) // BLOCK, BLOCK, columns)

    def pack_layer(pair, sub):
        layer = pair * PAIR + sub
        fetch(layer, sub).wait()
        lows = list(range(0, buffer_len, LANES))
        lows = [lows[0], lows[-1]] + lows[1:-1]
        for low in lows[:2]:
            transpose_tile(sub, low)
        edge_ref[layer, 0] = w_ref[blocks - 1]
        edge_ref[layer, 1] = w_ref[0]

        @pl.when(part < parts_n - 1)
        def _():
            edge(layer, 0).start()

        @pl.when(part > 0)
        def _():
            edge(layer, 1).start()

        for low in lows[2:]:
            transpose_tile(sub, low)

        @pl.when(layer + PAIR < layers)
        def _():
            fetch(layer + PAIR, sub).start()

        base = part * rows_dev

        @pl.when(part > 0)
        def _():
            edge(layer, 0).wait_recv()
            first = offset_ref[part, layer] - base
            head = jnp.where(row < first, halo_ref[layer, 0].astype(jnp.float32), w_ref[1].astype(jnp.float32))
            w_ref[1] = head.astype(w_ref.dtype)

        @pl.when(part < parts_n - 1)
        def _():
            edge(layer, 1).wait_recv()
            after = offset_ref[part + 1, layer] - base
            tail = w_ref[blocks - 2].astype(jnp.float32)
            tail = jnp.where(row + last >= after, halo_ref[layer, 1].astype(jnp.float32), tail)
            w_ref[blocks - 2] = tail.astype(w_ref.dtype)

        w_ref[0] = jnp.zeros((BLOCK, columns), w_ref.dtype)

        def gather(group, out):
            for k in range(slots):
                block = w_ref[table_ref[layer, group * slots + k]]
                for t in range(full):
                    out[pair, (sub * slots + k) * full + t] = block[:, t * LANES : (t + 1) * LANES]
                if rem:
                    rem_ref[group, sub * slots + k, :, 0:rem] = block[:, full * LANES :]
            if rem and sub == PAIR - 1:
                tile = rem_ref[group, 0].astype(jnp.float32)
                for i in range(1, PAIR * slots):
                    moved = pltpu.roll(rem_ref[group, i].astype(jnp.float32), i * rem, 1)
                    tile = jnp.where(lane >= i * rem, moved, tile)
                out[pair, PAIR * half] = tile.astype(out.dtype)

        def give(mask, carry):
            peer = partner(me, mask, groups)
            gather(peer, send_ref.at[peer])
            message(mask, pair, sub).start()
            return carry

        lax.fori_loop(2, groups, give, 0)
        give(1, 0)
        gather(me, recv_ref.at[me])

    def take(pair):
        for sub in range(PAIR):

            def arrive(mask, carry, sub=sub):
                arrival(mask, pair, sub).wait_recv()
                return carry

            lax.fori_loop(1, groups, arrive, 0)

    def unpack(pair):
        def put_code(i, low, high, code):
            codes_ref[pair * PAIR + i // slots, i % slots, :, low:high] = code.astype(codes_ref.dtype)

        def put_scale(sub, k, scale):
            scale_ref[pair * PAIR + sub, k : k + 1, :] = scale

        unpack_pair(dims, lambda s, n: recv_ref[s, pair, n], rem_code, rem_scale, rows, put_code, put_scale)

    def step(pair, carry):
        for sub in range(PAIR):
            pack_layer(pair, sub)

        @pl.when(pair > 0)
        def _():
            take(pair - 1)
            unpack(pair - 1)

        return carry

    lax.fori_loop(0, pairs, step, 0)
    take(pairs - 1)

    def drain(pair, carry):
        for sub in range(PAIR):

            def sent(mask, inner, sub=sub):
                message(mask, pair, sub).wait_send()
                return inner

            lax.fori_loop(1, groups, sent, 0)
            layer = pair * PAIR + sub

            @pl.when(part < parts_n - 1)
            def _(layer=layer):
                edge(layer, 0).wait_send()

            @pl.when(part > 0)
            def _(layer=layer):
                edge(layer, 1).wait_send()

        return carry

    lax.fori_loop(0, pairs, drain, 0)


def write_kernel(
    dims, table_ref, codes_ref, scale_ref, recv_ref, codes_out, scale_out, codes, scales, rem_code, rem_scale, rows, sems
):
    slots = dims[0]
    layers = codes_ref.shape[0]
    done = layers - PAIR
    pair = recv_ref.shape[1] - 1
    me = lax.axis_index("serve")
    copies = [pltpu.make_async_copy(codes_ref.at[n], codes_out.at[n], sems.at[n]) for n in range(done)]
    for copy in copies:
        copy.start()

    def put_code(i, low, high, code):
        codes[i // slots, i % slots, :, low:high] = code.astype(codes.dtype)

    def mask(layer, k, scale):
        return jnp.where(table_ref[layer, me * slots + k] > 0, scale, 0.0)

    def put_scale(sub, k, scale):
        scales[done + sub, k : k + 1, :] = mask(done + sub, k, scale)

    unpack_pair(dims, lambda s, n: recv_ref[s, pair, n], rem_code, rem_scale, rows, put_code, put_scale)
    tail = [
        pltpu.make_async_copy(codes, codes_out.at[pl.ds(done, PAIR)], sems.at[done]),
        pltpu.make_async_copy(scales, scale_out, sems.at[done + 1]),
    ]
    tail[0].start()

    def masked(layer, carry):
        for k in range(slots):
            scales[layer, k : k + 1, :] = mask(layer, k, scale_ref[layer, k : k + 1, :])
        return carry

    lax.fori_loop(0, done, masked, 0)
    tail[1].start()
    for copy in copies + tail:
        copy.wait()


def shards(train_weights, row_offset, block_group):
    train_n = lax.axis_size("train")
    serve_n = lax.axis_size("serve")
    layers, buffer_len, columns = train_weights.shape
    blocks_dev = block_group.shape[1]
    slots = (blocks_dev + serve_n - 1) // serve_n + 1
    full = columns // LANES
    rem = columns - full * LANES
    pairs = layers // PAIR
    pieces = PAIR * slots * full + (1 if rem else 0)
    width = columns * serve_n
    dtype = train_weights.dtype
    dims = (slots, full, rem, columns, serve_n)
    assert SHIFT == BLOCK and buffer_len % BLOCK == 0
    assert PAIR * slots * rem <= LANES and layers % PAIR == 0

    position = jnp.arange(blocks_dev, dtype=jnp.int32)
    earlier = position[None, :] < position[:, None]
    group_ids = block_group[:, :, 0]
    same_group = group_ids[:, :, None] == group_ids[:, None, :]
    order_in = jnp.sum((same_group & earlier[None]).astype(jnp.int32), axis=2)
    place = group_ids * slots + order_in
    slot_ids = jnp.arange(serve_n * slots, dtype=jnp.int32)
    hit = place[:, None, :] == slot_ids[None, :, None]
    table = jnp.sum(jnp.where(hit, position[None, None, :] + 1, 0), axis=2)

    smem = pl.BlockSpec(memory_space=pltpu.SMEM)
    vmem = pl.BlockSpec(memory_space=pltpu.VMEM)
    anywhere = pl.BlockSpec(memory_space=pl.ANY)
    codes, scales, received = pl.pallas_call(
        functools.partial(move_kernel, dims),
        in_specs=[smem, smem, anywhere],
        out_specs=[vmem, vmem, vmem],
        out_shape=[
            pltpu.VMEM((layers, slots, BLOCK, width), dtype),
            pltpu.VMEM((layers, slots, width), jnp.float32),
            pltpu.VMEM((serve_n, pairs, pieces, BLOCK, LANES), dtype),
        ],
        scratch_shapes=[
            pltpu.VMEM((serve_n, pairs, pieces, BLOCK, LANES), dtype),
            pltpu.VMEM((PAIR, columns, buffer_len), dtype),
            pltpu.VMEM((buffer_len // BLOCK, BLOCK, columns), dtype),
            pltpu.VMEM((serve_n, PAIR * slots, BLOCK, LANES), dtype),
            pltpu.VMEM((layers, 2, SHIFT, columns), dtype),
            pltpu.VMEM((layers, 2, SHIFT, columns), dtype),
            pltpu.VMEM((serve_n, BLOCK, LANES), jnp.float32),
            pltpu.VMEM((serve_n, 1, LANES), jnp.float32),
            pltpu.VMEM((PAIR * slots, 1, width), jnp.float32),
            pltpu.SemaphoreType.DMA((PAIR,)),
            pltpu.SemaphoreType.DMA((serve_n, pairs, PAIR)),
            pltpu.SemaphoreType.DMA((serve_n, pairs, PAIR)),
            pltpu.SemaphoreType.DMA((layers, 2)),
            pltpu.SemaphoreType.DMA((layers, 2)),
        ],
        compiler_params=pltpu.CompilerParams(
            collective_id=0, has_side_effects=True, vmem_limit_bytes=26 * MIB
        ),
        name="move",
    )(table, row_offset.T, jnp.swapaxes(train_weights, 1, 2))

    codes_out, scales_out = pl.pallas_call(
        functools.partial(write_kernel, dims),
        in_specs=[smem, vmem, vmem, vmem],
        out_specs=[pl.BlockSpec(memory_space=pltpu.HBM)] * 2,
        out_shape=[
            jax.ShapeDtypeStruct((layers, slots, BLOCK, width), dtype),
            jax.ShapeDtypeStruct((layers, slots, width), jnp.float32),
        ],
        scratch_shapes=[
            pltpu.VMEM((PAIR, slots, BLOCK, width), dtype),
            pltpu.VMEM((layers, slots, width), jnp.float32),
            pltpu.VMEM((serve_n, BLOCK, LANES), jnp.float32),
            pltpu.VMEM((serve_n, 1, LANES), jnp.float32),
            pltpu.VMEM((PAIR * slots, 1, width), jnp.float32),
            pltpu.SemaphoreType.DMA((layers,)),
        ],
        compiler_params=pltpu.CompilerParams(vmem_limit_bytes=6 * MIB),
        name="write",
    )(table, codes, scales, received)
    return (
        codes_out.reshape(layers, 1, 1, slots, BLOCK, width),
        scales_out.reshape(layers, 1, 1, slots, width),
    )


def solution(mesh):
    return jax.shard_map(
        shards,
        mesh=mesh,
        in_specs=(P(None, "train", "serve"), P(), P(None, "train", None)),
        out_specs=(
            P(None, "serve", "train", None, None, None),
            P(None, "serve", "train", None, None),
        ),
        check_vma=False,
    )
```

```python
import functools

import jax
import jax.numpy as jnp
from jax import lax
from jax.experimental import pallas as pl
from jax.experimental.pallas import tpu as pltpu
from jax.sharding import PartitionSpec as P

BLOCK = 32
SHIFT = 32
LANES = 128
PAIR = 2
RING = 3
MESH = pl.DeviceIdType.MESH
MIB = 1024 * 1024


def turned(values):
    return jnp.transpose(values.astype(jnp.float32))


def partner(me, mask, count):
    out, bit = 0, 1
    while bit < count:
        out = out + ((me // bit + mask // bit) % 2) * bit
        bit *= 2
    return out


def scaled(values):
    values = values.astype(jnp.float32)
    divisor = jnp.maximum(jnp.max(jnp.abs(values), axis=0, keepdims=True), 0.25)
    return values * (1.0 / divisor), divisor


def unpack_pair(dims, recv, rem_code, rem_scale, rows, put_code, put_scale):
    slots, full, rem, columns, sources = dims
    width = columns * sources
    tiles = -(-width // LANES)
    lane = lax.broadcasted_iota(jnp.int32, (BLOCK, LANES), 1)
    lane_row = lax.broadcasted_iota(jnp.int32, (1, LANES), 1)
    if rem:
        for s in range(sources):
            rem_code[s], rem_scale[s] = scaled(recv(s, PAIR * slots * full))

    def slot(i, carry):
        parts = [None] * tiles

        def put(tile, low, code, scale):
            if tile >= tiles:
                return
            if parts[tile] is None:
                parts[tile] = (code, scale)
            else:
                before = parts[tile]
                parts[tile] = (jnp.where(lane >= low, code, before[0]), jnp.where(lane_row >= low, scale, before[1]))

        def flush(below):
            for tile in range(below):
                if parts[tile] is not None:
                    code, scale = parts[tile]
                    end = min(width, (tile + 1) * LANES)
                    size = end - tile * LANES
                    put_code(i, tile * LANES, end, code[:, :size])
                    rows[i, :, tile * LANES : end] = scale[:, :size]
                    parts[tile] = None

        for s in range(sources):
            for t in range(full + (1 if rem else 0)):
                start = s * columns + t * LANES
                size = LANES if t < full else rem
                low = start % LANES
                if t < full:
                    code, scale = scaled(recv(s, i * full + t))
                    if low:
                        code, scale = pltpu.roll(code, low, 1), pltpu.roll(scale, low, 1)
                else:
                    turn = lax.rem(low + LANES - i * rem, LANES)
                    code, scale = pltpu.roll(rem_code[s], turn, 1), pltpu.roll(rem_scale[s], turn, 1)
                tile = start // LANES
                put(tile, low, code, scale)
                if low + size > LANES:
                    put(tile + 1, 0, code, scale)
                flush((start + size) // LANES)
        flush(tiles)
        return carry

    lax.fori_loop(0, PAIR * slots, slot, 0)
    for i in range(PAIR * slots):
        put_scale(i // slots, i % slots, rows[i])


def move_kernel(
    dims,
    offset_ref,
    group_ref,
    wt_ref,
    codes_ref,
    scale_ref,
    recv_ref,
    send_ref,
    in_ref,
    w_ref,
    rem_ref,
    edge_ref,
    halo_ref,
    rem_code,
    rem_scale,
    rows,
    table_ref,
    table_smem,
    in_sem,
    table_sem,
    send_sem,
    recv_sem,
    halo_send,
    halo_recv,
):
    slots, full, rem, columns, groups = dims
    pairs = recv_ref.shape[1]
    layers = pairs * PAIR
    blocks = w_ref.shape[0]
    buffer_len = blocks * BLOCK
    rows_dev = buffer_len - 2 * SHIFT
    me = lax.axis_index("serve")
    part = lax.axis_index("train")
    parts_n = lax.axis_size("train")
    half = slots * full
    rest = half + (1 if rem else 0)

    def fetch(layer, sub):
        return pltpu.make_async_copy(wt_ref.at[layer], in_ref.at[sub], in_sem.at[sub])

    def message(mask, pair, sub):
        peer = partner(me, mask, groups)
        span = pl.ds(sub * half, rest if sub == PAIR - 1 else half)
        return pltpu.make_async_remote_copy(
            send_ref.at[peer, pair % RING, span],
            recv_ref.at[me, pair, span],
            send_sem.at[mask, pair % RING, sub],
            recv_sem.at[mask, pair, sub],
            device_id={"serve": peer},
            device_id_type=MESH,
        )

    def arrival(mask, pair, sub):
        peer = partner(me, mask, groups)
        span = pl.ds(sub * half, rest if sub == PAIR - 1 else half)
        return pltpu.make_async_remote_copy(
            recv_ref.at[peer, pair, span],
            recv_ref.at[peer, pair, span],
            send_sem.at[mask, pair % RING, sub],
            recv_sem.at[mask, pair, sub],
            device_id={"serve": peer},
            device_id_type=MESH,
        )

    def edge(layer, side):
        to = part + 1 if side == 0 else part - 1
        return pltpu.make_async_remote_copy(
            edge_ref.at[layer, side],
            halo_ref.at[layer, side],
            halo_send.at[layer, side],
            halo_recv.at[layer, side],
            device_id={"train": to},
            device_id_type=MESH,
        )

    for sub in range(PAIR):
        fetch(sub, sub).start()

    barrier = pltpu.get_barrier_semaphore()

    def greet(mask, carry):
        pl.semaphore_signal(barrier, inc=1, device_id={"serve": partner(me, mask, groups)}, device_id_type=MESH)
        return carry

    lax.fori_loop(1, groups, greet, 0)

    @pl.when(part > 0)
    def _():
        pl.semaphore_signal(barrier, inc=1, device_id={"train": part - 1}, device_id_type=MESH)

    @pl.when(part < parts_n - 1)
    def _():
        pl.semaphore_signal(barrier, inc=1, device_id={"train": part + 1}, device_id_type=MESH)

    below = (part + parts_n - 1) // parts_n
    above = (2 * parts_n - 2 - part) // parts_n

    spot = lax.broadcasted_iota(jnp.int32, table_ref.shape, 1)
    spot_group = jnp.zeros(table_ref.shape, jnp.int32)
    for g in range(1, groups):
        spot_group = spot_group + jnp.where(spot >= g * slots, 1, 0)
    spot_slot = spot - spot_group * slots
    seen = jnp.zeros(table_ref.shape, jnp.int32)
    table = jnp.zeros(table_ref.shape, jnp.int32)
    for j in range(group_ref.shape[1]):
        mine = group_ref[:, j : j + 1] == spot_group
        table = jnp.where(mine & (seen == spot_slot), j + 1, table)
        seen = jnp.where(mine, seen + 1, seen)
    table_ref[...] = table
    to_smem = pltpu.make_async_copy(table_ref, table_smem, table_sem)
    to_smem.start()
    pl.semaphore_wait(barrier, groups - 1 + below + above)
    to_smem.wait()

    row = lax.broadcasted_iota(jnp.int32, (BLOCK, columns), 0)
    lane = lax.broadcasted_iota(jnp.int32, (BLOCK, LANES), 1)
    last = rows_dev - BLOCK

    def transpose_tile(sub, low):
        high = min(low + LANES, buffer_len)
        rows_of = turned(in_ref[sub, :, low:high]).astype(w_ref.dtype)
        w_ref[low // BLOCK : high // BLOCK] = rows_of.reshape((high - low) // BLOCK, BLOCK, columns)

    def pack_layer(pair, sub):
        layer = pair * PAIR + sub
        fetch(layer, sub).wait()
        lows = list(range(0, buffer_len, LANES))
        lows = [lows[0], lows[-1]] + lows[1:-1]
        for low in lows[:2]:
            transpose_tile(sub, low)
        edge_ref[layer, 0] = w_ref[blocks - 1]
        edge_ref[layer, 1] = w_ref[0]

        @pl.when(part < parts_n - 1)
        def _():
            edge(layer, 0).start()

        @pl.when(part > 0)
        def _():
            edge(layer, 1).start()

        for low in lows[2:]:
            transpose_tile(sub, low)

        @pl.when(layer + PAIR < layers)
        def _():
            fetch(layer + PAIR, sub).start()

        base = part * rows_dev

        @pl.when(part > 0)
        def _():
            edge(layer, 0).wait_recv()
            first = offset_ref[part, layer] - base
            head = jnp.where(row < first, halo_ref[layer, 0].astype(jnp.float32), w_ref[1].astype(jnp.float32))
            w_ref[1] = head.astype(w_ref.dtype)

        @pl.when(part < parts_n - 1)
        def _():
            edge(layer, 1).wait_recv()
            after = offset_ref[part + 1, layer] - base
            tail = w_ref[blocks - 2].astype(jnp.float32)
            tail = jnp.where(row + last >= after, halo_ref[layer, 1].astype(jnp.float32), tail)
            w_ref[blocks - 2] = tail.astype(w_ref.dtype)

        w_ref[0] = jnp.zeros((BLOCK, columns), w_ref.dtype)

        def gather(group, out):
            for k in range(slots):
                block = w_ref[table_smem[layer, group * slots + k]]
                for t in range(full):
                    out[(sub * slots + k) * full + t] = block[:, t * LANES : (t + 1) * LANES]
                if rem:
                    rem_ref[group, sub * slots + k, :, 0:rem] = block[:, full * LANES :]
            if rem and sub == PAIR - 1:
                tile = rem_ref[group, 0].astype(jnp.float32)
                for i in range(1, PAIR * slots):
                    moved = pltpu.roll(rem_ref[group, i].astype(jnp.float32), i * rem, 1)
                    tile = jnp.where(lane >= i * rem, moved, tile)
                out[PAIR * half] = tile.astype(out.dtype)

        def give(mask, carry):
            peer = partner(me, mask, groups)
            gather(peer, send_ref.at[peer, pair % RING])
            message(mask, pair, sub).start()
            return carry

        lax.fori_loop(2, groups, give, 0)
        give(1, 0)
        gather(me, recv_ref.at[me, pair])

    def take(pair):
        for sub in range(PAIR):

            def arrive(mask, carry, sub=sub):
                arrival(mask, pair, sub).wait_recv()
                return carry

            lax.fori_loop(1, groups, arrive, 0)

    def unpack(pair):
        def put_code(i, low, high, code):
            codes_ref[pair * PAIR + i // slots, i % slots, :, low:high] = code.astype(codes_ref.dtype)

        def put_scale(sub, k, scale):
            scale_ref[pair * PAIR + sub, k : k + 1, :] = scale

        unpack_pair(dims, lambda s, n: recv_ref[s, pair, n], rem_code, rem_scale, rows, put_code, put_scale)

    def sent(pair):
        for sub in range(PAIR):

            def leave(mask, carry, sub=sub):
                message(mask, pair, sub).wait_send()
                return carry

            lax.fori_loop(1, groups, leave, 0)

    def step(pair, carry):
        @pl.when(pair >= RING)
        def _():
            sent(pair - RING)

        for sub in range(PAIR):
            pack_layer(pair, sub)

        @pl.when(pair > 0)
        def _():
            take(pair - 1)
            unpack(pair - 1)

        return carry

    lax.fori_loop(0, pairs, step, 0)
    take(pairs - 1)
    unpack(pairs - 1)

    def drain(pair, carry):
        sent(pair)
        return carry

    lax.fori_loop(max(0, pairs - RING), pairs, drain, 0)

    def edges(layer, carry):
        @pl.when(part < parts_n - 1)
        def _():
            edge(layer, 0).wait_send()

        @pl.when(part > 0)
        def _():
            edge(layer, 1).wait_send()

        return carry

    lax.fori_loop(0, layers, edges, 0)


def write_kernel(group_ref, codes_ref, scale_ref, codes_out, scale_out, scales, sems):
    layers = codes_ref.shape[0]
    me = lax.axis_index("serve")
    copies = [pltpu.make_async_copy(codes_ref.at[n], codes_out.at[n], sems.at[n]) for n in range(layers)]
    for copy in copies:
        copy.start()
    slot = lax.broadcasted_iota(jnp.int32, scales.shape[1:], 0)
    for layer in range(layers):
        count = jnp.sum(jnp.where(group_ref[layer : layer + 1, :] == me, 1, 0), axis=1, keepdims=True)
        scales[layer] = jnp.where(slot < count, scale_ref[layer], 0.0)
    copies.append(pltpu.make_async_copy(scales, scale_out, sems.at[layers]))
    copies[-1].start()
    for copy in copies:
        copy.wait()


def shards(train_weights, row_offset, block_group):
    train_n = lax.axis_size("train")
    serve_n = lax.axis_size("serve")
    layers, buffer_len, columns = train_weights.shape
    blocks_dev = block_group.shape[1]
    slots = (blocks_dev + serve_n - 1) // serve_n + 1
    full = columns // LANES
    rem = columns - full * LANES
    pairs = layers // PAIR
    pieces = PAIR * slots * full + (1 if rem else 0)
    width = columns * serve_n
    dtype = train_weights.dtype
    spots = -(-serve_n * slots // LANES) * LANES
    dims = (slots, full, rem, columns, serve_n)
    assert SHIFT == BLOCK and buffer_len % BLOCK == 0
    assert PAIR * slots * rem <= LANES and layers % PAIR == 0

    group_ids = block_group[:, :, 0]

    smem = pl.BlockSpec(memory_space=pltpu.SMEM)
    vmem = pl.BlockSpec(memory_space=pltpu.VMEM)
    anywhere = pl.BlockSpec(memory_space=pl.ANY)
    codes, scales = pl.pallas_call(
        functools.partial(move_kernel, dims),
        in_specs=[smem, vmem, anywhere],
        out_specs=[vmem, vmem],
        out_shape=[
            pltpu.VMEM((layers, slots, BLOCK, width), dtype),
            pltpu.VMEM((layers, slots, width), jnp.float32),
        ],
        scratch_shapes=[
            pltpu.VMEM((serve_n, pairs, pieces, BLOCK, LANES), dtype),
            pltpu.VMEM((serve_n, RING, pieces, BLOCK, LANES), dtype),
            pltpu.VMEM((PAIR, columns, buffer_len), dtype),
            pltpu.VMEM((buffer_len // BLOCK, BLOCK, columns), dtype),
            pltpu.VMEM((serve_n, PAIR * slots, BLOCK, LANES), dtype),
            pltpu.VMEM((layers, 2, SHIFT, columns), dtype),
            pltpu.VMEM((layers, 2, SHIFT, columns), dtype),
            pltpu.VMEM((serve_n, BLOCK, LANES), jnp.float32),
            pltpu.VMEM((serve_n, 1, LANES), jnp.float32),
            pltpu.VMEM((PAIR * slots, 1, width), jnp.float32),
            pltpu.VMEM((layers, spots), jnp.int32),
            pltpu.SMEM((layers, spots), jnp.int32),
            pltpu.SemaphoreType.DMA((PAIR,)),
            pltpu.SemaphoreType.DMA,
            pltpu.SemaphoreType.DMA((serve_n, RING, PAIR)),
            pltpu.SemaphoreType.DMA((serve_n, pairs, PAIR)),
            pltpu.SemaphoreType.DMA((layers, 2)),
            pltpu.SemaphoreType.DMA((layers, 2)),
        ],
        compiler_params=pltpu.CompilerParams(
            collective_id=0, has_side_effects=True, vmem_limit_bytes=36 * MIB
        ),
        name="move",
    )(row_offset.T, group_ids, jnp.swapaxes(train_weights, 1, 2))

    codes_out, scales_out = pl.pallas_call(
        write_kernel,
        in_specs=[vmem, anywhere, vmem],
        out_specs=[pl.BlockSpec(memory_space=pltpu.HBM)] * 2,
        out_shape=[
            jax.ShapeDtypeStruct((layers, slots, BLOCK, width), dtype),
            jax.ShapeDtypeStruct((layers, slots, width), jnp.float32),
        ],
        scratch_shapes=[
            pltpu.VMEM((layers, slots, width), jnp.float32),
            pltpu.SemaphoreType.DMA((layers + 1,)),
        ],
        compiler_params=pltpu.CompilerParams(vmem_limit_bytes=2 * MIB),
        name="write",
    )(group_ids, codes, scales)
    return (
        codes_out.reshape(layers, 1, 1, slots, BLOCK, width),
        scales_out.reshape(layers, 1, 1, slots, width),
    )


def solution(mesh):
    return jax.shard_map(
        shards,
        mesh=mesh,
        in_specs=(P(None, "train", "serve"), P(), P(None, "train", None)),
        out_specs=(
            P(None, "serve", "train", None, None, None),
            P(None, "serve", "train", None, None),
        ),
        check_vma=False,
    )
```

```python
import functools

import jax
import jax.numpy as jnp
from jax import lax
from jax.experimental import pallas as pl
from jax.experimental.pallas import tpu as pltpu
from jax.sharding import PartitionSpec as P

BLOCK = 32
SHIFT = 32
LANES = 128
PAIR = 2
RING = 3
MESH = pl.DeviceIdType.MESH
MIB = 1024 * 1024


def turned(values):
    return jnp.transpose(values.astype(jnp.float32))


def partner(me, mask, count):
    out, bit = 0, 1
    while bit < count:
        out = out + ((me // bit + mask // bit) % 2) * bit
        bit *= 2
    return out


def scaled(values):
    values = values.astype(jnp.float32)
    divisor = jnp.maximum(jnp.max(jnp.abs(values), axis=0, keepdims=True), 0.25)
    return values * (1.0 / divisor), divisor


def scale_rest(dims, count, recv, rem_code, rem_scale):
    full, rem, columns, sources = dims
    if rem:
        for s in range(sources):
            rem_code[s], rem_scale[s] = scaled(recv(s, count * full))


def scale_slot(dims, i, recv, rem_code, rem_scale, put_code, put_scale):
    full, rem, columns, sources = dims
    width = columns * sources
    tiles = -(-width // LANES)
    lane = lax.broadcasted_iota(jnp.int32, (BLOCK, LANES), 1)
    lane_row = lax.broadcasted_iota(jnp.int32, (1, LANES), 1)
    parts = [None] * tiles

    def put(tile, low, code, scale):
        if tile >= tiles:
            return
        if parts[tile] is None:
            parts[tile] = (code, scale)
        else:
            before = parts[tile]
            parts[tile] = (jnp.where(lane >= low, code, before[0]), jnp.where(lane_row >= low, scale, before[1]))

    def flush(below):
        for tile in range(below):
            if parts[tile] is not None:
                code, scale = parts[tile]
                end = min(width, (tile + 1) * LANES)
                size = end - tile * LANES
                put_code(tile * LANES, end, code[:, :size])
                put_scale(tile * LANES, end, scale[:, :size])
                parts[tile] = None

    for s in range(sources):
        for t in range(full + (1 if rem else 0)):
            start = s * columns + t * LANES
            size = LANES if t < full else rem
            low = start % LANES
            if t < full:
                code, scale = scaled(recv(s, i * full + t))
                if low:
                    code, scale = pltpu.roll(code, low, 1), pltpu.roll(scale, low, 1)
            else:
                turn = lax.rem(low + LANES - i * rem, LANES)
                code, scale = pltpu.roll(rem_code[s], turn, 1), pltpu.roll(rem_scale[s], turn, 1)
            tile = start // LANES
            put(tile, low, code, scale)
            if low + size > LANES:
                put(tile + 1, 0, code, scale)
            flush((start + size) // LANES)
    flush(tiles)


def move_kernel(
    dims,
    base,
    offset_ref,
    group_ref,
    wt_ref,
    codes_ref,
    scale_ref,
    first_ref,
    second_ref,
    longest_ref,
    recv_ref,
    send_ref,
    in_ref,
    w_ref,
    rem_ref,
    edge_ref,
    halo_ref,
    over_ref,
    list_ref,
    rem_code,
    rem_scale,
    rows,
    table_ref,
    table_smem,
    length_ref,
    lengths_ref,
    in_sem,
    table_sem,
    send_sem,
    recv_sem,
    halo_send,
    halo_recv,
    list_send,
    list_recv,
    length_send,
    length_recv,
    second_sem,
):
    full, rem, columns, groups = dims
    slots = base + 1
    pairs = recv_ref.shape[1]
    layers = pairs * PAIR
    listed = layers // 2
    blocks = w_ref.shape[0]
    buffer_len = blocks * BLOCK
    rows_dev = buffer_len - 2 * SHIFT
    me = lax.axis_index("serve")
    part = lax.axis_index("train")
    parts_n = lax.axis_size("train")
    half = base * full
    rest = half + (1 if rem else 0)

    def fetch(layer, sub):
        return pltpu.make_async_copy(wt_ref.at[layer], in_ref.at[sub], in_sem.at[sub])

    def message(mask, pair, sub):
        peer = partner(me, mask, groups)
        span = pl.ds(sub * half, rest if sub == PAIR - 1 else half)
        return pltpu.make_async_remote_copy(
            send_ref.at[peer, pair % RING, span],
            recv_ref.at[me, pair, span],
            send_sem.at[mask, pair % RING, sub],
            recv_sem.at[mask, pair, sub],
            device_id={"serve": peer},
            device_id_type=MESH,
        )

    def arrival(mask, pair, sub):
        peer = partner(me, mask, groups)
        span = pl.ds(sub * half, rest if sub == PAIR - 1 else half)
        return pltpu.make_async_remote_copy(
            recv_ref.at[peer, pair, span],
            recv_ref.at[peer, pair, span],
            send_sem.at[mask, pair % RING, sub],
            recv_sem.at[mask, pair, sub],
            device_id={"serve": peer},
            device_id_type=MESH,
        )

    def list_message(mask):
        peer = partner(me, mask, groups)
        return pltpu.make_async_remote_copy(
            list_ref.at[0, peer],
            first_ref.at[me],
            list_send.at[mask],
            list_recv.at[mask],
            device_id={"serve": peer},
            device_id_type=MESH,
        )

    def edge(layer, side):
        to = part + 1 if side == 0 else part - 1
        return pltpu.make_async_remote_copy(
            edge_ref.at[layer, side],
            halo_ref.at[layer, side],
            halo_send.at[layer, side],
            halo_recv.at[layer, side],
            device_id={"train": to},
            device_id_type=MESH,
        )

    def length_message(ahead):
        return pltpu.make_async_remote_copy(
            length_ref,
            lengths_ref.at[ahead],
            length_send.at[ahead],
            length_recv.at[ahead],
            device_id={"train": (part + ahead) % parts_n},
            device_id_type=MESH,
        )

    for sub in range(PAIR):
        fetch(sub, sub).start()

    barrier = pltpu.get_barrier_semaphore()

    def greet(mask, carry):
        pl.semaphore_signal(barrier, inc=1, device_id={"serve": partner(me, mask, groups)}, device_id_type=MESH)
        return carry

    lax.fori_loop(1, groups, greet, 0)
    for ahead in range(1, parts_n):
        pl.semaphore_signal(barrier, inc=1, device_id={"train": (part + ahead) % parts_n}, device_id_type=MESH)

    spot = lax.broadcasted_iota(jnp.int32, (layers, groups * layers), 1)
    spot_group = jnp.zeros(spot.shape, jnp.int32)
    for g in range(1, groups):
        spot_group = spot_group + jnp.where(spot >= g * layers, 1, 0)
    spot_slot = spot - spot_group * layers
    seen = jnp.zeros(spot.shape, jnp.int32)
    table = jnp.zeros(spot.shape, jnp.int32)
    for j in range(group_ref.shape[1]):
        mine = group_ref[:, j : j + 1] == spot_group
        table = jnp.where(mine & (seen == spot_slot), j + 1, table)
        seen = jnp.where(mine, seen + 1, seen)
    table_ref[0:layers, :] = table
    length = jnp.zeros((1, groups * layers), jnp.int32)
    entry = jnp.full((1, groups * layers), layers, jnp.int32)
    for n in range(layers):
        long = seen[n : n + 1, :] == slots
        entry = jnp.where(long & (length == spot_slot[0:1, :]), n, entry)
        length = jnp.where(long, length + 1, length)
    table_ref[layers : layers + 1, :] = entry
    to_smem = pltpu.make_async_copy(table_ref, table_smem, table_sem)
    to_smem.start()
    most = jnp.max(length.astype(jnp.float32), axis=1, keepdims=True)
    length_ref[...] = jnp.broadcast_to(most, length_ref.shape)
    over_ref[:, layers] = jnp.zeros((groups, BLOCK, columns), over_ref.dtype)
    to_smem.wait()
    pl.semaphore_wait(barrier, groups - 1 + parts_n - 1)

    row = lax.broadcasted_iota(jnp.int32, (BLOCK, columns), 0)
    lane = lax.broadcasted_iota(jnp.int32, (BLOCK, LANES), 1)
    last = rows_dev - BLOCK

    def transpose_tile(sub, low):
        high = min(low + LANES, buffer_len)
        rows_of = turned(in_ref[sub, :, low:high]).astype(w_ref.dtype)
        w_ref[low // BLOCK : high // BLOCK] = rows_of.reshape((high - low) // BLOCK, BLOCK, columns)

    def joined(group, count):
        tile = rem_ref[group, 0].astype(jnp.float32)
        for i in range(1, count):
            moved = pltpu.roll(rem_ref[group, i].astype(jnp.float32), i * rem, 1)
            tile = jnp.where(lane >= i * rem, moved, tile)
        return tile

    def pack_layer(pair, sub):
        layer = pair * PAIR + sub
        fetch(layer, sub).wait()
        lows = list(range(0, buffer_len, LANES))
        lows = [lows[0], lows[-1]] + lows[1:-1]
        for low in lows[:2]:
            transpose_tile(sub, low)
        edge_ref[layer, 0] = w_ref[blocks - 1]
        edge_ref[layer, 1] = w_ref[0]

        @pl.when(part < parts_n - 1)
        def _():
            edge(layer, 0).start()

        @pl.when(part > 0)
        def _():
            edge(layer, 1).start()

        for low in lows[2:]:
            transpose_tile(sub, low)

        @pl.when(layer + PAIR < layers)
        def _():
            fetch(layer + PAIR, sub).start()

        base_row = part * rows_dev

        @pl.when(part > 0)
        def _():
            edge(layer, 0).wait_recv()
            first = offset_ref[part, layer] - base_row
            head = jnp.where(row < first, halo_ref[layer, 0].astype(jnp.float32), w_ref[1].astype(jnp.float32))
            w_ref[1] = head.astype(w_ref.dtype)

        @pl.when(part < parts_n - 1)
        def _():
            edge(layer, 1).wait_recv()
            after = offset_ref[part + 1, layer] - base_row
            tail = w_ref[blocks - 2].astype(jnp.float32)
            tail = jnp.where(row + last >= after, halo_ref[layer, 1].astype(jnp.float32), tail)
            w_ref[blocks - 2] = tail.astype(w_ref.dtype)

        w_ref[0] = jnp.zeros((BLOCK, columns), w_ref.dtype)

        def gather(group, out):
            for k in range(base):
                block = w_ref[table_smem[layer, group * layers + k]]
                for t in range(full):
                    out[(sub * base + k) * full + t] = block[:, t * LANES : (t + 1) * LANES]
                if rem:
                    rem_ref[group, sub * base + k, :, 0:rem] = block[:, full * LANES :]
            over_ref[group, layer] = w_ref[table_smem[layer, group * layers + base]]
            if rem and sub == PAIR - 1:
                out[PAIR * half] = joined(group, PAIR * base).astype(out.dtype)

        def give(mask, carry):
            peer = partner(me, mask, groups)
            gather(peer, send_ref.at[peer, pair % RING])
            message(mask, pair, sub).start()
            return carry

        lax.fori_loop(2, groups, give, 0)
        give(1, 0)
        gather(me, recv_ref.at[me, pair])

    def pack_list(group, which, out):
        for e in range(listed):
            block = over_ref[group, table_smem[layers, group * layers + which * listed + e]]
            for t in range(full):
                out[e * full + t] = block[:, t * LANES : (t + 1) * LANES]
            if rem:
                rem_ref[group, e, :, 0:rem] = block[:, full * LANES :]
        if rem:
            out[listed * full] = joined(group, listed).astype(out.dtype)

    def take(pair):
        for sub in range(PAIR):

            def arrive(mask, carry, sub=sub):
                arrival(mask, pair, sub).wait_recv()
                return carry

            lax.fori_loop(1, groups, arrive, 0)

    def unpack(pair):
        def recv(s, n):
            return recv_ref[s, pair, n]

        scale_rest(dims, PAIR * base, recv, rem_code, rem_scale)

        def slot(i, carry):
            def put_code(low, high, code):
                codes_ref[pair * PAIR + i // base, i % base, :, low:high] = code.astype(codes_ref.dtype)

            def put_scale(low, high, scale):
                rows[i, :, low:high] = scale

            scale_slot(dims, i, recv, rem_code, rem_scale, put_code, put_scale)
            return carry

        lax.fori_loop(0, PAIR * base, slot, 0)
        for i in range(PAIR * base):
            scale_ref[pair * PAIR + i // base, i % base : i % base + 1, :] = rows[i]

    def sent(pair):
        for sub in range(PAIR):

            def leave(mask, carry, sub=sub):
                message(mask, pair, sub).wait_send()
                return carry

            lax.fori_loop(1, groups, leave, 0)

    def step(pair, carry):
        @pl.when(pair >= RING)
        def _():
            sent(pair - RING)

        for sub in range(PAIR):
            pack_layer(pair, sub)

        @pl.when(pair > 0)
        def _():
            take(pair - 1)
            unpack(pair - 1)

        return carry

    for ahead in range(1, parts_n):
        length_message(ahead).start()
    lax.fori_loop(0, pairs, step, 0)

    def give_list(mask, carry):
        peer = partner(me, mask, groups)
        pack_list(peer, 0, list_ref.at[0, peer])
        list_message(mask).start()
        return carry

    lax.fori_loop(1, groups, give_list, 0)
    pack_list(me, 0, first_ref.at[me])

    def second(group, carry):
        pack_list(group, 1, list_ref.at[1, group])
        return carry

    lax.fori_loop(0, groups, second, 0)
    keep = pltpu.make_async_copy(list_ref.at[1], second_ref, second_sem)
    keep.start()
    for ahead in range(1, parts_n):
        length_message(ahead).wait()
        most = jnp.maximum(most, lengths_ref[ahead, 0:1, 0:1])
    longest_ref[0, 0] = jnp.max(most).astype(jnp.int32)

    take(pairs - 1)
    unpack(pairs - 1)

    def drain(pair, carry):
        sent(pair)
        return carry

    lax.fori_loop(max(0, pairs - RING), pairs, drain, 0)

    def edges(layer, carry):
        @pl.when(part < parts_n - 1)
        def _():
            edge(layer, 0).wait_send()

        @pl.when(part > 0)
        def _():
            edge(layer, 1).wait_send()

        return carry

    lax.fori_loop(0, layers, edges, 0)
    keep.wait()

    def listed_all(mask, carry):
        list_message(mask).wait()
        return carry

    lax.fori_loop(1, groups, listed_all, 0)


def list_places(group_ref, place_ref, slots):
    layers = group_ref.shape[0]
    me = lax.axis_index("serve")
    count = jnp.sum(jnp.where(group_ref[...] == me, 1, 0), axis=1, keepdims=True)
    length = jnp.zeros((1, 1), jnp.int32)
    for n in range(layers):
        long = count[n : n + 1, :] == slots
        place_ref[n : n + 1, :] = jnp.broadcast_to(jnp.where(long, length, layers), (1, place_ref.shape[1]))
        length = jnp.where(long, length + 1, length)
    return count


def write_kernel(
    dims,
    base,
    group_ref,
    codes_ref,
    scale_ref,
    first_ref,
    codes_out,
    scale_out,
    scales,
    extra,
    extra_scale,
    rem_code,
    rem_scale,
    place_ref,
    place_smem,
    sems,
    extra_sems,
    place_sem,
):
    full, rem, columns, groups = dims
    layers = codes_ref.shape[0]
    listed = layers // 2
    copies = [
        pltpu.make_async_copy(codes_ref.at[n], codes_out.at[n, pl.ds(0, base)], sems.at[n]) for n in range(layers)
    ]
    for copy in copies:
        copy.start()
    count = list_places(group_ref, place_ref, base + 1)
    to_smem = pltpu.make_async_copy(place_ref, place_smem, place_sem)
    to_smem.start()
    extra[layers] = jnp.zeros(extra.shape[1:], extra.dtype)

    def recv(s, n):
        return first_ref[s, n]

    scale_rest(dims, listed, recv, rem_code, rem_scale)
    slot = lax.broadcasted_iota(jnp.int32, scales.shape[1:], 0)
    to_smem.wait()

    def last_slot(layer, carry):
        place = place_smem[layer, 0]
        long = place < layers
        extra_scale[layer] = jnp.zeros(extra_scale.shape[1:], jnp.float32)

        @pl.when(long)
        def _():
            def put_code(low, high, code):
                extra[layer, :, low:high] = code.astype(extra.dtype)

            def put_scale(low, high, scale):
                extra_scale[layer, :, low:high] = scale

            scale_slot(dims, jnp.minimum(place, listed - 1), recv, rem_code, rem_scale, put_code, put_scale)

        pltpu.make_async_copy(
            extra.at[jnp.where(long, layer, layers)], codes_out.at[layer, base], extra_sems.at[layer]
        ).start()
        return carry

    lax.fori_loop(0, layers, last_slot, 0)
    for n in range(layers):
        own = jnp.where(slot < count[n : n + 1, :], scale_ref[n], 0.0)
        scales[n] = jnp.where(slot < base, own, jnp.broadcast_to(extra_scale[n], own.shape))
    copies.append(pltpu.make_async_copy(scales, scale_out, sems.at[layers]))
    copies[-1].start()
    for n in range(layers):
        copies.append(pltpu.make_async_copy(extra.at[n], codes_out.at[n, base], extra_sems.at[n]))
    for copy in copies:
        copy.wait()


def late_kernel(
    dims,
    base,
    group_ref,
    got_ref,
    codes_in,
    scale_in,
    codes_out,
    scale_out,
    extra,
    extra_scale,
    scales,
    rem_code,
    rem_scale,
    place_ref,
    place_smem,
    sem,
):
    del codes_in, scale_in
    full, rem, columns, groups = dims
    layers = codes_out.shape[0]
    listed = layers // 2
    list_places(group_ref, place_ref, base + 1)
    to_smem = pltpu.make_async_copy(place_ref, place_smem, sem)
    to_smem.start()
    to_smem.wait()

    def recv(s, n):
        return got_ref[s, n]

    scale_rest(dims, listed, recv, rem_code, rem_scale)
    slot = lax.broadcasted_iota(jnp.int32, scales.shape, 0)

    def last_slot(layer, carry):
        place = place_smem[layer, 0]

        @pl.when((place >= listed) & (place < layers))
        def _():
            def put_code(low, high, code):
                extra[:, low:high] = code.astype(extra.dtype)

            def put_scale(low, high, scale):
                extra_scale[:, low:high] = scale

            scale_slot(dims, place - listed, recv, rem_code, rem_scale, put_code, put_scale)
            pltpu.sync_copy(extra, codes_out.at[layer, base])
            pltpu.sync_copy(scale_out.at[layer], scales)
            scales[...] = jnp.where(slot < base, scales[...], jnp.broadcast_to(extra_scale[...], scales.shape))
            pltpu.sync_copy(scales, scale_out.at[layer])

        return carry

    lax.fori_loop(0, layers, last_slot, 0)


def shards(train_weights, row_offset, block_group):
    train_n = lax.axis_size("train")
    serve_n = lax.axis_size("serve")
    layers, buffer_len, columns = train_weights.shape
    blocks_dev = block_group.shape[1]
    base = (blocks_dev + serve_n - 1) // serve_n
    slots = base + 1
    full = columns // LANES
    rem = columns - full * LANES
    pairs = layers // PAIR
    listed = layers // 2
    pieces = PAIR * base * full + (1 if rem else 0)
    pieces_list = listed * full + (1 if rem else 0)
    rests = max(PAIR * base, listed)
    spots = serve_n * layers
    width = columns * serve_n
    dtype = train_weights.dtype
    dims = (full, rem, columns, serve_n)
    assert SHIFT == BLOCK and buffer_len % BLOCK == 0
    assert rests * rem <= LANES and layers % PAIR == 0 and slots <= layers

    group_ids = block_group[:, :, 0]
    smem = pl.BlockSpec(memory_space=pltpu.SMEM)
    vmem = pl.BlockSpec(memory_space=pltpu.VMEM)
    anywhere = pl.BlockSpec(memory_space=pl.ANY)
    codes, scales, first, second, longest = pl.pallas_call(
        functools.partial(move_kernel, dims, base),
        in_specs=[smem, vmem, anywhere],
        out_specs=[vmem, vmem, vmem, pl.BlockSpec(memory_space=pltpu.HBM), smem],
        out_shape=[
            pltpu.VMEM((layers, base, BLOCK, width), dtype),
            pltpu.VMEM((layers, slots, width), jnp.float32),
            pltpu.VMEM((serve_n, pieces_list, BLOCK, LANES), dtype),
            jax.ShapeDtypeStruct((serve_n, pieces_list, BLOCK, LANES), dtype),
            jax.ShapeDtypeStruct((1, 1), jnp.int32),
        ],
        scratch_shapes=[
            pltpu.VMEM((serve_n, pairs, pieces, BLOCK, LANES), dtype),
            pltpu.VMEM((serve_n, RING, pieces, BLOCK, LANES), dtype),
            pltpu.VMEM((PAIR, columns, buffer_len), dtype),
            pltpu.VMEM((buffer_len // BLOCK, BLOCK, columns), dtype),
            pltpu.VMEM((serve_n, rests, BLOCK, LANES), dtype),
            pltpu.VMEM((layers, 2, SHIFT, columns), dtype),
            pltpu.VMEM((layers, 2, SHIFT, columns), dtype),
            pltpu.VMEM((serve_n, layers + 1, BLOCK, columns), dtype),
            pltpu.VMEM((2, serve_n, pieces_list, BLOCK, LANES), dtype),
            pltpu.VMEM((serve_n, BLOCK, LANES), jnp.float32),
            pltpu.VMEM((serve_n, 1, LANES), jnp.float32),
            pltpu.VMEM((PAIR * base, 1, width), jnp.float32),
            pltpu.VMEM((layers + 8, spots), jnp.int32),
            pltpu.SMEM((layers + 8, spots), jnp.int32),
            pltpu.VMEM((8, LANES), jnp.float32),
            pltpu.VMEM((train_n, 8, LANES), jnp.float32),
            pltpu.SemaphoreType.DMA((PAIR,)),
            pltpu.SemaphoreType.DMA,
            pltpu.SemaphoreType.DMA((serve_n, RING, PAIR)),
            pltpu.SemaphoreType.DMA((serve_n, pairs, PAIR)),
            pltpu.SemaphoreType.DMA((layers, 2)),
            pltpu.SemaphoreType.DMA((layers, 2)),
            pltpu.SemaphoreType.DMA((serve_n,)),
            pltpu.SemaphoreType.DMA((serve_n,)),
            pltpu.SemaphoreType.DMA((train_n,)),
            pltpu.SemaphoreType.DMA((train_n,)),
            pltpu.SemaphoreType.DMA,
        ],
        compiler_params=pltpu.CompilerParams(
            collective_id=0, has_side_effects=True, vmem_limit_bytes=36 * MIB
        ),
        name="move",
    )(row_offset.T, group_ids, jnp.swapaxes(train_weights, 1, 2))

    codes_shape = jax.ShapeDtypeStruct((layers, slots, BLOCK, width), dtype)
    scales_shape = jax.ShapeDtypeStruct((layers, slots, width), jnp.float32)
    hbm = pl.BlockSpec(memory_space=pltpu.HBM)
    rest_scratch = [
        pltpu.VMEM((serve_n, BLOCK, LANES), jnp.float32),
        pltpu.VMEM((serve_n, 1, LANES), jnp.float32),
        pltpu.VMEM((layers, LANES), jnp.int32),
        pltpu.SMEM((layers, LANES), jnp.int32),
    ]
    codes_out, scales_out = pl.pallas_call(
        functools.partial(write_kernel, dims, base),
        in_specs=[vmem, anywhere, vmem, vmem],
        out_specs=[hbm, hbm],
        out_shape=[codes_shape, scales_shape],
        scratch_shapes=[
            pltpu.VMEM((layers, slots, width), jnp.float32),
            pltpu.VMEM((layers + 1, BLOCK, width), dtype),
            pltpu.VMEM((layers, 1, width), jnp.float32),
            *rest_scratch,
            pltpu.SemaphoreType.DMA((layers + 1,)),
            pltpu.SemaphoreType.DMA((layers,)),
            pltpu.SemaphoreType.DMA,
        ],
        compiler_params=pltpu.CompilerParams(vmem_limit_bytes=6 * MIB),
        name="write",
    )(group_ids, codes, scales, first)

    def late(state):
        got = lax.all_to_all(second, "serve", split_axis=0, concat_axis=0, tiled=True)
        late_codes, late_scales = pl.pallas_call(
            functools.partial(late_kernel, dims, base),
            in_specs=[vmem, vmem, hbm, hbm],
            out_specs=[hbm, hbm],
            out_shape=[codes_shape, scales_shape],
            input_output_aliases={2: 0, 3: 1},
            scratch_shapes=[
                pltpu.VMEM((BLOCK, width), dtype),
                pltpu.VMEM((1, width), jnp.float32),
                pltpu.VMEM((slots, width), jnp.float32),
                *rest_scratch,
                pltpu.SemaphoreType.DMA,
            ],
            compiler_params=pltpu.CompilerParams(vmem_limit_bytes=6 * MIB),
            name="late",
        )(group_ids, got, state[1], state[2])
        return jnp.zeros((), jnp.int32), late_codes, late_scales

    state = (longest[0, 0], codes_out, scales_out)
    _, codes_out, scales_out = lax.while_loop(lambda now: now[0] > listed, late, state)
    return (
        codes_out.reshape(layers, 1, 1, slots, BLOCK, width),
        scales_out.reshape(layers, 1, 1, slots, width),
    )


def solution(mesh):
    return jax.shard_map(
        shards,
        mesh=mesh,
        in_specs=(P(None, "train", "serve"), P(), P(None, "train", None)),
        out_specs=(
            P(None, "serve", "train", None, None, None),
            P(None, "serve", "train", None, None),
        ),
        check_vma=False,
    )
```

```python
import functools

import jax
import jax.numpy as jnp
from jax import lax
from jax.experimental import pallas as pl
from jax.experimental.pallas import tpu as pltpu
from jax.sharding import PartitionSpec as P

BLOCK = 32
SHIFT = 32
LANES = 128
PAIR = 2
RING = 3
MESH = pl.DeviceIdType.MESH
MIB = 1024 * 1024


def turned(values):
    return jnp.transpose(values.astype(jnp.float32))


def partner(me, mask, count):
    out, bit = 0, 1
    while bit < count:
        out = out + ((me // bit + mask // bit) % 2) * bit
        bit *= 2
    return out


def scaled(values):
    values = values.astype(jnp.float32)
    divisor = jnp.maximum(jnp.max(jnp.abs(values), axis=0, keepdims=True), 0.25)
    return values * (1.0 / divisor), divisor


def scale_rest(dims, count, recv, rem_code, rem_scale):
    full, rem, columns, sources = dims
    if rem:
        for s in range(sources):
            rem_code[s], rem_scale[s] = scaled(recv(s, count * full))


def scale_slot(dims, i, recv, rem_code, rem_scale, put_code, put_scale):
    full, rem, columns, sources = dims
    width = columns * sources
    tiles = -(-width // LANES)
    lane = lax.broadcasted_iota(jnp.int32, (BLOCK, LANES), 1)
    lane_row = lax.broadcasted_iota(jnp.int32, (1, LANES), 1)
    parts = [None] * tiles

    def put(tile, low, code, scale):
        if tile >= tiles:
            return
        if parts[tile] is None:
            parts[tile] = (code, scale)
        else:
            before = parts[tile]
            parts[tile] = (jnp.where(lane >= low, code, before[0]), jnp.where(lane_row >= low, scale, before[1]))

    def flush(below):
        for tile in range(below):
            if parts[tile] is not None:
                code, scale = parts[tile]
                end = min(width, (tile + 1) * LANES)
                size = end - tile * LANES
                put_code(tile * LANES, end, code[:, :size])
                put_scale(tile * LANES, end, scale[:, :size])
                parts[tile] = None

    for s in range(sources):
        for t in range(full + (1 if rem else 0)):
            start = s * columns + t * LANES
            size = LANES if t < full else rem
            low = start % LANES
            if t < full:
                code, scale = scaled(recv(s, i * full + t))
                if low:
                    code, scale = pltpu.roll(code, low, 1), pltpu.roll(scale, low, 1)
            else:
                turn = lax.rem(low + LANES - i * rem, LANES)
                code, scale = pltpu.roll(rem_code[s], turn, 1), pltpu.roll(rem_scale[s], turn, 1)
            tile = start // LANES
            put(tile, low, code, scale)
            if low + size > LANES:
                put(tile + 1, 0, code, scale)
            flush((start + size) // LANES)
    flush(tiles)


def move_kernel(
    dims,
    base,
    offset_hbm,
    group_hbm,
    wt_ref,
    codes_ref,
    scale_ref,
    tail_ref,
    all_ref,
    second_ref,
    longest_ref,
    recv_ref,
    send_ref,
    in_ref,
    w_ref,
    rem_ref,
    edge_ref,
    halo_ref,
    over_ref,
    list_ref,
    rem_code,
    rem_scale,
    rows,
    table_ref,
    table_smem,
    length_ref,
    lengths_ref,
    offset_ref,
    group_ref,
    in_sem,
    table_sem,
    small_sem,
    send_sem,
    recv_sem,
    halo_send,
    halo_recv,
    list_send,
    list_recv,
    length_send,
    length_recv,
    second_sem,
):
    full, rem, columns, groups = dims
    slots = base + 1
    pairs = recv_ref.shape[1] + 1
    layers = pairs * PAIR
    listed = layers // 2
    blocks = w_ref.shape[0]
    buffer_len = blocks * BLOCK
    rows_dev = buffer_len - 2 * SHIFT
    me = lax.axis_index("serve")
    part = lax.axis_index("train")
    parts_n = lax.axis_size("train")
    half = base * full
    rest = half + (1 if rem else 0)

    def fetch(layer, sub):
        return pltpu.make_async_copy(wt_ref.at[layer], in_ref.at[sub], in_sem.at[sub])

    def message(mask, pair, sub, final):
        peer = partner(me, mask, groups)
        span = pl.ds(sub * half, rest if sub == PAIR - 1 else half)
        return pltpu.make_async_remote_copy(
            send_ref.at[peer, pair % RING, span],
            tail_ref.at[me, span] if final else recv_ref.at[me, pair, span],
            send_sem.at[mask, pair % RING, sub],
            recv_sem.at[mask, pair, sub],
            device_id={"serve": peer},
            device_id_type=MESH,
        )

    def arrival(mask, pair, sub, final):
        peer = partner(me, mask, groups)
        span = pl.ds(sub * half, rest if sub == PAIR - 1 else half)
        place = tail_ref.at[peer, span] if final else recv_ref.at[peer, pair, span]
        return pltpu.make_async_remote_copy(
            place,
            place,
            send_sem.at[mask, pair % RING, sub],
            recv_sem.at[mask, pair, sub],
            device_id={"serve": peer},
            device_id_type=MESH,
        )

    bits = [1 << n for n in range(groups.bit_length() - 1)]
    orders = [bits[1:] + bits[:1], bits[:0:-1] + bits[:1]]
    pieces_list = all_ref.shape[1]
    spans = [pl.ds(0, pieces_list // 2), pl.ds(pieces_list // 2, pieces_list - pieces_list // 2)]

    def stage(number):
        for which, order in enumerate(orders):
            held = [0]
            for bit in order[:number]:
                held = held + [mask + bit for mask in held]
            for mask in held:
                yield which, order[number], mask

    def list_message(which, bit, mask):
        place = all_ref.at[partner(me, mask, groups), spans[which]]
        return pltpu.make_async_remote_copy(
            place,
            place,
            list_send.at[which, bit + mask],
            list_recv.at[which, bit + mask],
            device_id={"serve": partner(me, bit, groups)},
            device_id_type=MESH,
        )

    def list_arrival(which, bit, mask):
        place = all_ref.at[partner(me, bit + mask, groups), spans[which]]
        return pltpu.make_async_remote_copy(
            place,
            place,
            list_send.at[which, bit + mask],
            list_recv.at[which, bit + mask],
            device_id={"serve": partner(me, bit, groups)},
            device_id_type=MESH,
        )

    def edge(layer, side):
        to = part + 1 if side == 0 else part - 1
        return pltpu.make_async_remote_copy(
            edge_ref.at[layer, side],
            halo_ref.at[layer, side],
            halo_send.at[layer, side],
            halo_recv.at[layer, side],
            device_id={"train": to},
            device_id_type=MESH,
        )

    def length_message(ahead):
        return pltpu.make_async_remote_copy(
            length_ref,
            lengths_ref.at[ahead],
            length_send.at[ahead],
            length_recv.at[ahead],
            device_id={"train": (part + ahead) % parts_n},
            device_id_type=MESH,
        )

    get_group = pltpu.make_async_copy(group_hbm, group_ref, small_sem.at[0])
    get_group.start()
    fetch(0, 0).start()
    get_offset = pltpu.make_async_copy(offset_hbm, offset_ref, small_sem.at[1])
    get_offset.start()
    for sub in range(1, PAIR):
        fetch(sub, sub).start()

    barrier = pltpu.get_barrier_semaphore()

    def greet(mask, carry):
        pl.semaphore_signal(barrier, inc=1, device_id={"serve": partner(me, mask, groups)}, device_id_type=MESH)
        return carry

    lax.fori_loop(1, groups, greet, 0)
    for ahead in range(1, parts_n):
        pl.semaphore_signal(barrier, inc=1, device_id={"train": (part + ahead) % parts_n}, device_id_type=MESH)

    get_group.wait()
    spot = lax.broadcasted_iota(jnp.int32, (layers, groups * layers), 1)
    spot_group = jnp.zeros(spot.shape, jnp.int32)
    for g in range(1, groups):
        spot_group = spot_group + jnp.where(spot >= g * layers, 1, 0)
    spot_slot = spot - spot_group * layers
    seen = jnp.zeros(spot.shape, jnp.int32)
    table = jnp.zeros(spot.shape, jnp.int32)
    for j in range(group_ref.shape[1]):
        mine = group_ref[:, j : j + 1] == spot_group
        table = jnp.where(mine & (seen == spot_slot), j + 1, table)
        seen = jnp.where(mine, seen + 1, seen)
    table_ref[0:layers, :] = table
    none = layers * groups
    length = jnp.zeros((1, groups * layers), jnp.int32)
    entry = jnp.full(length.shape, none, jnp.int32)
    total = jnp.zeros((1, LANES), jnp.int32)
    shared = jnp.full(total.shape, none, jnp.int32)
    number = lax.broadcasted_iota(jnp.int32, total.shape, 1)
    long = jnp.where(seen == slots, 1, 0)
    for n in range(layers):
        here = long[n : n + 1, :]
        entry = jnp.where((here > 0) & (length == spot_slot[0:1, :]), n * groups + spot_group[0:1, :], entry)
        length = length + here
        for g in range(groups):
            one = jnp.broadcast_to(here[:, g * layers : g * layers + 1], total.shape)
            shared = jnp.where((one > 0) & (total == number), n * groups + g, shared)
            total = total + one
    table_ref[layers : layers + 1, :] = entry
    table_ref[layers + 1 : layers + 2, 0:LANES] = shared
    to_smem = pltpu.make_async_copy(table_ref, table_smem, table_sem)
    to_smem.start()
    most = total.astype(jnp.float32)
    length_ref[...] = jnp.broadcast_to(most, length_ref.shape)
    over_ref[none] = jnp.zeros((BLOCK, columns), over_ref.dtype)
    get_offset.wait()
    to_smem.wait()
    pl.semaphore_wait(barrier, groups - 1 + parts_n - 1)

    row = lax.broadcasted_iota(jnp.int32, (BLOCK, columns), 0)
    lane = lax.broadcasted_iota(jnp.int32, (BLOCK, LANES), 1)
    last = rows_dev - BLOCK

    def transpose_tile(sub, low):
        high = min(low + LANES, buffer_len)
        rows_of = turned(in_ref[sub, :, low:high]).astype(w_ref.dtype)
        w_ref[low // BLOCK : high // BLOCK] = rows_of.reshape((high - low) // BLOCK, BLOCK, columns)

    def joined(group, count):
        tile = rem_ref[group, 0].astype(jnp.float32)
        for i in range(1, count):
            moved = pltpu.roll(rem_ref[group, i].astype(jnp.float32), i * rem, 1)
            tile = jnp.where(lane >= i * rem, moved, tile)
        return tile

    def prepare(pair, sub):
        layer = pair * PAIR + sub
        fetch(layer, sub).wait()
        lows = list(range(0, buffer_len, LANES))
        lows = [lows[0], lows[-1]] + lows[1:-1]
        for low in lows[:2]:
            transpose_tile(sub, low)
        edge_ref[layer, 0] = w_ref[blocks - 1]
        edge_ref[layer, 1] = w_ref[0]

        @pl.when(part < parts_n - 1)
        def _():
            edge(layer, 0).start()

        @pl.when(part > 0)
        def _():
            edge(layer, 1).start()

        for low in lows[2:]:
            transpose_tile(sub, low)

        @pl.when(layer + PAIR < layers)
        def _():
            fetch(layer + PAIR, sub).start()

        base_row = part * rows_dev

        @pl.when(part > 0)
        def _():
            edge(layer, 0).wait_recv()
            first = offset_ref[part, layer] - base_row
            head = jnp.where(row < first, halo_ref[layer, 0].astype(jnp.float32), w_ref[1].astype(jnp.float32))
            w_ref[1] = head.astype(w_ref.dtype)

        @pl.when(part < parts_n - 1)
        def _():
            edge(layer, 1).wait_recv()
            after = offset_ref[part + 1, layer] - base_row
            tail = w_ref[blocks - 2].astype(jnp.float32)
            tail = jnp.where(row + last >= after, halo_ref[layer, 1].astype(jnp.float32), tail)
            w_ref[blocks - 2] = tail.astype(w_ref.dtype)

        w_ref[0] = jnp.zeros((BLOCK, columns), w_ref.dtype)

        def last_slots(group, carry):
            over_ref[layer * groups + group] = w_ref[table_smem[layer, group * layers + base]]
            return carry

        lax.fori_loop(0, groups, last_slots, 0)

    def gather(pair, sub, group, out):
        for k in range(base):
            block = w_ref[table_smem[pair * PAIR + sub, group * layers + k]]
            for t in range(full):
                out[(sub * base + k) * full + t] = block[:, t * LANES : (t + 1) * LANES]
            if rem:
                rem_ref[group, sub * base + k, :, 0:rem] = block[:, full * LANES :]
        if rem and sub == PAIR - 1:
            out[PAIR * half] = joined(group, PAIR * base).astype(out.dtype)

    def give(low, high, pair, sub, final):
        def one(mask, carry):
            peer = partner(me, mask, groups)
            gather(pair, sub, peer, send_ref.at[peer, pair % RING])
            message(mask, pair, sub, final).start()
            return carry

        lax.fori_loop(low, high, one, 0)

    def own(pair, sub, final):
        gather(pair, sub, me, tail_ref.at[me] if final else recv_ref.at[me, pair])

    def pack_list(entry_of, out):
        for e in range(listed):
            block = over_ref[entry_of(e)]
            for t in range(full):
                out[e * full + t] = block[:, t * LANES : (t + 1) * LANES]
            if rem:
                rem_ref[groups, e, :, 0:rem] = block[:, full * LANES :]
        if rem:
            out[listed * full] = joined(groups, listed).astype(out.dtype)

    def take(pair, final):
        for sub in range(PAIR):

            def arrive(mask, carry, sub=sub):
                arrival(mask, pair, sub, final).wait_recv()
                return carry

            lax.fori_loop(1, groups, arrive, 0)

    def unpack(pair):
        def recv(s, n):
            return recv_ref[s, pair, n]

        scale_rest(dims, PAIR * base, recv, rem_code, rem_scale)

        def slot(i, carry):
            def put_code(low, high, code):
                codes_ref[pair * PAIR + i // base, i % base, :, low:high] = code.astype(codes_ref.dtype)

            def put_scale(low, high, scale):
                rows[i, :, low:high] = scale

            scale_slot(dims, i, recv, rem_code, rem_scale, put_code, put_scale)
            return carry

        lax.fori_loop(0, PAIR * base, slot, 0)
        for i in range(PAIR * base):
            scale_ref[pair * PAIR + i // base, i % base : i % base + 1, :] = rows[i]

    def sent(pair, final):
        for sub in range(PAIR):

            def leave(mask, carry, sub=sub):
                message(mask, pair, sub, final).wait_send()
                return carry

            lax.fori_loop(1, groups, leave, 0)

    def step(pair, carry):
        @pl.when(pair >= RING)
        def _():
            sent(pair - RING, False)

        for sub in range(PAIR):
            prepare(pair, sub)
            give(2, groups, pair, sub, False)
            give(1, 2, pair, sub, False)
            own(pair, sub, False)

        @pl.when(pair > 0)
        def _():
            take(pair - 1, False)
            unpack(pair - 1)

        return carry

    for ahead in range(1, parts_n):
        length_message(ahead).start()
    end = pairs - 1
    lax.fori_loop(0, end, step, 0)

    if end >= RING:
        sent(end - RING, False)
    for sub in range(PAIR - 1):
        prepare(end, sub)
        give(2, groups, end, sub, True)
        give(1, 2, end, sub, True)
        own(end, sub, True)
    sub = PAIR - 1
    early = max(2, groups * 3 // 4)
    prepare(end, sub)
    pack_list(lambda e: table_smem[layers + 1, e], all_ref.at[me])
    for copy in stage(0):
        list_message(*copy).start()
    give(2, early, end, sub, True)
    give(1, 2, end, sub, True)
    own(end, sub, True)
    take(end - 1, False)
    unpack(end - 1)
    for number in range(1, len(bits)):
        for copy in stage(number - 1):
            list_arrival(*copy).wait_recv()
        for copy in stage(number):
            list_message(*copy).start()
        if number == 1:
            give(early, groups, end, sub, True)

            def second(group, carry):
                for which in range(2):
                    pack_list(
                        lambda e: table_smem[layers, group * layers + which * listed + e], list_ref.at[group, which]
                    )
                return carry

            lax.fori_loop(0, groups, second, 0)
            keep = pltpu.make_async_copy(list_ref, second_ref, second_sem)
            keep.start()
            for ahead in range(1, parts_n):
                length_message(ahead).wait()
                most = jnp.maximum(most, lengths_ref[ahead, 0:1, :])
            longest_ref[0, 0] = jnp.max(most).astype(jnp.int32)

    def edges(layer, carry):
        @pl.when(part < parts_n - 1)
        def _():
            edge(layer, 0).wait_send()

        @pl.when(part > 0)
        def _():
            edge(layer, 1).wait_send()

        return carry

    lax.fori_loop(0, layers, edges, 0)
    keep.wait()
    for copy in stage(len(bits) - 1):
        list_arrival(*copy).wait_recv()
    for number in range(len(bits)):
        for copy in stage(number):
            list_message(*copy).wait_send()

    def drain(pair, carry):
        sent(pair, False)
        return carry

    lax.fori_loop(max(0, end - RING + 1), end, drain, 0)
    sent(end, True)
    take(end, True)


def list_places(group_ref, place_ref, slots, groups, shared):
    layers = group_ref.shape[0]
    me = lax.axis_index("serve")
    count = jnp.sum(jnp.where(group_ref[...] == me, 1, 0), axis=1, keepdims=True)
    ahead = jnp.zeros((layers, 1), jnp.int32)
    every = jnp.where(count == slots, 1, 0)
    if shared:
        every = jnp.zeros((layers, 1), jnp.int32)
        for g in range(groups):
            filled = jnp.sum(jnp.where(group_ref[...] == g, 1, 0), axis=1, keepdims=True)
            one = jnp.where(filled == slots, 1, 0)
            ahead = ahead + jnp.where(g < me, one, 0)
            every = every + one
    length = jnp.zeros((1, 1), jnp.int32)
    for n in range(layers):
        place = jnp.where(count[n : n + 1, :] == slots, length + ahead[n : n + 1, :], layers * groups)
        place_ref[n : n + 1, :] = jnp.broadcast_to(place, (1, place_ref.shape[1]))
        length = length + every[n : n + 1, :]
    return count


def write_kernel(
    dims,
    base,
    group_ref,
    codes_ref,
    scale_ref,
    tail_ref,
    all_ref,
    codes_out,
    scale_out,
    scales,
    codes,
    rows,
    extra,
    extra_scale,
    rem_code,
    rem_scale,
    place_ref,
    place_smem,
    sems,
    extra_sems,
    place_sem,
):
    full, rem, columns, groups = dims
    layers = scale_out.shape[0]
    done = layers - PAIR
    listed = layers // 2
    copies = [pltpu.make_async_copy(codes_ref.at[n], codes_out.at[n, pl.ds(0, base)], sems.at[n]) for n in range(done)]
    for copy in copies:
        copy.start()
    count = list_places(group_ref, place_ref, base + 1, groups, True)
    to_smem = pltpu.make_async_copy(place_ref, place_smem, place_sem)
    to_smem.start()
    extra[layers] = jnp.zeros(extra.shape[1:], extra.dtype)
    scale_rest(dims, PAIR * base, lambda s, n: tail_ref[s, n], rem_code, rem_scale)

    def last_pair(sub):
        def slot(k, carry):
            def put_code(low, high, code):
                codes[sub, k, :, low:high] = code.astype(codes.dtype)

            def put_scale(low, high, scale):
                rows[sub * base + k, :, low:high] = scale

            scale_slot(dims, sub * base + k, lambda s, n: tail_ref[s, n], rem_code, rem_scale, put_code, put_scale)
            return carry

        lax.fori_loop(0, base, slot, 0)
        copies.append(pltpu.make_async_copy(codes.at[sub], codes_out.at[done + sub, pl.ds(0, base)], sems.at[done + sub]))
        copies[-1].start()

    for sub in range(PAIR):
        last_pair(sub)

    def recv(s, n):
        return all_ref[s, n]

    scale_rest(dims, listed, recv, rem_code, rem_scale)
    slot = lax.broadcasted_iota(jnp.int32, scales.shape[1:], 0)
    to_smem.wait()

    def last_slot(layer, carry):
        place = place_smem[layer, 0]
        long = place < layers * groups
        extra_scale[layer] = jnp.zeros(extra_scale.shape[1:], jnp.float32)

        @pl.when(long)
        def _():
            def put_code(low, high, code):
                extra[layer, :, low:high] = code.astype(extra.dtype)

            def put_scale(low, high, scale):
                extra_scale[layer, :, low:high] = scale

            scale_slot(dims, jnp.minimum(place, listed - 1), recv, rem_code, rem_scale, put_code, put_scale)

        pltpu.make_async_copy(
            extra.at[jnp.where(long, layer, layers)], codes_out.at[layer, base], extra_sems.at[layer]
        ).start()
        return carry

    lax.fori_loop(0, layers, last_slot, 0)
    for sub in range(PAIR):
        for k in range(base):
            scales[done + sub, k : k + 1, :] = rows[sub * base + k]
    for n in range(layers):
        scale = scale_ref[n] if n < done else scales[n]
        scale = jnp.where(slot < count[n : n + 1, :], scale, 0.0)
        scales[n] = jnp.where(slot < base, scale, jnp.broadcast_to(extra_scale[n], scale.shape))
    copies.append(pltpu.make_async_copy(scales, scale_out, sems.at[layers]))
    copies[-1].start()
    for n in range(layers):
        copies.append(pltpu.make_async_copy(extra.at[n], codes_out.at[n, base], extra_sems.at[n]))
    for copy in copies:
        copy.wait()


def late_kernel(
    dims,
    base,
    group_ref,
    got_ref,
    codes_in,
    scale_in,
    codes_out,
    scale_out,
    extra,
    extra_scale,
    scales,
    rem_code,
    rem_scale,
    place_ref,
    place_smem,
    sem,
):
    del codes_in, scale_in
    full, rem, columns, groups = dims
    layers = codes_out.shape[0]
    listed = layers // 2
    list_places(group_ref, place_ref, base + 1, groups, False)
    to_smem = pltpu.make_async_copy(place_ref, place_smem, sem)
    to_smem.start()
    to_smem.wait()
    slot = lax.broadcasted_iota(jnp.int32, scales.shape, 0)
    for which in range(2):

        def recv(s, n, which=which):
            return got_ref[s, which, n]

        scale_rest(dims, listed, recv, rem_code, rem_scale)

        def last_slot(layer, carry, which=which, recv=recv):
            place = place_smem[layer, 0] - which * listed

            @pl.when((place >= 0) & (place < listed))
            def _():
                def put_code(low, high, code):
                    extra[:, low:high] = code.astype(extra.dtype)

                def put_scale(low, high, scale):
                    extra_scale[:, low:high] = scale

                scale_slot(dims, place, recv, rem_code, rem_scale, put_code, put_scale)
                pltpu.sync_copy(extra, codes_out.at[layer, base])
                pltpu.sync_copy(scale_out.at[layer], scales)
                scales[...] = jnp.where(slot < base, scales[...], jnp.broadcast_to(extra_scale[...], scales.shape))
                pltpu.sync_copy(scales, scale_out.at[layer])

            return carry

        lax.fori_loop(0, layers, last_slot, 0)


def shards(train_weights, row_offset, block_group):
    train_n = lax.axis_size("train")
    serve_n = lax.axis_size("serve")
    layers, buffer_len, columns = train_weights.shape
    blocks_dev = block_group.shape[1]
    base = (blocks_dev + serve_n - 1) // serve_n
    slots = base + 1
    full = columns // LANES
    rem = columns - full * LANES
    pairs = layers // PAIR
    listed = layers // 2
    pieces = PAIR * base * full + (1 if rem else 0)
    pieces_list = listed * full + (1 if rem else 0)
    rests = max(PAIR * base, listed)
    spots = serve_n * layers
    width = columns * serve_n
    dtype = train_weights.dtype
    dims = (full, rem, columns, serve_n)
    assert SHIFT == BLOCK and buffer_len % BLOCK == 0
    assert rests * rem <= LANES and layers % PAIR == 0 and slots <= layers and pairs > 1

    group_ids = block_group[:, :, 0]
    smem = pl.BlockSpec(memory_space=pltpu.SMEM)
    vmem = pl.BlockSpec(memory_space=pltpu.VMEM)
    anywhere = pl.BlockSpec(memory_space=pl.ANY)
    hbm = pl.BlockSpec(memory_space=pltpu.HBM)
    codes, scales, tail, shared, second, longest = pl.pallas_call(
        functools.partial(move_kernel, dims, base),
        in_specs=[anywhere, anywhere, anywhere],
        out_specs=[vmem, vmem, vmem, vmem, hbm, smem],
        out_shape=[
            pltpu.VMEM((layers - PAIR, base, BLOCK, width), dtype),
            pltpu.VMEM((layers - PAIR, slots, width), jnp.float32),
            pltpu.VMEM((serve_n, pieces, BLOCK, LANES), dtype),
            pltpu.VMEM((serve_n, pieces_list, BLOCK, LANES), dtype),
            jax.ShapeDtypeStruct((serve_n, 2, pieces_list, BLOCK, LANES), dtype),
            jax.ShapeDtypeStruct((1, 1), jnp.int32),
        ],
        scratch_shapes=[
            pltpu.VMEM((serve_n, pairs - 1, pieces, BLOCK, LANES), dtype),
            pltpu.VMEM((serve_n, RING, pieces, BLOCK, LANES), dtype),
            pltpu.VMEM((PAIR, columns, buffer_len), dtype),
            pltpu.VMEM((buffer_len // BLOCK, BLOCK, columns), dtype),
            pltpu.VMEM((serve_n + 1, rests, BLOCK, LANES), dtype),
            pltpu.VMEM((layers, 2, SHIFT, columns), dtype),
            pltpu.VMEM((layers, 2, SHIFT, columns), dtype),
            pltpu.VMEM((serve_n * layers + 1, BLOCK, columns), dtype),
            pltpu.VMEM((serve_n, 2, pieces_list, BLOCK, LANES), dtype),
            pltpu.VMEM((serve_n, BLOCK, LANES), jnp.float32),
            pltpu.VMEM((serve_n, 1, LANES), jnp.float32),
            pltpu.VMEM((PAIR * base, 1, width), jnp.float32),
            pltpu.VMEM((layers + 8, spots), jnp.int32),
            pltpu.SMEM((layers + 8, spots), jnp.int32),
            pltpu.VMEM((8, LANES), jnp.float32),
            pltpu.VMEM((train_n, 8, LANES), jnp.float32),
            pltpu.SMEM((train_n + 1, layers), jnp.int32),
            pltpu.VMEM((layers, blocks_dev), jnp.int32),
            pltpu.SemaphoreType.DMA((PAIR,)),
            pltpu.SemaphoreType.DMA,
            pltpu.SemaphoreType.DMA((2,)),
            pltpu.SemaphoreType.DMA((serve_n, RING, PAIR)),
            pltpu.SemaphoreType.DMA((serve_n, pairs, PAIR)),
            pltpu.SemaphoreType.DMA((layers, 2)),
            pltpu.SemaphoreType.DMA((layers, 2)),
            pltpu.SemaphoreType.DMA((2, serve_n)),
            pltpu.SemaphoreType.DMA((2, serve_n)),
            pltpu.SemaphoreType.DMA((train_n,)),
            pltpu.SemaphoreType.DMA((train_n,)),
            pltpu.SemaphoreType.DMA,
        ],
        compiler_params=pltpu.CompilerParams(
            collective_id=0, has_side_effects=True, vmem_limit_bytes=36 * MIB
        ),
        name="move",
    )(row_offset.T, group_ids, jnp.swapaxes(train_weights, 1, 2))

    codes_shape = jax.ShapeDtypeStruct((layers, slots, BLOCK, width), dtype)
    scales_shape = jax.ShapeDtypeStruct((layers, slots, width), jnp.float32)
    rest_scratch = [
        pltpu.VMEM((serve_n, BLOCK, LANES), jnp.float32),
        pltpu.VMEM((serve_n, 1, LANES), jnp.float32),
        pltpu.VMEM((layers, LANES), jnp.int32),
        pltpu.SMEM((layers, LANES), jnp.int32),
    ]
    codes_out, scales_out = pl.pallas_call(
        functools.partial(write_kernel, dims, base),
        in_specs=[vmem, anywhere, vmem, vmem, vmem],
        out_specs=[hbm, hbm],
        out_shape=[codes_shape, pltpu.HBM((layers, slots, width), jnp.float32)],
        scratch_shapes=[
            pltpu.VMEM((layers, slots, width), jnp.float32),
            pltpu.VMEM((PAIR, base, BLOCK, width), dtype),
            pltpu.VMEM((PAIR * base, 1, width), jnp.float32),
            pltpu.VMEM((layers + 1, BLOCK, width), dtype),
            pltpu.VMEM((layers, 1, width), jnp.float32),
            *rest_scratch,
            pltpu.SemaphoreType.DMA((layers + 1,)),
            pltpu.SemaphoreType.DMA((layers,)),
            pltpu.SemaphoreType.DMA,
        ],
        compiler_params=pltpu.CompilerParams(vmem_limit_bytes=10 * MIB),
        name="write",
    )(group_ids, codes, scales, tail, shared)

    def late(state):
        got = lax.all_to_all(second, "serve", split_axis=0, concat_axis=0, tiled=True)
        late_codes, late_scales = pl.pallas_call(
            functools.partial(late_kernel, dims, base),
            in_specs=[vmem, vmem, hbm, hbm],
            out_specs=[hbm, hbm],
            out_shape=[codes_shape, scales_shape],
            input_output_aliases={2: 0, 3: 1},
            scratch_shapes=[
                pltpu.VMEM((BLOCK, width), dtype),
                pltpu.VMEM((1, width), jnp.float32),
                pltpu.VMEM((slots, width), jnp.float32),
                *rest_scratch,
                pltpu.SemaphoreType.DMA,
            ],
            compiler_params=pltpu.CompilerParams(vmem_limit_bytes=6 * MIB),
            name="late",
        )(group_ids, got, state[1], state[2])
        return jnp.zeros((), jnp.int32), late_codes, late_scales

    state = (longest[0, 0], codes_out, scales_out)
    _, codes_out, scales_out = lax.while_loop(lambda now: now[0] > listed, late, state)
    return (
        codes_out.reshape(layers, 1, 1, slots, BLOCK, width),
        scales_out.reshape(layers, 1, 1, slots, width),
    )


def solution(mesh):
    return jax.shard_map(
        shards,
        mesh=mesh,
        in_specs=(P(None, "train", "serve"), P(), P(None, "train", None)),
        out_specs=(
            P(None, "serve", "train", None, None, None),
            P(None, "serve", "train", None, None),
        ),
        check_vma=False,
    )
```

```python
import functools

import jax
import jax.numpy as jnp
from jax import lax
from jax.experimental import pallas as pl
from jax.experimental.pallas import tpu as pltpu
from jax.sharding import PartitionSpec as P

BLOCK = 32
SHIFT = 32
LANES = 128
PAIR = 2
RING = 3
TURNS = 4
MESH = pl.DeviceIdType.MESH
MIB = 1024 * 1024


def turned(values):
    return jnp.transpose(values.astype(jnp.float32))


def partner(me, mask, count):
    out, bit = 0, 1
    while bit < count:
        out = out + ((me // bit + mask // bit) % 2) * bit
        bit *= 2
    return out


def scaled(values):
    values = values.astype(jnp.float32)
    divisor = jnp.maximum(jnp.max(jnp.abs(values), axis=0, keepdims=True), 0.25)
    return values * (1.0 / divisor), divisor


def scale_rest(dims, count, recv, rem_code, rem_scale):
    full, rem, columns, sources = dims
    if rem:
        for s in range(sources):
            rem_code[s], rem_scale[s] = scaled(recv(s, count * full))


def scale_slot(dims, i, recv, rem_code, rem_scale, put_code, put_scale):
    full, rem, columns, sources = dims
    width = columns * sources
    tiles = -(-width // LANES)
    lane = lax.broadcasted_iota(jnp.int32, (BLOCK, LANES), 1)
    lane_row = lax.broadcasted_iota(jnp.int32, (1, LANES), 1)
    parts = [None] * tiles

    def put(tile, low, code, scale):
        if tile >= tiles:
            return
        if parts[tile] is None:
            parts[tile] = (code, scale)
        else:
            before = parts[tile]
            parts[tile] = (jnp.where(lane >= low, code, before[0]), jnp.where(lane_row >= low, scale, before[1]))

    def flush(below):
        for tile in range(below):
            if parts[tile] is not None:
                code, scale = parts[tile]
                end = min(width, (tile + 1) * LANES)
                size = end - tile * LANES
                put_code(tile * LANES, end, code[:, :size])
                put_scale(tile * LANES, end, scale[:, :size])
                parts[tile] = None

    for s in range(sources):
        for t in range(full + (1 if rem else 0)):
            start = s * columns + t * LANES
            size = LANES if t < full else rem
            low = start % LANES
            if t < full:
                code, scale = scaled(recv(s, i * full + t))
                if low:
                    code, scale = pltpu.roll(code, low, 1), pltpu.roll(scale, low, 1)
            else:
                turn = lax.rem(low + LANES - i * rem, LANES)
                code, scale = pltpu.roll(rem_code[s], turn, 1), pltpu.roll(rem_scale[s], turn, 1)
            tile = start // LANES
            put(tile, low, code, scale)
            if low + size > LANES:
                put(tile + 1, 0, code, scale)
            flush((start + size) // LANES)
    flush(tiles)


def move_kernel(
    dims,
    base,
    offset_hbm,
    group_hbm,
    wt_ref,
    codes_ref,
    scale_ref,
    tail_ref,
    shared_codes,
    shared_scale,
    second_ref,
    longest_ref,
    all_ref,
    recv_ref,
    send_ref,
    in_ref,
    w_ref,
    rem_ref,
    edge_ref,
    halo_ref,
    over_ref,
    list_ref,
    rem_code,
    rem_scale,
    rows,
    table_ref,
    table_smem,
    length_ref,
    lengths_ref,
    offset_ref,
    group_ref,
    in_sem,
    table_sem,
    small_sem,
    send_sem,
    recv_sem,
    halo_send,
    halo_recv,
    list_send,
    list_recv,
    length_send,
    length_recv,
    second_sem,
):
    full, rem, columns, groups = dims
    slots = base + 1
    pairs = recv_ref.shape[1] + 1
    layers = pairs * PAIR
    listed = layers // 2
    blocks = w_ref.shape[0]
    buffer_len = blocks * BLOCK
    rows_dev = buffer_len - 2 * SHIFT
    me = lax.axis_index("serve")
    part = lax.axis_index("train")
    parts_n = lax.axis_size("train")
    half = base * full
    rest = half + (1 if rem else 0)

    def fetch(layer, sub):
        return pltpu.make_async_copy(wt_ref.at[layer], in_ref.at[sub], in_sem.at[sub])

    def message(mask, pair, sub, final):
        peer = partner(me, mask, groups)
        span = pl.ds(sub * half, rest if sub == PAIR - 1 else half)
        return pltpu.make_async_remote_copy(
            send_ref.at[peer, pair % RING, span],
            tail_ref.at[me, span] if final else recv_ref.at[me, pair, span],
            send_sem.at[mask, pair % RING, sub],
            recv_sem.at[mask, pair % TURNS, sub],
            device_id={"serve": peer},
            device_id_type=MESH,
        )

    def arrival(mask, pair, sub, final):
        peer = partner(me, mask, groups)
        span = pl.ds(sub * half, rest if sub == PAIR - 1 else half)
        place = tail_ref.at[peer, span] if final else recv_ref.at[peer, pair, span]
        return pltpu.make_async_remote_copy(
            place,
            place,
            send_sem.at[mask, pair % RING, sub],
            recv_sem.at[mask, pair % TURNS, sub],
            device_id={"serve": peer},
            device_id_type=MESH,
        )

    bits = [1 << n for n in range(groups.bit_length() - 1)]
    orders = [bits[1:], bits[:0:-1]]
    pieces_list = all_ref.shape[1]
    spans = [pl.ds(0, pieces_list // 2), pl.ds(pieces_list // 2, pieces_list - pieces_list // 2)]

    def stage(number):
        for which, order in enumerate(orders):
            if number < 0:
                yield which, 0, 0
                continue
            held = [0]
            for bit in order[:number]:
                held = held + [mask + bit for mask in held]
            for mask in held:
                yield which, order[number], mask

    def list_message(which, bit, mask):
        place = all_ref.at[partner(me, mask, groups), spans[which]]
        return pltpu.make_async_remote_copy(
            place,
            place,
            list_send.at[which, bit + mask],
            list_recv.at[which, bit + mask],
            device_id={"serve": partner(me, bit, groups)},
            device_id_type=MESH,
        )

    def list_arrival(which, bit, mask):
        place = all_ref.at[partner(me, bit + mask, groups), spans[which]]
        return pltpu.make_async_remote_copy(
            place,
            place,
            list_send.at[which, bit + mask],
            list_recv.at[which, bit + mask],
            device_id={"serve": partner(me, bit, groups)},
            device_id_type=MESH,
        )

    def edge(layer, side):
        to = part + 1 if side == 0 else part - 1
        return pltpu.make_async_remote_copy(
            edge_ref.at[layer, side],
            halo_ref.at[layer, side],
            halo_send.at[layer % 2, side],
            halo_recv.at[layer % 2, side],
            device_id={"train": to},
            device_id_type=MESH,
        )

    def length_message(ahead):
        return pltpu.make_async_remote_copy(
            length_ref,
            lengths_ref.at[ahead],
            length_send.at[ahead],
            length_recv.at[ahead],
            device_id={"train": (part + ahead) % parts_n},
            device_id_type=MESH,
        )

    get_group = pltpu.make_async_copy(group_hbm, group_ref, small_sem.at[0])
    get_group.start()
    fetch(0, 0).start()
    get_offset = pltpu.make_async_copy(offset_hbm, offset_ref, small_sem.at[1])
    get_offset.start()
    for sub in range(1, PAIR):
        fetch(sub, sub).start()

    barrier = pltpu.get_barrier_semaphore()

    def greet(mask, carry):
        pl.semaphore_signal(barrier, inc=1, device_id={"serve": partner(me, mask, groups)}, device_id_type=MESH)
        return carry

    lax.fori_loop(1, groups, greet, 0)
    for ahead in range(1, parts_n):
        pl.semaphore_signal(barrier, inc=1, device_id={"train": (part + ahead) % parts_n}, device_id_type=MESH)

    row = lax.broadcasted_iota(jnp.int32, (BLOCK, columns), 0)
    lane = lax.broadcasted_iota(jnp.int32, (BLOCK, LANES), 1)
    last = rows_dev - BLOCK

    def transpose_tile(sub, low):
        high = min(low + LANES, buffer_len)
        rows_of = turned(in_ref[sub, :, low:high]).astype(w_ref.dtype)
        w_ref[low // BLOCK : high // BLOCK] = rows_of.reshape((high - low) // BLOCK, BLOCK, columns)

    def joined(group, count):
        tile = rem_ref[group, 0].astype(jnp.float32)
        for i in range(1, count):
            moved = pltpu.roll(rem_ref[group, i].astype(jnp.float32), i * rem, 1)
            tile = jnp.where(lane >= i * rem, moved, tile)
        return tile

    def edge_ends(layer, act):
        @pl.when(part < parts_n - 1)
        def _():
            act(edge(layer, 0))

        @pl.when(part > 0)
        def _():
            act(edge(layer, 1))

    def send_edges(layer, sub):
        fetch(layer, sub).wait()
        low = (buffer_len - 1) // LANES * LANES
        edge_ref[layer, 0] = turned(in_ref[sub, :, low:buffer_len])[-SHIFT:].astype(edge_ref.dtype)
        edge_ref[layer, 1] = turned(in_ref[sub, :, 0:LANES])[:SHIFT].astype(edge_ref.dtype)

        @pl.when(layer >= 2)
        def _():
            edge_ends(layer - 2, lambda copy: copy.wait_send())

        edge_ends(layer, lambda copy: copy.start())

    def prepare(pair, sub):
        layer = pair * PAIR + sub
        for low in range(0, buffer_len, LANES):
            transpose_tile(sub, low)

        @pl.when(layer + PAIR < layers)
        def _():
            fetch(layer + PAIR, sub).start()

        base_row = part * rows_dev

        @pl.when(part > 0)
        def _():
            edge(layer, 0).wait_recv()
            first = offset_ref[part, layer] - base_row
            head = jnp.where(row < first, halo_ref[layer, 0].astype(jnp.float32), w_ref[1].astype(jnp.float32))
            w_ref[1] = head.astype(w_ref.dtype)

        @pl.when(part < parts_n - 1)
        def _():
            edge(layer, 1).wait_recv()
            after = offset_ref[part + 1, layer] - base_row
            tail = w_ref[blocks - 2].astype(jnp.float32)
            tail = jnp.where(row + last >= after, halo_ref[layer, 1].astype(jnp.float32), tail)
            w_ref[blocks - 2] = tail.astype(w_ref.dtype)

        w_ref[0] = jnp.zeros((BLOCK, columns), w_ref.dtype)
        if sub == 0:

            @pl.when(pair == 0)
            def _():
                to_smem.wait()

        def last_slots(group, carry):
            over_ref[layer * groups + group] = w_ref[table_smem[layer, group * layers + base]]
            return carry

        lax.fori_loop(0, groups, last_slots, 0)

    def gather(pair, sub, group, out):
        for k in range(base):
            block = w_ref[table_smem[pair * PAIR + sub, group * layers + k]]
            for t in range(full):
                out[(sub * base + k) * full + t] = block[:, t * LANES : (t + 1) * LANES]
            if rem:
                rem_ref[group, sub * base + k, :, 0:rem] = block[:, full * LANES :]
        if rem and sub == PAIR - 1:
            out[PAIR * half] = joined(group, PAIR * base).astype(out.dtype)

    def give(low, high, pair, sub, final):
        def one(mask, carry):
            peer = partner(me, mask, groups)
            gather(pair, sub, peer, send_ref.at[peer, pair % RING])
            message(mask, pair, sub, final).start()
            return carry

        lax.fori_loop(low, high, one, 0)

    def own(pair, sub, final):
        gather(pair, sub, me, tail_ref.at[me] if final else recv_ref.at[me, pair])

    def pack_list(entry_of, out):
        for e in range(listed):
            block = over_ref[entry_of(e)]
            for t in range(full):
                out[e * full + t] = block[:, t * LANES : (t + 1) * LANES]
            if rem:
                rem_ref[groups, e, :, 0:rem] = block[:, full * LANES :]
        if rem:
            out[listed * full] = joined(groups, listed).astype(out.dtype)

    def take(pair, final):
        for sub in range(PAIR):

            def arrive(mask, carry, sub=sub):
                arrival(mask, pair, sub, final).wait_recv()
                return carry

            lax.fori_loop(1, groups, arrive, 0)

    def unpack(pair):
        def recv(s, n):
            return recv_ref[s, pair, n]

        scale_rest(dims, PAIR * base, recv, rem_code, rem_scale)

        def slot(i, carry):
            def put_code(low, high, code):
                codes_ref[pair * PAIR + i // base, i % base, :, low:high] = code.astype(codes_ref.dtype)

            def put_scale(low, high, scale):
                rows[i, :, low:high] = scale

            scale_slot(dims, i, recv, rem_code, rem_scale, put_code, put_scale)
            return carry

        lax.fori_loop(0, PAIR * base, slot, 0)
        for i in range(PAIR * base):
            scale_ref[pair * PAIR + i // base, i % base : i % base + 1, :] = rows[i]

    def sent(pair, final):
        for sub in range(PAIR):

            def leave(mask, carry, sub=sub):
                message(mask, pair, sub, final).wait_send()
                return carry

            lax.fori_loop(1, groups, leave, 0)

    def step(pair, carry):
        @pl.when(pair >= RING)
        def _():
            sent(pair - RING, False)

        for sub in range(PAIR):
            prepare(pair, sub)
            give(2, groups, pair, sub, False)
            give(1, 2, pair, sub, False)
            own(pair, sub, False)
            send_edges(pair * PAIR + sub + 1, (sub + 1) % PAIR)

        @pl.when(pair > 0)
        def _():
            take(pair - 1, False)
            unpack(pair - 1)

        return carry

    pl.semaphore_wait(barrier, groups - 1 + parts_n - 1)
    send_edges(0, 0)
    get_offset.wait()
    get_group.wait()
    spot = lax.broadcasted_iota(jnp.int32, (layers, groups * layers), 1)
    spot_group = jnp.zeros(spot.shape, jnp.int32)
    for g in range(1, groups):
        spot_group = spot_group + jnp.where(spot >= g * layers, 1, 0)
    spot_slot = spot - spot_group * layers
    seen = jnp.zeros(spot.shape, jnp.int32)
    table = jnp.zeros(spot.shape, jnp.int32)
    for j in range(group_ref.shape[1]):
        mine = group_ref[:, j : j + 1] == spot_group
        table = jnp.where(mine & (seen == spot_slot), j + 1, table)
        seen = jnp.where(mine, seen + 1, seen)
    table_ref[0:layers, :] = table
    none = layers * groups
    length = jnp.zeros((1, groups * layers), jnp.int32)
    entry = jnp.full(length.shape, none, jnp.int32)
    total = jnp.zeros((1, LANES), jnp.int32)
    shared = jnp.full(total.shape, none, jnp.int32)
    number = lax.broadcasted_iota(jnp.int32, total.shape, 1)
    long = jnp.where(seen == slots, 1, 0)
    for n in range(layers):
        here = long[n : n + 1, :]
        entry = jnp.where((here > 0) & (length == spot_slot[0:1, :]), n * groups + spot_group[0:1, :], entry)
        length = length + here
        for g in range(groups):
            one = jnp.broadcast_to(here[:, g * layers : g * layers + 1], total.shape)
            shared = jnp.where((one > 0) & (total == number), n * groups + g, shared)
            total = total + one
    table_ref[layers : layers + 1, :] = entry
    table_ref[layers + 1 : layers + 2, 0:LANES] = shared
    to_smem = pltpu.make_async_copy(table_ref, table_smem, table_sem)
    to_smem.start()
    most = total.astype(jnp.float32)
    length_ref[...] = jnp.broadcast_to(most, length_ref.shape)
    over_ref[none] = jnp.zeros((BLOCK, columns), over_ref.dtype)

    for ahead in range(1, parts_n):
        length_message(ahead).start()
    end = pairs - 1
    lax.fori_loop(0, end, step, 0)

    if end >= RING:
        sent(end - RING, False)
    for sub in range(PAIR - 1):
        prepare(end, sub)
        give(2, groups, end, sub, True)
        give(1, 2, end, sub, True)
        own(end, sub, True)
        send_edges(end * PAIR + sub + 1, sub + 1)
    sub = PAIR - 1
    direct = max(2, groups * 3 // 4)
    prepare(end, sub)
    pack_list(lambda e: table_smem[layers + 1, e], all_ref.at[me])
    for copy in stage(0):
        list_message(*copy).start()
    for which in range(2):
        list_message(which, 1, 0).start()
    give(direct, groups, end, sub, True)
    give(1, 2, end, sub, True)
    own(end, sub, True)

    def second(group, carry):
        for which in range(2):
            pack_list(lambda e: table_smem[layers, group * layers + which * listed + e], list_ref.at[group, which])
        return carry

    lax.fori_loop(0, groups, second, 0)
    keep = pltpu.make_async_copy(list_ref, second_ref, second_sem)
    keep.start()
    for ahead in range(1, parts_n):
        length_message(ahead).wait()
        most = jnp.maximum(most, lengths_ref[ahead, 0:1, :])
    longest_ref[0, 0] = jnp.max(most).astype(jnp.int32)
    for n in range(2):
        edge_ends(layers - 1 - n, lambda copy: copy.wait_send())

    take(end - 1, False)
    unpack(end - 1)
    high = len(bits) - 1
    for number in range(1, high + 1):
        for copy in stage(number - 1):
            list_arrival(*copy).wait_recv()
        if number < high:
            for copy in stage(number):
                list_message(*copy).start()
        for which, bit, mask in stage(number - 1):
            list_message(which, 1, bit + mask).start()
        if number == 1:
            give(2, direct, end, sub, True)
    if high < 1:
        give(2, direct, end, sub, True)
    for which, bit, mask in [copy for number in range(-1, high) for copy in stage(number)]:
        list_arrival(which, 1, bit + mask).wait_recv()

    def recv(s, n):
        return all_ref[s, n]

    scale_rest(dims, listed, recv, rem_code, rem_scale)

    def listed_slot(e, carry):
        def put_code(low, high, code):
            shared_codes[e, :, low:high] = code.astype(shared_codes.dtype)

        def put_scale(low, high, scale):
            shared_scale[e, :, low:high] = scale

        scale_slot(dims, e, recv, rem_code, rem_scale, put_code, put_scale)
        return carry

    lax.fori_loop(0, listed, listed_slot, 0)
    shared_codes[listed] = jnp.zeros(shared_codes.shape[1:], shared_codes.dtype)
    shared_scale[listed] = jnp.zeros(shared_scale.shape[1:], jnp.float32)

    keep.wait()
    for which, bit, mask in [copy for number in range(-1, high) for copy in stage(number)]:
        list_message(which, 1, bit + mask).wait_send()
    for number in range(high):
        for copy in stage(number):
            list_message(*copy).wait_send()

    def drain(pair, carry):
        sent(pair, False)
        return carry

    lax.fori_loop(max(0, end - RING + 1), end, drain, 0)
    sent(end, True)
    take(end, True)


def list_places(group_ref, place_ref, slots, groups, shared):
    layers = group_ref.shape[0]
    me = lax.axis_index("serve")
    count = jnp.sum(jnp.where(group_ref[...] == me, 1, 0), axis=1, keepdims=True)
    ahead = jnp.zeros((layers, 1), jnp.int32)
    every = jnp.where(count == slots, 1, 0)
    if shared:
        every = jnp.zeros((layers, 1), jnp.int32)
        for g in range(groups):
            filled = jnp.sum(jnp.where(group_ref[...] == g, 1, 0), axis=1, keepdims=True)
            one = jnp.where(filled == slots, 1, 0)
            ahead = ahead + jnp.where(g < me, one, 0)
            every = every + one
    length = jnp.zeros((1, 1), jnp.int32)
    for n in range(layers):
        place = jnp.where(count[n : n + 1, :] == slots, length + ahead[n : n + 1, :], layers * groups)
        place_ref[n : n + 1, :] = jnp.broadcast_to(place, (1, place_ref.shape[1]))
        length = length + every[n : n + 1, :]
    return count


def write_kernel(
    dims,
    base,
    group_ref,
    codes_ref,
    scale_ref,
    tail_ref,
    shared_codes,
    shared_scale,
    codes_out,
    scale_out,
    scales,
    codes,
    rows,
    rem_code,
    rem_scale,
    place_ref,
    place_smem,
    sems,
    last_sems,
    place_sem,
):
    groups = dims[3]
    layers = scale_out.shape[0]
    done = layers - PAIR
    listed = layers // 2
    copies = [pltpu.make_async_copy(codes_ref.at[n], codes_out.at[n, pl.ds(0, base)], sems.at[n]) for n in range(done)]
    for copy in copies:
        copy.start()
    count = list_places(group_ref, place_ref, base + 1, groups, True)
    to_smem = pltpu.make_async_copy(place_ref, place_smem, place_sem)
    to_smem.start()

    def recv(s, n):
        return tail_ref[s, n]

    scale_rest(dims, PAIR * base, recv, rem_code, rem_scale)

    def last_pair(sub):
        def slot(k, carry):
            def put_code(low, high, code):
                codes[sub, k, :, low:high] = code.astype(codes.dtype)

            def put_scale(low, high, scale):
                rows[sub * base + k, :, low:high] = scale

            scale_slot(dims, sub * base + k, recv, rem_code, rem_scale, put_code, put_scale)
            return carry

        lax.fori_loop(0, base, slot, 0)
        copies.append(pltpu.make_async_copy(codes.at[sub], codes_out.at[done + sub, pl.ds(0, base)], sems.at[done + sub]))
        copies[-1].start()

    last_pair(0)
    to_smem.wait()
    places = [jnp.minimum(place_smem[n, 0], listed) for n in range(layers)]
    for n in range(layers):
        copies.append(pltpu.make_async_copy(shared_codes.at[places[n]], codes_out.at[n, base], last_sems.at[n]))
        copies[-1].start()
    for sub in range(1, PAIR):
        last_pair(sub)
    slot = lax.broadcasted_iota(jnp.int32, scales.shape[1:], 0)
    for sub in range(PAIR):
        for k in range(base):
            scales[done + sub, k : k + 1, :] = rows[sub * base + k]
    for n in range(layers):
        scale = scale_ref[n] if n < done else scales[n]
        scale = jnp.where(slot < count[n : n + 1, :], scale, 0.0)
        scales[n] = jnp.where(slot < base, scale, jnp.broadcast_to(shared_scale[places[n]], scale.shape))
    copies.append(pltpu.make_async_copy(scales, scale_out, sems.at[layers]))
    copies[-1].start()
    for copy in copies:
        copy.wait()


def late_kernel(
    dims,
    base,
    group_ref,
    got_ref,
    codes_in,
    scale_in,
    codes_out,
    scale_out,
    extra,
    extra_scale,
    scales,
    rem_code,
    rem_scale,
    place_ref,
    place_smem,
    sem,
):
    del codes_in, scale_in
    full, rem, columns, groups = dims
    layers = codes_out.shape[0]
    listed = layers // 2
    list_places(group_ref, place_ref, base + 1, groups, False)
    to_smem = pltpu.make_async_copy(place_ref, place_smem, sem)
    to_smem.start()
    to_smem.wait()
    slot = lax.broadcasted_iota(jnp.int32, scales.shape, 0)
    for which in range(2):

        def recv(s, n, which=which):
            return got_ref[s, which, n]

        scale_rest(dims, listed, recv, rem_code, rem_scale)

        def last_slot(layer, carry, which=which, recv=recv):
            place = place_smem[layer, 0] - which * listed

            @pl.when((place >= 0) & (place < listed))
            def _():
                def put_code(low, high, code):
                    extra[:, low:high] = code.astype(extra.dtype)

                def put_scale(low, high, scale):
                    extra_scale[:, low:high] = scale

                scale_slot(dims, place, recv, rem_code, rem_scale, put_code, put_scale)
                pltpu.sync_copy(extra, codes_out.at[layer, base])
                pltpu.sync_copy(scale_out.at[layer], scales)
                scales[...] = jnp.where(slot < base, scales[...], jnp.broadcast_to(extra_scale[...], scales.shape))
                pltpu.sync_copy(scales, scale_out.at[layer])

            return carry

        lax.fori_loop(0, layers, last_slot, 0)


def shards(train_weights, row_offset, block_group):
    train_n = lax.axis_size("train")
    serve_n = lax.axis_size("serve")
    layers, buffer_len, columns = train_weights.shape
    blocks_dev = block_group.shape[1]
    base = (blocks_dev + serve_n - 1) // serve_n
    slots = base + 1
    full = columns // LANES
    rem = columns - full * LANES
    pairs = layers // PAIR
    listed = layers // 2
    pieces = PAIR * base * full + (1 if rem else 0)
    pieces_list = listed * full + (1 if rem else 0)
    rests = max(PAIR * base, listed)
    spots = serve_n * layers
    width = columns * serve_n
    dtype = train_weights.dtype
    dims = (full, rem, columns, serve_n)
    assert SHIFT == BLOCK and buffer_len % BLOCK == 0
    assert rests * rem <= LANES and layers % PAIR == 0 and slots <= layers and pairs > 1

    group_ids = block_group[:, :, 0]
    smem = pl.BlockSpec(memory_space=pltpu.SMEM)
    vmem = pl.BlockSpec(memory_space=pltpu.VMEM)
    anywhere = pl.BlockSpec(memory_space=pl.ANY)
    hbm = pl.BlockSpec(memory_space=pltpu.HBM)
    codes, scales, tail, shared_codes, shared_scale, second, longest = pl.pallas_call(
        functools.partial(move_kernel, dims, base),
        in_specs=[hbm, hbm, hbm],
        out_specs=[vmem, vmem, vmem, vmem, vmem, hbm, smem],
        out_shape=[
            pltpu.VMEM((layers - PAIR, base, BLOCK, width), dtype),
            pltpu.VMEM((layers - PAIR, slots, width), jnp.float32),
            pltpu.VMEM((serve_n, pieces, BLOCK, LANES), dtype),
            pltpu.VMEM((listed + 1, BLOCK, width), dtype),
            pltpu.VMEM((listed + 1, 1, width), jnp.float32),
            jax.ShapeDtypeStruct((serve_n, 2, pieces_list, BLOCK, LANES), dtype),
            jax.ShapeDtypeStruct((1, 1), jnp.int32),
        ],
        scratch_shapes=[
            pltpu.VMEM((serve_n, pieces_list, BLOCK, LANES), dtype),
            pltpu.VMEM((serve_n, pairs - 1, pieces, BLOCK, LANES), dtype),
            pltpu.VMEM((serve_n, RING, pieces, BLOCK, LANES), dtype),
            pltpu.VMEM((PAIR, columns, buffer_len), dtype),
            pltpu.VMEM((buffer_len // BLOCK, BLOCK, columns), dtype),
            pltpu.VMEM((serve_n + 1, rests, BLOCK, LANES), dtype),
            pltpu.VMEM((layers, 2, SHIFT, columns), dtype),
            pltpu.VMEM((layers, 2, SHIFT, columns), dtype),
            pltpu.VMEM((serve_n * layers + 1, BLOCK, columns), dtype),
            pltpu.VMEM((serve_n, 2, pieces_list, BLOCK, LANES), dtype),
            pltpu.VMEM((serve_n, BLOCK, LANES), jnp.float32),
            pltpu.VMEM((serve_n, 1, LANES), jnp.float32),
            pltpu.VMEM((PAIR * base, 1, width), jnp.float32),
            pltpu.VMEM((layers + 8, spots), jnp.int32),
            pltpu.SMEM((layers + 8, spots), jnp.int32),
            pltpu.VMEM((8, LANES), jnp.float32),
            pltpu.VMEM((train_n, 8, LANES), jnp.float32),
            pltpu.SMEM((train_n + 1, layers), jnp.int32),
            pltpu.VMEM((layers, blocks_dev), jnp.int32),
            pltpu.SemaphoreType.DMA((PAIR,)),
            pltpu.SemaphoreType.DMA,
            pltpu.SemaphoreType.DMA((2,)),
            pltpu.SemaphoreType.DMA((serve_n, RING, PAIR)),
            pltpu.SemaphoreType.DMA((serve_n, TURNS, PAIR)),
            pltpu.SemaphoreType.DMA((2, 2)),
            pltpu.SemaphoreType.DMA((2, 2)),
            pltpu.SemaphoreType.DMA((2, serve_n)),
            pltpu.SemaphoreType.DMA((2, serve_n)),
            pltpu.SemaphoreType.DMA((train_n,)),
            pltpu.SemaphoreType.DMA((train_n,)),
            pltpu.SemaphoreType.DMA,
        ],
        compiler_params=pltpu.CompilerParams(
            collective_id=0, has_side_effects=True, vmem_limit_bytes=36 * MIB
        ),
        name="move",
    )(row_offset.T, group_ids, jnp.swapaxes(train_weights, 1, 2))

    codes_shape = jax.ShapeDtypeStruct((layers, slots, BLOCK, width), dtype)
    scales_shape = jax.ShapeDtypeStruct((layers, slots, width), jnp.float32)
    rest_scratch = [
        pltpu.VMEM((serve_n, BLOCK, LANES), jnp.float32),
        pltpu.VMEM((serve_n, 1, LANES), jnp.float32),
        pltpu.VMEM((layers, LANES), jnp.int32),
        pltpu.SMEM((layers, LANES), jnp.int32),
    ]
    codes_out, scales_out = pl.pallas_call(
        functools.partial(write_kernel, dims, base),
        in_specs=[vmem, anywhere, vmem, vmem, vmem, vmem],
        out_specs=[hbm, hbm],
        out_shape=[codes_shape, pltpu.HBM((layers, slots, width), jnp.float32)],
        scratch_shapes=[
            pltpu.VMEM((layers, slots, width), jnp.float32),
            pltpu.VMEM((PAIR, base, BLOCK, width), dtype),
            pltpu.VMEM((PAIR * base, 1, width), jnp.float32),
            *rest_scratch,
            pltpu.SemaphoreType.DMA((layers + 1,)),
            pltpu.SemaphoreType.DMA((layers,)),
            pltpu.SemaphoreType.DMA,
        ],
        compiler_params=pltpu.CompilerParams(vmem_limit_bytes=10 * MIB),
        name="write",
    )(group_ids, codes, scales, tail, shared_codes, shared_scale)

    def late(state):
        got = lax.all_to_all(second, "serve", split_axis=0, concat_axis=0, tiled=True)
        late_codes, late_scales = pl.pallas_call(
            functools.partial(late_kernel, dims, base),
            in_specs=[vmem, vmem, hbm, hbm],
            out_specs=[hbm, hbm],
            out_shape=[codes_shape, scales_shape],
            input_output_aliases={2: 0, 3: 1},
            scratch_shapes=[
                pltpu.VMEM((BLOCK, width), dtype),
                pltpu.VMEM((1, width), jnp.float32),
                pltpu.VMEM((slots, width), jnp.float32),
                *rest_scratch,
                pltpu.SemaphoreType.DMA,
            ],
            compiler_params=pltpu.CompilerParams(vmem_limit_bytes=6 * MIB),
            name="late",
        )(group_ids, got, state[1], state[2])
        return jnp.zeros((), jnp.int32), late_codes, late_scales

    state = (longest[0, 0], codes_out, scales_out)
    _, codes_out, scales_out = lax.while_loop(lambda now: now[0] > listed, late, state)
    return (
        codes_out.reshape(layers, 1, 1, slots, BLOCK, width),
        scales_out.reshape(layers, 1, 1, slots, width),
    )


def solution(mesh):
    return jax.shard_map(
        shards,
        mesh=mesh,
        in_specs=(P(None, "train", "serve"), P(), P(None, "train", None)),
        out_specs=(
            P(None, "serve", "train", None, None, None),
            P(None, "serve", "train", None, None),
        ),
        check_vma=False,
    )
```

```python
import functools

import jax
import jax.numpy as jnp
from jax import lax
from jax.experimental import pallas as pl
from jax.experimental.pallas import tpu as pltpu
from jax.sharding import PartitionSpec as P

BLOCK = 32
SHIFT = 32
LANES = 128
PAIR = 2
RING = 3
TURNS = 4
MESH = pl.DeviceIdType.MESH
MIB = 1024 * 1024


def turned(values):
    return jnp.transpose(values.astype(jnp.float32))


def partner(me, mask, count):
    out, bit = 0, 1
    while bit < count:
        out = out + ((me // bit + mask // bit) % 2) * bit
        bit *= 2
    return out


def scaled(values):
    values = values.astype(jnp.float32)
    divisor = jnp.maximum(jnp.max(jnp.abs(values), axis=0, keepdims=True), 0.25)
    return values * (1.0 / divisor), divisor


def scale_rest(dims, count, recv, rem_code, rem_scale):
    full, rem, columns, sources = dims
    if rem:
        for s in range(sources):
            rem_code[s], rem_scale[s] = scaled(recv(s, count * full))


def scale_slot(dims, i, recv, rem_code, rem_scale, put_code, put_scale):
    full, rem, columns, sources = dims
    width = columns * sources
    tiles = -(-width // LANES)
    lane = lax.broadcasted_iota(jnp.int32, (BLOCK, LANES), 1)
    lane_row = lax.broadcasted_iota(jnp.int32, (1, LANES), 1)
    parts = [None] * tiles

    def put(tile, low, code, scale):
        if tile >= tiles:
            return
        if parts[tile] is None:
            parts[tile] = (code, scale)
        else:
            before = parts[tile]
            parts[tile] = (jnp.where(lane >= low, code, before[0]), jnp.where(lane_row >= low, scale, before[1]))

    def flush(below):
        for tile in range(below):
            if parts[tile] is not None:
                code, scale = parts[tile]
                end = min(width, (tile + 1) * LANES)
                size = end - tile * LANES
                put_code(tile * LANES, end, code[:, :size])
                put_scale(tile * LANES, end, scale[:, :size])
                parts[tile] = None

    for s in range(sources):
        for t in range(full + (1 if rem else 0)):
            start = s * columns + t * LANES
            size = LANES if t < full else rem
            low = start % LANES
            if t < full:
                code, scale = scaled(recv(s, i * full + t))
                if low:
                    code, scale = pltpu.roll(code, low, 1), pltpu.roll(scale, low, 1)
            else:
                turn = lax.rem(low + LANES - i * rem, LANES)
                code, scale = pltpu.roll(rem_code[s], turn, 1), pltpu.roll(rem_scale[s], turn, 1)
            tile = start // LANES
            put(tile, low, code, scale)
            if low + size > LANES:
                put(tile + 1, 0, code, scale)
            flush((start + size) // LANES)
    flush(tiles)


def move_kernel(
    dims,
    base,
    offset_hbm,
    group_hbm,
    wt_ref,
    codes_ref,
    scale_ref,
    tail_ref,
    shared_codes,
    shared_scale,
    second_ref,
    longest_ref,
    all_ref,
    recv_ref,
    send_ref,
    in_ref,
    w_ref,
    rem_ref,
    edge_ref,
    halo_ref,
    over_ref,
    list_ref,
    rem_code,
    rem_scale,
    rows,
    table_ref,
    table_smem,
    length_ref,
    lengths_ref,
    longest_smem,
    offset_ref,
    group_ref,
    in_sem,
    table_sem,
    small_sem,
    send_sem,
    recv_sem,
    halo_send,
    halo_recv,
    list_send,
    list_recv,
    length_send,
    length_recv,
    second_sem,
):
    full, rem, columns, groups = dims
    slots = base + 1
    pairs = recv_ref.shape[1] + 1
    layers = pairs * PAIR
    listed = layers // 2
    blocks = w_ref.shape[0]
    buffer_len = blocks * BLOCK
    rows_dev = buffer_len - 2 * SHIFT
    me = lax.axis_index("serve")
    part = lax.axis_index("train")
    parts_n = lax.axis_size("train")
    half = base * full
    rest = half + (1 if rem else 0)

    def fetch(layer, sub):
        return pltpu.make_async_copy(wt_ref.at[layer], in_ref.at[sub], in_sem.at[sub])

    def message(mask, pair, sub, final):
        peer = partner(me, mask, groups)
        span = pl.ds(sub * half, rest if sub == PAIR - 1 else half)
        return pltpu.make_async_remote_copy(
            send_ref.at[peer, pair % RING, span],
            tail_ref.at[me, span] if final else recv_ref.at[me, pair, span],
            send_sem.at[pair % RING, sub],
            recv_sem.at[pair % TURNS, sub],
            device_id={"serve": peer},
            device_id_type=MESH,
        )

    def arrival(pair, sub, final):
        span = pl.ds(sub * half, rest if sub == PAIR - 1 else half)
        others = pl.ds(0, groups - 1)
        place = tail_ref.at[others, span] if final else recv_ref.at[others, pair, span]
        return pltpu.make_async_copy(place, place, recv_sem.at[pair % TURNS, sub])

    def departure(pair, sub):
        span = pl.ds(sub * half, rest if sub == PAIR - 1 else half)
        place = send_ref.at[pl.ds(0, groups - 1), pair % RING, span]
        return pltpu.make_async_copy(place, place, send_sem.at[pair % RING, sub])

    bits = [1 << n for n in range(groups.bit_length() - 1)]
    orders = [bits[1:], bits[:0:-1]]
    pieces_list = all_ref.shape[1]
    spans = [pl.ds(0, pieces_list // 2), pl.ds(pieces_list // 2, pieces_list - pieces_list // 2)]

    def stage(number):
        for which, order in enumerate(orders):
            if number < 0:
                yield which, 0, 0
                continue
            held = [0]
            for bit in order[:number]:
                held = held + [mask + bit for mask in held]
            for mask in held:
                yield which, order[number], mask

    def list_message(number, which, bit, mask):
        place = all_ref.at[partner(me, mask, groups), spans[which]]
        return pltpu.make_async_remote_copy(
            place,
            place,
            list_send.at[number],
            list_recv.at[number],
            device_id={"serve": partner(me, bit, groups)},
            device_id_type=MESH,
        )

    def lists_passed(number, sem):
        place = all_ref.at[pl.ds(0, 1 << number)]
        return pltpu.make_async_copy(place, place, sem.at[number])

    def edge(layer, side):
        to = part + 1 if side == 0 else part - 1
        return pltpu.make_async_remote_copy(
            edge_ref.at[layer, side],
            halo_ref.at[layer, side],
            halo_send.at[layer % 2, side],
            halo_recv.at[layer % 2, side],
            device_id={"train": to},
            device_id_type=MESH,
        )

    def length_message(turn, side):
        return pltpu.make_async_remote_copy(
            length_ref.at[turn],
            lengths_ref.at[turn, side],
            length_send.at[side],
            length_recv.at[turn, side],
            device_id={"train": part + 1 if side == 0 else part - 1},
            device_id_type=MESH,
        )

    lengths_ref[...] = jnp.zeros(lengths_ref.shape, jnp.float32)
    get_group = pltpu.make_async_copy(group_hbm, group_ref, small_sem.at[0])
    get_group.start()
    fetch(0, 0).start()
    get_offset = pltpu.make_async_copy(offset_hbm, offset_ref, small_sem.at[1])
    get_offset.start()
    for sub in range(1, PAIR):
        fetch(sub, sub).start()

    barrier = pltpu.get_barrier_semaphore()

    def greet(mask, carry):
        pl.semaphore_signal(barrier, inc=1, device_id={"serve": partner(me, mask, groups)}, device_id_type=MESH)
        return carry

    lax.fori_loop(1, groups, greet, 0)

    @pl.when(part > 0)
    def _():
        pl.semaphore_signal(barrier, inc=1, device_id={"train": part - 1}, device_id_type=MESH)

    @pl.when(part < parts_n - 1)
    def _():
        pl.semaphore_signal(barrier, inc=1, device_id={"train": part + 1}, device_id_type=MESH)

    below = (part + parts_n - 1) // parts_n
    above = (2 * parts_n - 2 - part) // parts_n

    row = lax.broadcasted_iota(jnp.int32, (BLOCK, columns), 0)
    lane = lax.broadcasted_iota(jnp.int32, (BLOCK, LANES), 1)
    last = rows_dev - BLOCK

    def transpose_tile(sub, low):
        high = min(low + LANES, buffer_len)
        rows_of = turned(in_ref[sub, :, low:high]).astype(w_ref.dtype)
        w_ref[low // BLOCK : high // BLOCK] = rows_of.reshape((high - low) // BLOCK, BLOCK, columns)

    def joined(group, count):
        tile = rem_ref[group, 0].astype(jnp.float32)
        for i in range(1, count):
            moved = pltpu.roll(rem_ref[group, i].astype(jnp.float32), i * rem, 1)
            tile = jnp.where(lane >= i * rem, moved, tile)
        return tile

    def edge_ends(layer, act):
        @pl.when(part < parts_n - 1)
        def _():
            act(edge(layer, 0))

        @pl.when(part > 0)
        def _():
            act(edge(layer, 1))

    def send_edges(layer, sub):
        fetch(layer, sub).wait()
        low = (buffer_len - 1) // LANES * LANES
        edge_ref[layer, 0] = turned(in_ref[sub, :, low:buffer_len])[-SHIFT:].astype(edge_ref.dtype)
        edge_ref[layer, 1] = turned(in_ref[sub, :, 0:LANES])[:SHIFT].astype(edge_ref.dtype)

        @pl.when(layer >= 2)
        def _():
            edge_ends(layer - 2, lambda copy: copy.wait_send())

        edge_ends(layer, lambda copy: copy.start())

    def prepare(pair, sub):
        layer = pair * PAIR + sub
        for low in range(0, buffer_len, LANES):
            transpose_tile(sub, low)

        @pl.when(layer + PAIR < layers)
        def _():
            fetch(layer + PAIR, sub).start()

        base_row = part * rows_dev

        @pl.when(part > 0)
        def _():
            edge(layer, 0).wait_recv()
            first = offset_ref[part, layer] - base_row
            head = jnp.where(row < first, halo_ref[layer, 0].astype(jnp.float32), w_ref[1].astype(jnp.float32))
            w_ref[1] = head.astype(w_ref.dtype)

        @pl.when(part < parts_n - 1)
        def _():
            edge(layer, 1).wait_recv()
            after = offset_ref[part + 1, layer] - base_row
            tail = w_ref[blocks - 2].astype(jnp.float32)
            tail = jnp.where(row + last >= after, halo_ref[layer, 1].astype(jnp.float32), tail)
            w_ref[blocks - 2] = tail.astype(w_ref.dtype)

        w_ref[0] = jnp.zeros((BLOCK, columns), w_ref.dtype)
        if sub == 0:

            @pl.when(pair == 0)
            def _():
                to_smem.wait()

        def last_slots(group, carry):
            over_ref[layer * groups + group] = w_ref[table_smem[layer, group * layers + base]]
            return carry

        lax.fori_loop(0, groups, last_slots, 0)

    def gather(pair, sub, group, out):
        for k in range(base):
            block = w_ref[table_smem[pair * PAIR + sub, group * layers + k]]
            for t in range(full):
                out[(sub * base + k) * full + t] = block[:, t * LANES : (t + 1) * LANES]
            if rem:
                rem_ref[group, sub * base + k, :, 0:rem] = block[:, full * LANES :]
        if rem and sub == PAIR - 1:
            out[PAIR * half] = joined(group, PAIR * base).astype(out.dtype)

    def give(low, high, pair, sub, pack, send, final):
        def one(mask, carry):
            peer = partner(me, mask, groups)
            if pack:
                gather(pair, sub, peer, send_ref.at[peer, pair % RING])
            if send:
                message(mask, pair, sub, final).start()
            return carry

        lax.fori_loop(low, high, one, 0)

    def own(pair, sub, final):
        gather(pair, sub, me, tail_ref.at[me] if final else recv_ref.at[me, pair])

    def pack_list(entry_of, out):
        for e in range(listed):
            block = over_ref[entry_of(e)]
            for t in range(full):
                out[e * full + t] = block[:, t * LANES : (t + 1) * LANES]
            if rem:
                rem_ref[groups, e, :, 0:rem] = block[:, full * LANES :]
        if rem:
            out[listed * full] = joined(groups, listed).astype(out.dtype)

    def take(pair, final):
        for sub in range(PAIR):
            arrival(pair, sub, final).wait()

    def unpack(pair):
        def recv(s, n):
            return recv_ref[s, pair, n]

        scale_rest(dims, PAIR * base, recv, rem_code, rem_scale)

        def slot(i, carry):
            def put_code(low, high, code):
                codes_ref[pair * PAIR + i // base, i % base, :, low:high] = code.astype(codes_ref.dtype)

            def put_scale(low, high, scale):
                rows[i, :, low:high] = scale

            scale_slot(dims, i, recv, rem_code, rem_scale, put_code, put_scale)
            return carry

        lax.fori_loop(0, PAIR * base, slot, 0)
        for i in range(PAIR * base):
            scale_ref[pair * PAIR + i // base, i % base : i % base + 1, :] = rows[i]

    def sent(pair):
        for sub in range(PAIR):
            departure(pair, sub).wait()

    def step(pair, carry):
        @pl.when(pair >= RING)
        def _():
            sent(pair - RING)

        for sub in range(PAIR):
            prepare(pair, sub)
            give(2, groups, pair, sub, True, True, False)
            give(1, 2, pair, sub, True, True, False)
            own(pair, sub, False)
            send_edges(pair * PAIR + sub + 1, (sub + 1) % PAIR)

        @pl.when(pair > 0)
        def _():
            take(pair - 1, False)
            unpack(pair - 1)

        return carry

    pl.semaphore_wait(barrier, groups - 1 + below + above)
    send_edges(0, 0)
    get_offset.wait()
    get_group.wait()
    spot = lax.broadcasted_iota(jnp.int32, (layers, groups * layers), 1)
    spot_group = jnp.zeros(spot.shape, jnp.int32)
    for g in range(1, groups):
        spot_group = spot_group + jnp.where(spot >= g * layers, 1, 0)
    spot_slot = spot - spot_group * layers
    seen = jnp.zeros(spot.shape, jnp.int32)
    table = jnp.zeros(spot.shape, jnp.int32)
    for j in range(group_ref.shape[1]):
        mine = group_ref[:, j : j + 1] == spot_group
        table = jnp.where(mine & (seen == spot_slot), j + 1, table)
        seen = jnp.where(mine, seen + 1, seen)
    table_ref[0:layers, :] = table
    none = layers * groups
    length = jnp.zeros((1, groups * layers), jnp.int32)
    entry = jnp.full(length.shape, none, jnp.int32)
    total = jnp.zeros((1, LANES), jnp.int32)
    shared = jnp.full(total.shape, none, jnp.int32)
    number = lax.broadcasted_iota(jnp.int32, total.shape, 1)
    long = jnp.where(seen == slots, 1, 0)
    for n in range(layers):
        here = long[n : n + 1, :]
        entry = jnp.where((here > 0) & (length == spot_slot[0:1, :]), n * groups + spot_group[0:1, :], entry)
        length = length + here
        for g in range(groups):
            one = jnp.broadcast_to(here[:, g * layers : g * layers + 1], total.shape)
            shared = jnp.where((one > 0) & (total == number), n * groups + g, shared)
            total = total + one
    table_ref[layers : layers + 1, :] = entry
    table_ref[layers + 1 : layers + 2, 0:LANES] = shared
    to_smem = pltpu.make_async_copy(table_ref, table_smem, table_sem)
    to_smem.start()
    most = jnp.broadcast_to(total.astype(jnp.float32), length_ref.shape[1:])
    over_ref[none] = jnp.zeros((BLOCK, columns), over_ref.dtype)

    end = pairs - 1
    lax.fori_loop(0, end, step, 0)

    if end >= RING:
        sent(end - RING)
    for sub in range(PAIR):
        prepare(end, sub)
        give(1, groups, end, sub, True, False, True)
        own(end, sub, True)
        if sub < PAIR - 1:
            send_edges(end * PAIR + sub + 1, sub + 1)
    pack_list(lambda e: table_smem[layers + 1, e], all_ref.at[me])
    high = len(bits) - 1
    for copy in stage(0):
        list_message(0, *copy).start()
    for which in range(2):
        list_message(high, which, 1, 0).start()
    for sub in range(PAIR - 1):
        give(2, groups, end, sub, False, True, True)
        give(1, 2, end, sub, False, True, True)

    def second(group, carry):
        for which in range(2):
            pack_list(lambda e: table_smem[layers, group * layers + which * listed + e], list_ref.at[group, which])
        return carry

    lax.fori_loop(0, groups, second, 0)
    keep = pltpu.make_async_copy(list_ref, second_ref, second_sem.at[0])
    keep.start()
    for n in range(2):
        edge_ends(layers - 1 - n, lambda copy: copy.wait_send())

    def to_neighbours(turn, act):
        @pl.when(part < parts_n - 1)
        def _():
            act(length_message(turn, 0))

        @pl.when(part > 0)
        def _():
            act(length_message(turn, 1))

    def from_neighbours(turn):
        @pl.when(part > 0)
        def _():
            length_message(turn, 0).wait_recv()

        @pl.when(part < parts_n - 1)
        def _():
            length_message(turn, 1).wait_recv()

    for turn in range(parts_n - 1):
        length_ref[turn] = most
        to_neighbours(turn, lambda copy: copy.start())
        from_neighbours(turn)
        for side in range(2):
            most = jnp.maximum(most, lengths_ref[turn, side])
        to_neighbours(turn, lambda copy: copy.wait_send())
    longest_smem[0, 0] = jnp.max(most).astype(jnp.int32)
    tell = pltpu.make_async_copy(longest_smem, longest_ref, second_sem.at[1])
    tell.start()

    take(end - 1, False)
    unpack(end - 1)
    for number in range(1, high + 1):
        lists_passed(number - 1, list_recv).wait()
        if number < high:
            for copy in stage(number):
                list_message(number, *copy).start()
        for which, bit, mask in stage(number - 1):
            list_message(high, which, 1, bit + mask).start()
        if number == 1:
            give(groups * 3 // 4, groups, end, PAIR - 1, False, True, True)
            give(1, groups * 3 // 4, end, PAIR - 1, False, True, True)
    lists_passed(high, list_recv).wait()

    def recv(s, n):
        return all_ref[s, n]

    scale_rest(dims, listed, recv, rem_code, rem_scale)

    def listed_slot(e, carry):
        def put_code(low, high, code):
            shared_codes[e, :, low:high] = code.astype(shared_codes.dtype)

        def put_scale(low, high, scale):
            shared_scale[e, :, low:high] = scale

        scale_slot(dims, e, recv, rem_code, rem_scale, put_code, put_scale)
        return carry

    lax.fori_loop(0, listed, listed_slot, 0)
    shared_codes[listed] = jnp.zeros(shared_codes.shape[1:], shared_codes.dtype)
    shared_scale[listed] = jnp.zeros(shared_scale.shape[1:], jnp.float32)

    keep.wait()
    tell.wait()
    for number in range(high + 1):
        lists_passed(number, list_send).wait()
    for pair in range(max(0, end - RING + 1), end + 1):
        sent(pair)
    take(end, True)


def list_places(group_ref, place_ref, slots, groups, shared):
    layers = group_ref.shape[0]
    me = lax.axis_index("serve")
    count = jnp.sum(jnp.where(group_ref[...] == me, 1, 0), axis=1, keepdims=True)
    ahead = jnp.zeros((layers, 1), jnp.int32)
    every = jnp.where(count == slots, 1, 0)
    if shared:
        every = jnp.zeros((layers, 1), jnp.int32)
        for g in range(groups):
            filled = jnp.sum(jnp.where(group_ref[...] == g, 1, 0), axis=1, keepdims=True)
            one = jnp.where(filled == slots, 1, 0)
            ahead = ahead + jnp.where(g < me, one, 0)
            every = every + one
    length = jnp.zeros((1, 1), jnp.int32)
    for n in range(layers):
        place = jnp.where(count[n : n + 1, :] == slots, length + ahead[n : n + 1, :], layers * groups)
        place_ref[n : n + 1, :] = jnp.broadcast_to(place, (1, place_ref.shape[1]))
        length = length + every[n : n + 1, :]
    return count


def write_kernel(
    dims,
    base,
    group_ref,
    codes_ref,
    scale_ref,
    tail_ref,
    shared_codes,
    shared_scale,
    codes_out,
    scale_out,
    scales,
    codes,
    rows,
    rem_code,
    rem_scale,
    place_ref,
    place_smem,
    sems,
    last_sems,
    place_sem,
):
    groups = dims[3]
    layers = scale_out.shape[0]
    done = layers - PAIR
    listed = layers // 2
    copies = [pltpu.make_async_copy(codes_ref.at[n], codes_out.at[n, pl.ds(0, base)], sems.at[n]) for n in range(done)]
    for copy in copies:
        copy.start()
    count = list_places(group_ref, place_ref, base + 1, groups, True)
    to_smem = pltpu.make_async_copy(place_ref, place_smem, place_sem)
    to_smem.start()

    def recv(s, n):
        return tail_ref[s, n]

    scale_rest(dims, PAIR * base, recv, rem_code, rem_scale)

    def last_pair(sub):
        def slot(k, carry):
            def put_code(low, high, code):
                codes[sub, k, :, low:high] = code.astype(codes.dtype)

            def put_scale(low, high, scale):
                rows[sub * base + k, :, low:high] = scale

            scale_slot(dims, sub * base + k, recv, rem_code, rem_scale, put_code, put_scale)
            return carry

        lax.fori_loop(0, base, slot, 0)
        copies.append(pltpu.make_async_copy(codes.at[sub], codes_out.at[done + sub, pl.ds(0, base)], sems.at[done + sub]))
        copies[-1].start()

    last_pair(0)
    to_smem.wait()
    places = [jnp.minimum(place_smem[n, 0], listed) for n in range(layers)]
    for n in range(layers):
        copies.append(pltpu.make_async_copy(shared_codes.at[places[n]], codes_out.at[n, base], last_sems.at[n]))
        copies[-1].start()
    for sub in range(1, PAIR):
        last_pair(sub)
    slot = lax.broadcasted_iota(jnp.int32, scales.shape[1:], 0)
    for sub in range(PAIR):
        for k in range(base):
            scales[done + sub, k : k + 1, :] = rows[sub * base + k]
    for n in range(layers):
        scale = scale_ref[n] if n < done else scales[n]
        scale = jnp.where(slot < count[n : n + 1, :], scale, 0.0)
        scales[n] = jnp.where(slot < base, scale, jnp.broadcast_to(shared_scale[places[n]], scale.shape))
    copies.append(pltpu.make_async_copy(scales, scale_out, sems.at[layers]))
    copies[-1].start()
    for copy in copies:
        copy.wait()


def late_kernel(
    dims,
    base,
    group_ref,
    got_ref,
    codes_in,
    scale_in,
    codes_out,
    scale_out,
    extra,
    extra_scale,
    scales,
    rem_code,
    rem_scale,
    place_ref,
    place_smem,
    sem,
):
    del codes_in, scale_in
    full, rem, columns, groups = dims
    layers = codes_out.shape[0]
    listed = layers // 2
    list_places(group_ref, place_ref, base + 1, groups, False)
    to_smem = pltpu.make_async_copy(place_ref, place_smem, sem)
    to_smem.start()
    to_smem.wait()
    slot = lax.broadcasted_iota(jnp.int32, scales.shape, 0)
    for which in range(2):

        def recv(s, n, which=which):
            return got_ref[s, which, n]

        scale_rest(dims, listed, recv, rem_code, rem_scale)

        def last_slot(layer, carry, which=which, recv=recv):
            place = place_smem[layer, 0] - which * listed

            @pl.when((place >= 0) & (place < listed))
            def _():
                def put_code(low, high, code):
                    extra[:, low:high] = code.astype(extra.dtype)

                def put_scale(low, high, scale):
                    extra_scale[:, low:high] = scale

                scale_slot(dims, place, recv, rem_code, rem_scale, put_code, put_scale)
                pltpu.sync_copy(extra, codes_out.at[layer, base])
                pltpu.sync_copy(scale_out.at[layer], scales)
                scales[...] = jnp.where(slot < base, scales[...], jnp.broadcast_to(extra_scale[...], scales.shape))
                pltpu.sync_copy(scales, scale_out.at[layer])

            return carry

        lax.fori_loop(0, layers, last_slot, 0)


def shards(train_weights, row_offset, block_group):
    train_n = lax.axis_size("train")
    serve_n = lax.axis_size("serve")
    layers, buffer_len, columns = train_weights.shape
    blocks_dev = block_group.shape[1]
    base = (blocks_dev + serve_n - 1) // serve_n
    slots = base + 1
    full = columns // LANES
    rem = columns - full * LANES
    pairs = layers // PAIR
    listed = layers // 2
    pieces = PAIR * base * full + (1 if rem else 0)
    pieces_list = listed * full + (1 if rem else 0)
    rests = max(PAIR * base, listed)
    spots = serve_n * layers
    width = columns * serve_n
    dtype = train_weights.dtype
    dims = (full, rem, columns, serve_n)
    assert SHIFT == BLOCK and buffer_len % BLOCK == 0
    assert rests * rem <= LANES and layers % PAIR == 0 and slots <= layers and pairs > 1

    group_ids = block_group[:, :, 0]
    smem = pl.BlockSpec(memory_space=pltpu.SMEM)
    vmem = pl.BlockSpec(memory_space=pltpu.VMEM)
    anywhere = pl.BlockSpec(memory_space=pl.ANY)
    hbm = pl.BlockSpec(memory_space=pltpu.HBM)
    codes, scales, tail, shared_codes, shared_scale, second, longest = pl.pallas_call(
        functools.partial(move_kernel, dims, base),
        in_specs=[hbm, hbm, hbm],
        out_specs=[vmem, vmem, vmem, vmem, vmem, hbm, hbm],
        out_shape=[
            pltpu.VMEM((layers - PAIR, base, BLOCK, width), dtype),
            pltpu.VMEM((layers - PAIR, slots, width), jnp.float32),
            pltpu.VMEM((serve_n, pieces, BLOCK, LANES), dtype),
            pltpu.VMEM((listed + 1, BLOCK, width), dtype),
            pltpu.VMEM((listed + 1, 1, width), jnp.float32),
            jax.ShapeDtypeStruct((serve_n, 2, pieces_list, BLOCK, LANES), dtype),
            jax.ShapeDtypeStruct((1, 1), jnp.int32),
        ],
        scratch_shapes=[
            pltpu.VMEM((serve_n, pieces_list, BLOCK, LANES), dtype),
            pltpu.VMEM((serve_n, pairs - 1, pieces, BLOCK, LANES), dtype),
            pltpu.VMEM((serve_n, RING, pieces, BLOCK, LANES), dtype),
            pltpu.VMEM((PAIR, columns, buffer_len), dtype),
            pltpu.VMEM((buffer_len // BLOCK, BLOCK, columns), dtype),
            pltpu.VMEM((serve_n + 1, rests, BLOCK, LANES), dtype),
            pltpu.VMEM((layers, 2, SHIFT, columns), dtype),
            pltpu.VMEM((layers, 2, SHIFT, columns), dtype),
            pltpu.VMEM((serve_n * layers + 1, BLOCK, columns), dtype),
            pltpu.VMEM((serve_n, 2, pieces_list, BLOCK, LANES), dtype),
            pltpu.VMEM((serve_n, BLOCK, LANES), jnp.float32),
            pltpu.VMEM((serve_n, 1, LANES), jnp.float32),
            pltpu.VMEM((PAIR * base, 1, width), jnp.float32),
            pltpu.VMEM((layers + 8, spots), jnp.int32),
            pltpu.SMEM((layers + 8, spots), jnp.int32),
            pltpu.VMEM((train_n, 8, LANES), jnp.float32),
            pltpu.VMEM((train_n, 2, 8, LANES), jnp.float32),
            pltpu.SMEM((1, 1), jnp.int32),
            pltpu.SMEM((train_n + 1, layers), jnp.int32),
            pltpu.VMEM((layers, blocks_dev), jnp.int32),
            pltpu.SemaphoreType.DMA((PAIR,)),
            pltpu.SemaphoreType.DMA,
            pltpu.SemaphoreType.DMA((2,)),
            pltpu.SemaphoreType.DMA((RING, PAIR)),
            pltpu.SemaphoreType.DMA((TURNS, PAIR)),
            pltpu.SemaphoreType.DMA((2, 2)),
            pltpu.SemaphoreType.DMA((2, 2)),
            pltpu.SemaphoreType.DMA((serve_n.bit_length() - 1,)),
            pltpu.SemaphoreType.DMA((serve_n.bit_length() - 1,)),
            pltpu.SemaphoreType.DMA((2,)),
            pltpu.SemaphoreType.DMA((train_n, 2)),
            pltpu.SemaphoreType.DMA((2,)),
        ],
        compiler_params=pltpu.CompilerParams(
            collective_id=0, has_side_effects=True, vmem_limit_bytes=36 * MIB
        ),
        name="move",
    )(pltpu.with_memory_space_constraint(row_offset.T, pltpu.HBM), group_ids, jnp.swapaxes(train_weights, 1, 2))

    codes_shape = jax.ShapeDtypeStruct((layers, slots, BLOCK, width), dtype)
    scales_shape = jax.ShapeDtypeStruct((layers, slots, width), jnp.float32)
    rest_scratch = [
        pltpu.VMEM((serve_n, BLOCK, LANES), jnp.float32),
        pltpu.VMEM((serve_n, 1, LANES), jnp.float32),
        pltpu.VMEM((layers, LANES), jnp.int32),
        pltpu.SMEM((layers, LANES), jnp.int32),
    ]
    codes_out, scales_out = pl.pallas_call(
        functools.partial(write_kernel, dims, base),
        in_specs=[vmem, anywhere, vmem, vmem, vmem, vmem],
        out_specs=[hbm, hbm],
        out_shape=[codes_shape, pltpu.HBM((layers, slots, width), jnp.float32)],
        scratch_shapes=[
            pltpu.VMEM((layers, slots, width), jnp.float32),
            pltpu.VMEM((PAIR, base, BLOCK, width), dtype),
            pltpu.VMEM((PAIR * base, 1, width), jnp.float32),
            *rest_scratch,
            pltpu.SemaphoreType.DMA((layers + 1,)),
            pltpu.SemaphoreType.DMA((layers,)),
            pltpu.SemaphoreType.DMA,
        ],
        compiler_params=pltpu.CompilerParams(vmem_limit_bytes=10 * MIB),
        name="write",
    )(group_ids, codes, scales, tail, shared_codes, shared_scale)

    def late(state):
        got = lax.all_to_all(second, "serve", split_axis=0, concat_axis=0, tiled=True)
        late_codes, late_scales = pl.pallas_call(
            functools.partial(late_kernel, dims, base),
            in_specs=[vmem, vmem, hbm, hbm],
            out_specs=[hbm, hbm],
            out_shape=[codes_shape, scales_shape],
            input_output_aliases={2: 0, 3: 1},
            scratch_shapes=[
                pltpu.VMEM((BLOCK, width), dtype),
                pltpu.VMEM((1, width), jnp.float32),
                pltpu.VMEM((slots, width), jnp.float32),
                *rest_scratch,
                pltpu.SemaphoreType.DMA,
            ],
            compiler_params=pltpu.CompilerParams(vmem_limit_bytes=6 * MIB),
            name="late",
        )(group_ids, got, state[1], state[2])
        return jnp.zeros((), jnp.int32), late_codes, late_scales

    state = (longest[0, 0], codes_out, scales_out)
    _, codes_out, scales_out = lax.while_loop(lambda now: now[0] > listed, late, state)
    return (
        codes_out.reshape(layers, 1, 1, slots, BLOCK, width),
        scales_out.reshape(layers, 1, 1, slots, width),
    )


def solution(mesh):
    return jax.shard_map(
        shards,
        mesh=mesh,
        in_specs=(P(None, "train", "serve"), P(), P(None, "train", None)),
        out_specs=(
            P(None, "serve", "train", None, None, None),
            P(None, "serve", "train", None, None),
        ),
        check_vma=False,
    )
```

```python
import functools

import jax
import jax.numpy as jnp
from jax import lax
from jax.experimental import pallas as pl
from jax.experimental.pallas import tpu as pltpu
from jax.sharding import PartitionSpec as P

BLOCK = 32
SHIFT = 32
LANES = 128
PAIR = 2
RING = 3
TURNS = 4
MESH = pl.DeviceIdType.MESH
MIB = 1024 * 1024


def turned(values):
    return jnp.transpose(values.astype(jnp.float32))


def partner(me, mask, count):
    out, bit = 0, 1
    while bit < count:
        out = out + ((me // bit + mask // bit) % 2) * bit
        bit *= 2
    return out


def scaled(values):
    values = values.astype(jnp.float32)
    divisor = jnp.maximum(jnp.max(jnp.abs(values), axis=0, keepdims=True), 0.25)
    return values * (1.0 / divisor), divisor


def scale_rest(dims, count, recv, rem_code, rem_scale):
    full, rem, columns, sources = dims
    if rem:
        for s in range(sources):
            rem_code[s], rem_scale[s] = scaled(recv(s, count * full))


def scale_slot(dims, i, recv, rem_code, rem_scale, put_code, put_scale, place=None):
    place = i if place is None else place
    full, rem, columns, sources = dims
    width = columns * sources
    tiles = -(-width // LANES)
    lane = lax.broadcasted_iota(jnp.int32, (BLOCK, LANES), 1)
    lane_row = lax.broadcasted_iota(jnp.int32, (1, LANES), 1)
    parts = [None] * tiles

    def put(tile, low, code, scale):
        if tile >= tiles:
            return
        if parts[tile] is None:
            parts[tile] = (code, scale)
        else:
            before = parts[tile]
            parts[tile] = (jnp.where(lane >= low, code, before[0]), jnp.where(lane_row >= low, scale, before[1]))

    def flush(below):
        for tile in range(below):
            if parts[tile] is not None:
                code, scale = parts[tile]
                end = min(width, (tile + 1) * LANES)
                size = end - tile * LANES
                put_code(tile * LANES, end, code[:, :size])
                put_scale(tile * LANES, end, scale[:, :size])
                parts[tile] = None

    for s in range(sources):
        for t in range(full + (1 if rem else 0)):
            start = s * columns + t * LANES
            size = LANES if t < full else rem
            low = start % LANES
            if t < full:
                code, scale = scaled(recv(s, i * full + t))
                if low:
                    code, scale = pltpu.roll(code, low, 1), pltpu.roll(scale, low, 1)
            else:
                turn = lax.rem(low + LANES - place * rem, LANES)
                code, scale = pltpu.roll(rem_code[s], turn, 1), pltpu.roll(rem_scale[s], turn, 1)
            tile = start // LANES
            put(tile, low, code, scale)
            if low + size > LANES:
                put(tile + 1, 0, code, scale)
            flush((start + size) // LANES)
    flush(tiles)


def move_kernel(
    dims,
    base,
    offset_hbm,
    group_hbm,
    wt_ref,
    codes_ref,
    scale_ref,
    tail_ref,
    shared_codes,
    shared_scale,
    second_ref,
    longest_ref,
    all_ref,
    turned_ref,
    recv_ref,
    send_ref,
    in_ref,
    w_ref,
    rem_ref,
    edge_ref,
    halo_ref,
    over_ref,
    list_ref,
    rem_code,
    rem_scale,
    rows,
    table_ref,
    table_smem,
    length_ref,
    lengths_ref,
    longest_smem,
    offset_ref,
    group_ref,
    in_sem,
    table_sem,
    small_sem,
    send_sem,
    recv_sem,
    halo_send,
    halo_recv,
    list_send,
    list_recv,
    length_send,
    length_recv,
    second_sem,
):
    full, rem, columns, groups = dims
    slots = base + 1
    pairs = recv_ref.shape[1] + 1
    layers = pairs * PAIR
    listed = layers // 2
    blocks = w_ref.shape[0]
    buffer_len = blocks * BLOCK
    rows_dev = buffer_len - 2 * SHIFT
    me = lax.axis_index("serve")
    part = lax.axis_index("train")
    parts_n = lax.axis_size("train")
    half = base * full
    rest = half + (1 if rem else 0)
    ahead = base > 2

    def fetch(layer, sub):
        return pltpu.make_async_copy(wt_ref.at[layer], in_ref.at[sub], in_sem.at[sub])

    def landing(source, pair, sub, final):
        if ahead and isinstance(pair, int) and pair == 0 and sub == 0:
            return turned_ref.at[source]
        return tail_ref.at[source] if final else recv_ref.at[source, pair]

    def message(mask, pair, sub, final, slots_of=None):
        peer = partner(me, mask, groups)
        span = pl.ds(sub * half, rest if sub == PAIR - 1 else half)
        if slots_of is not None:
            span = pl.ds(slots_of[0] * full, (slots_of[1] - slots_of[0]) * full)
        return pltpu.make_async_remote_copy(
            send_ref.at[peer, pair % RING, span],
            landing(me, pair, sub, final).at[span],
            send_sem.at[pair % RING, sub],
            recv_sem.at[pair % TURNS, sub],
            device_id={"serve": peer},
            device_id_type=MESH,
        )

    def arrival(pair, sub, final):
        span = pl.ds(sub * half, rest if sub == PAIR - 1 else half)
        others = pl.ds(0, groups - 1)
        place = tail_ref.at[others, span] if final else recv_ref.at[others, pair, span]
        return pltpu.make_async_copy(place, place, recv_sem.at[pair % TURNS, sub])

    def departure(pair, sub):
        span = pl.ds(sub * half, rest if sub == PAIR - 1 else half)
        place = send_ref.at[pl.ds(0, groups - 1), pair % RING, span]
        return pltpu.make_async_copy(place, place, send_sem.at[pair % RING, sub])

    bits = [1 << n for n in range(groups.bit_length() - 1)]
    orders = [bits[1:], bits[:0:-1]]
    pieces_list = all_ref.shape[1]
    spans = [pl.ds(0, pieces_list // 2), pl.ds(pieces_list // 2, pieces_list - pieces_list // 2)]

    def stage(number):
        for which, order in enumerate(orders):
            if number < 0:
                yield which, 0, 0
                continue
            held = [0]
            for bit in order[:number]:
                held = held + [mask + bit for mask in held]
            for mask in held:
                yield which, order[number], mask

    def list_message(number, which, bit, mask):
        place = all_ref.at[partner(me, mask, groups), spans[which]]
        return pltpu.make_async_remote_copy(
            place,
            place,
            list_send.at[number],
            list_recv.at[number],
            device_id={"serve": partner(me, bit, groups)},
            device_id_type=MESH,
        )

    def lists_passed(number, sem):
        place = all_ref.at[pl.ds(0, 1 << number)]
        return pltpu.make_async_copy(place, place, sem.at[number])

    def edge(layer, side):
        to = part + 1 if side == 0 else part - 1
        return pltpu.make_async_remote_copy(
            edge_ref.at[layer, side],
            halo_ref.at[layer, side],
            halo_send.at[layer % 2, side],
            halo_recv.at[layer % 2, side],
            device_id={"train": to},
            device_id_type=MESH,
        )

    def length_message(turn, side):
        return pltpu.make_async_remote_copy(
            length_ref.at[turn],
            lengths_ref.at[turn, side],
            length_send.at[side],
            length_recv.at[turn, side],
            device_id={"train": part + 1 if side == 0 else part - 1},
            device_id_type=MESH,
        )

    lengths_ref[...] = jnp.zeros(lengths_ref.shape, jnp.float32)
    get_group = pltpu.make_async_copy(group_hbm, group_ref, small_sem.at[0])
    get_group.start()
    fetch(0, 0).start()
    get_offset = pltpu.make_async_copy(offset_hbm, offset_ref, small_sem.at[1])
    get_offset.start()
    for sub in range(1, PAIR):
        fetch(sub, sub).start()

    barrier = pltpu.get_barrier_semaphore()

    def greet(mask, carry):
        pl.semaphore_signal(barrier, inc=1, device_id={"serve": partner(me, mask, groups)}, device_id_type=MESH)
        return carry

    lax.fori_loop(1, groups, greet, 0)

    @pl.when(part > 0)
    def _():
        pl.semaphore_signal(barrier, inc=1, device_id={"train": part - 1}, device_id_type=MESH)

    @pl.when(part < parts_n - 1)
    def _():
        pl.semaphore_signal(barrier, inc=1, device_id={"train": part + 1}, device_id_type=MESH)

    below = (part + parts_n - 1) // parts_n
    above = (2 * parts_n - 2 - part) // parts_n

    row = lax.broadcasted_iota(jnp.int32, (BLOCK, columns), 0)
    lane = lax.broadcasted_iota(jnp.int32, (BLOCK, LANES), 1)
    last = rows_dev - BLOCK

    def transpose_tile(sub, low):
        high = min(low + LANES, buffer_len)
        rows_of = turned(in_ref[sub, :, low:high]).astype(w_ref.dtype)
        w_ref[low // BLOCK : high // BLOCK] = rows_of.reshape((high - low) // BLOCK, BLOCK, columns)

    def joined(group, count):
        tile = rem_ref[group, 0].astype(jnp.float32)
        for i in range(1, count):
            moved = pltpu.roll(rem_ref[group, i].astype(jnp.float32), i * rem, 1)
            tile = jnp.where(lane >= i * rem, moved, tile)
        return tile

    def edge_ends(layer, act):
        @pl.when(part < parts_n - 1)
        def _():
            act(edge(layer, 0))

        @pl.when(part > 0)
        def _():
            act(edge(layer, 1))

    def send_edges(layer, sub):
        fetch(layer, sub).wait()
        low = (buffer_len - 1) // LANES * LANES
        edge_ref[layer, 0] = turned(in_ref[sub, :, low:buffer_len])[-SHIFT:].astype(edge_ref.dtype)
        edge_ref[layer, 1] = turned(in_ref[sub, :, 0:LANES])[:SHIFT].astype(edge_ref.dtype)

        @pl.when(layer >= 2)
        def _():
            edge_ends(layer - 2, lambda copy: copy.wait_send())

        edge_ends(layer, lambda copy: copy.start())

    def turn_layer(pair, sub):
        layer = pair * PAIR + sub
        for low in range(0, buffer_len, LANES):
            transpose_tile(sub, low)

        @pl.when(layer + PAIR < layers)
        def _():
            fetch(layer + PAIR, sub).start()

        w_ref[0] = jnp.zeros((BLOCK, columns), w_ref.dtype)

    def finish_layer(pair, sub):
        layer = pair * PAIR + sub
        base_row = part * rows_dev

        @pl.when(part > 0)
        def _():
            edge(layer, 0).wait_recv()
            first = offset_ref[part, layer] - base_row
            head = jnp.where(row < first, halo_ref[layer, 0].astype(jnp.float32), w_ref[1].astype(jnp.float32))
            w_ref[1] = head.astype(w_ref.dtype)

        @pl.when(part < parts_n - 1)
        def _():
            edge(layer, 1).wait_recv()
            after = offset_ref[part + 1, layer] - base_row
            tail = w_ref[blocks - 2].astype(jnp.float32)
            tail = jnp.where(row + last >= after, halo_ref[layer, 1].astype(jnp.float32), tail)
            w_ref[blocks - 2] = tail.astype(w_ref.dtype)

        def last_slots(group, carry):
            over_ref[layer * groups + group] = w_ref[table_smem[layer, group * layers + base]]
            return carry

        lax.fori_loop(0, groups, last_slots, 0)

    def prepare(pair, sub):
        turn_layer(pair, sub)
        finish_layer(pair, sub)

    def gather(pair, sub, group, out, slots_of=None):
        for k in range(*(slots_of or (0, base))):
            block = w_ref[table_smem[pair * PAIR + sub, group * layers + k]]
            for t in range(full):
                out[(sub * base + k) * full + t] = block[:, t * LANES : (t + 1) * LANES]
            if rem:
                rem_ref[group, sub * base + k, :, 0:rem] = block[:, full * LANES :]
        if rem and sub == PAIR - 1:
            out[PAIR * half] = joined(group, PAIR * base).astype(out.dtype)

    def give(low, high, pair, sub, pack, send, final, slots_of=None):
        def one(mask, carry):
            peer = partner(me, mask, groups)
            if pack:
                gather(pair, sub, peer, send_ref.at[peer, pair % RING], slots_of)
            if send:
                message(mask, pair, sub, final, slots_of).start()
            return carry

        lax.fori_loop(low, high, one, 0)

    def own(pair, sub, final):
        gather(pair, sub, me, landing(me, pair, sub, final))

    def pack_list(entry_of, out):
        for e in range(listed):
            block = over_ref[entry_of(e)]
            for t in range(full):
                out[e * full + t] = block[:, t * LANES : (t + 1) * LANES]
            if rem:
                rem_ref[groups, e, :, 0:rem] = block[:, full * LANES :]
        if rem:
            out[listed * full] = joined(groups, listed).astype(out.dtype)

    def take(pair, final):
        for sub in range(PAIR):
            arrival(pair, sub, final).wait()

    def unpack(pair):
        def recv(s, n):
            return recv_ref[s, pair, n]

        scale_rest(dims, PAIR * base, recv, rem_code, rem_scale)

        def slot(i, carry):
            def put_code(low, high, code):
                codes_ref[pair * PAIR + i // base, i % base, :, low:high] = code.astype(codes_ref.dtype)

            def put_scale(low, high, scale):
                rows[i, :, low:high] = scale

            place = i
            if ahead:
                place = table_smem[layers + 2, me * layers + jnp.minimum(i, base - 1)]
                place = jnp.where((pair == 0) & (i < base), place, i)
            scale_slot(dims, i, recv, rem_code, rem_scale, put_code, put_scale, place)
            return carry

        lax.fori_loop(0, PAIR * base, slot, 0)
        for i in range(PAIR * base):
            scale_ref[pair * PAIR + i // base, i % base : i % base + 1, :] = rows[i]

    def sent(pair):
        for sub in range(PAIR):
            departure(pair, sub).wait()

    def step(pair, carry):
        @pl.when(pair >= RING)
        def _():
            sent(pair - RING)

        for sub in range(PAIR):
            prepare(pair, sub)
            give(2, groups, pair, sub, True, True, False)
            give(1, 2, pair, sub, True, True, False)
            own(pair, sub, False)
            send_edges(pair * PAIR + sub + 1, (sub + 1) % PAIR)

        take(pair - 1, False)
        if ahead:

            @pl.when(pair == 1)
            def _():
                def restore(source, inner):
                    for k in range(base):
                        place = table_smem[layers + 2, me * layers + k]
                        for t in range(full):
                            recv_ref[source, 0, k * full + t] = turned_ref[source, place * full + t]
                    return inner

                lax.fori_loop(0, groups, restore, 0)

        unpack(pair - 1)
        return carry

    get_group.wait()
    spot = lax.broadcasted_iota(jnp.int32, (layers, groups * layers), 1)
    spot_group = jnp.zeros(spot.shape, jnp.int32)
    for g in range(1, groups):
        spot_group = spot_group + jnp.where(spot >= g * layers, 1, 0)
    spot_slot = spot - spot_group * layers
    seen = jnp.zeros(spot.shape, jnp.int32)
    table = jnp.zeros(spot.shape, jnp.int32)
    moved = jnp.zeros((1, groups * layers), jnp.int32)
    for j in range(group_ref.shape[1]):
        mine = group_ref[:, j : j + 1] == spot_group
        table = jnp.where(mine & (seen == spot_slot), j + 1, table)
        moved = jnp.where(mine[0:1, :] & (seen[0:1, :] + 1 == spot_slot[0:1, :]), j + 1, moved)
        seen = jnp.where(mine, seen + 1, seen)
    table_ref[0:layers, :] = table
    if ahead:
        count, k = seen[0:1, :], spot_slot[0:1, :]
        final_block = group_ref.shape[1]
        turns = (group_ref[0:1, final_block - 1 : final_block] == spot_group[0:1, :]) & (count <= base)
        turned_row = jnp.where(k == 0, final_block, jnp.where(k < count, moved, 0))
        table_ref[0:1, :] = jnp.where(turns, turned_row, table[0:1, :])
        position = jnp.where(k == count - 1, 0, jnp.where(k < count, k + 1, k))
        table_ref[layers + 2 : layers + 3, :] = jnp.where(turns, position, k)
    none = layers * groups
    length = jnp.zeros((1, groups * layers), jnp.int32)
    entry = jnp.full(length.shape, none, jnp.int32)
    total = jnp.zeros((1, LANES), jnp.int32)
    shared = jnp.full(total.shape, none, jnp.int32)
    number = lax.broadcasted_iota(jnp.int32, total.shape, 1)
    long = jnp.where(seen == slots, 1, 0)
    for n in range(layers):
        here = long[n : n + 1, :]
        entry = jnp.where((here > 0) & (length == spot_slot[0:1, :]), n * groups + spot_group[0:1, :], entry)
        length = length + here
        for g in range(groups):
            one = jnp.broadcast_to(here[:, g * layers : g * layers + 1], total.shape)
            shared = jnp.where((one > 0) & (total == number), n * groups + g, shared)
            total = total + one
    table_ref[layers : layers + 1, :] = entry
    table_ref[layers + 1 : layers + 2, 0:LANES] = shared
    to_smem = pltpu.make_async_copy(table_ref, table_smem, table_sem)
    to_smem.start()
    most = jnp.broadcast_to(total.astype(jnp.float32), length_ref.shape[1:])
    over_ref[none] = jnp.zeros((BLOCK, columns), over_ref.dtype)

    pl.semaphore_wait(barrier, groups - 1 + below + above)
    send_edges(0, 0)
    get_offset.wait()
    end = pairs - 1
    to_smem.wait()
    for sub in range(PAIR):
        turn_layer(0, sub)
        if sub == 0 and ahead:
            give(2, groups, 0, sub, True, True, False, (2, base))
            finish_layer(0, sub)
            give(2, groups, 0, sub, True, True, False, (0, 2))
            give(1, 2, 0, sub, True, True, False)
        else:
            finish_layer(0, sub)
            give(2, groups, 0, sub, True, True, False)
            give(1, 2, 0, sub, True, True, False)
        own(0, sub, False)
        send_edges(sub + 1, (sub + 1) % PAIR)
    lax.fori_loop(1, end, step, 0)

    if end >= RING:
        sent(end - RING)
    for sub in range(PAIR):
        prepare(end, sub)
        give(1, groups, end, sub, True, False, True)
        own(end, sub, True)
        if sub < PAIR - 1:
            send_edges(end * PAIR + sub + 1, sub + 1)
    pack_list(lambda e: table_smem[layers + 1, e], all_ref.at[me])
    high = len(bits) - 1
    for copy in stage(0):
        list_message(0, *copy).start()
    for which in range(2):
        list_message(high, which, 1, 0).start()
    for sub in range(PAIR - 1):
        give(2, groups, end, sub, False, True, True)
        give(1, 2, end, sub, False, True, True)

    def second(group, carry):
        for which in range(2):
            pack_list(lambda e: table_smem[layers, group * layers + which * listed + e], list_ref.at[group, which])
        return carry

    lax.fori_loop(0, groups, second, 0)
    keep = pltpu.make_async_copy(list_ref, second_ref, second_sem.at[0])
    keep.start()
    for n in range(2):
        edge_ends(layers - 1 - n, lambda copy: copy.wait_send())

    def to_neighbours(turn, act):
        @pl.when(part < parts_n - 1)
        def _():
            act(length_message(turn, 0))

        @pl.when(part > 0)
        def _():
            act(length_message(turn, 1))

    def from_neighbours(turn):
        @pl.when(part > 0)
        def _():
            length_message(turn, 0).wait_recv()

        @pl.when(part < parts_n - 1)
        def _():
            length_message(turn, 1).wait_recv()

    for turn in range(parts_n - 1):
        length_ref[turn] = most
        to_neighbours(turn, lambda copy: copy.start())
        from_neighbours(turn)
        for side in range(2):
            most = jnp.maximum(most, lengths_ref[turn, side])
        to_neighbours(turn, lambda copy: copy.wait_send())
    longest_smem[0, 0] = jnp.max(most).astype(jnp.int32)
    tell = pltpu.make_async_copy(longest_smem, longest_ref, second_sem.at[1])
    tell.start()

    take(end - 1, False)
    unpack(end - 1)
    for number in range(1, high + 1):
        lists_passed(number - 1, list_recv).wait()
        if number < high:
            for copy in stage(number):
                list_message(number, *copy).start()
        for which, bit, mask in stage(number - 1):
            list_message(high, which, 1, bit + mask).start()
        if number == 1:
            give(groups * 3 // 4, groups, end, PAIR - 1, False, True, True)
            give(1, groups * 3 // 4, end, PAIR - 1, False, True, True)
    lists_passed(high, list_recv).wait()

    def recv(s, n):
        return all_ref[s, n]

    scale_rest(dims, listed, recv, rem_code, rem_scale)

    def listed_slot(e, carry):
        def put_code(low, high, code):
            shared_codes[e, :, low:high] = code.astype(shared_codes.dtype)

        def put_scale(low, high, scale):
            shared_scale[e, :, low:high] = scale

        scale_slot(dims, e, recv, rem_code, rem_scale, put_code, put_scale)
        return carry

    lax.fori_loop(0, listed, listed_slot, 0)
    shared_codes[listed] = jnp.zeros(shared_codes.shape[1:], shared_codes.dtype)
    shared_scale[listed] = jnp.zeros(shared_scale.shape[1:], jnp.float32)

    keep.wait()
    tell.wait()
    for number in range(high + 1):
        lists_passed(number, list_send).wait()
    for pair in range(max(0, end - RING + 1), end + 1):
        sent(pair)
    take(end, True)


def list_places(group_ref, place_ref, slots, groups, shared):
    layers = group_ref.shape[0]
    me = lax.axis_index("serve")
    count = jnp.sum(jnp.where(group_ref[...] == me, 1, 0), axis=1, keepdims=True)
    ahead = jnp.zeros((layers, 1), jnp.int32)
    every = jnp.where(count == slots, 1, 0)
    if shared:
        every = jnp.zeros((layers, 1), jnp.int32)
        for g in range(groups):
            filled = jnp.sum(jnp.where(group_ref[...] == g, 1, 0), axis=1, keepdims=True)
            one = jnp.where(filled == slots, 1, 0)
            ahead = ahead + jnp.where(g < me, one, 0)
            every = every + one
    length = jnp.zeros((1, 1), jnp.int32)
    for n in range(layers):
        place = jnp.where(count[n : n + 1, :] == slots, length + ahead[n : n + 1, :], layers * groups)
        place_ref[n : n + 1, :] = jnp.broadcast_to(place, (1, place_ref.shape[1]))
        length = length + every[n : n + 1, :]
    return count


def write_kernel(
    dims,
    base,
    group_ref,
    codes_ref,
    scale_ref,
    tail_ref,
    shared_codes,
    shared_scale,
    codes_out,
    scale_out,
    scales,
    codes,
    rows,
    rem_code,
    rem_scale,
    place_ref,
    place_smem,
    sems,
    last_sems,
    place_sem,
):
    groups = dims[3]
    layers = scale_out.shape[0]
    done = layers - PAIR
    listed = layers // 2
    copies = [pltpu.make_async_copy(codes_ref.at[n], codes_out.at[n, pl.ds(0, base)], sems.at[n]) for n in range(done)]
    for copy in copies:
        copy.start()
    count = list_places(group_ref, place_ref, base + 1, groups, True)
    to_smem = pltpu.make_async_copy(place_ref, place_smem, place_sem)
    to_smem.start()

    def recv(s, n):
        return tail_ref[s, n]

    scale_rest(dims, PAIR * base, recv, rem_code, rem_scale)

    def last_pair(sub):
        def slot(k, carry):
            def put_code(low, high, code):
                codes[sub, k, :, low:high] = code.astype(codes.dtype)

            def put_scale(low, high, scale):
                rows[sub * base + k, :, low:high] = scale

            scale_slot(dims, sub * base + k, recv, rem_code, rem_scale, put_code, put_scale)
            return carry

        lax.fori_loop(0, base, slot, 0)
        copies.append(pltpu.make_async_copy(codes.at[sub], codes_out.at[done + sub, pl.ds(0, base)], sems.at[done + sub]))
        copies[-1].start()

    last_pair(0)
    to_smem.wait()
    places = [jnp.minimum(place_smem[n, 0], listed) for n in range(layers)]
    for n in range(layers):
        copies.append(pltpu.make_async_copy(shared_codes.at[places[n]], codes_out.at[n, base], last_sems.at[n]))
        copies[-1].start()
    for sub in range(1, PAIR):
        last_pair(sub)
    slot = lax.broadcasted_iota(jnp.int32, scales.shape[1:], 0)
    for sub in range(PAIR):
        for k in range(base):
            scales[done + sub, k : k + 1, :] = rows[sub * base + k]
    for n in range(layers):
        scale = scale_ref[n] if n < done else scales[n]
        scale = jnp.where(slot < count[n : n + 1, :], scale, 0.0)
        scales[n] = jnp.where(slot < base, scale, jnp.broadcast_to(shared_scale[places[n]], scale.shape))
    copies.append(pltpu.make_async_copy(scales, scale_out, sems.at[layers]))
    copies[-1].start()
    for copy in copies:
        copy.wait()


def late_kernel(
    dims,
    base,
    group_ref,
    got_ref,
    codes_in,
    scale_in,
    codes_out,
    scale_out,
    extra,
    extra_scale,
    scales,
    rem_code,
    rem_scale,
    place_ref,
    place_smem,
    sem,
):
    del codes_in, scale_in
    full, rem, columns, groups = dims
    layers = codes_out.shape[0]
    listed = layers // 2
    list_places(group_ref, place_ref, base + 1, groups, False)
    to_smem = pltpu.make_async_copy(place_ref, place_smem, sem)
    to_smem.start()
    to_smem.wait()
    slot = lax.broadcasted_iota(jnp.int32, scales.shape, 0)
    for which in range(2):

        def recv(s, n, which=which):
            return got_ref[s, which, n]

        scale_rest(dims, listed, recv, rem_code, rem_scale)

        def last_slot(layer, carry, which=which, recv=recv):
            place = place_smem[layer, 0] - which * listed

            @pl.when((place >= 0) & (place < listed))
            def _():
                def put_code(low, high, code):
                    extra[:, low:high] = code.astype(extra.dtype)

                def put_scale(low, high, scale):
                    extra_scale[:, low:high] = scale

                scale_slot(dims, place, recv, rem_code, rem_scale, put_code, put_scale)
                pltpu.sync_copy(extra, codes_out.at[layer, base])
                pltpu.sync_copy(scale_out.at[layer], scales)
                scales[...] = jnp.where(slot < base, scales[...], jnp.broadcast_to(extra_scale[...], scales.shape))
                pltpu.sync_copy(scales, scale_out.at[layer])

            return carry

        lax.fori_loop(0, layers, last_slot, 0)


def shards(train_weights, row_offset, block_group):
    train_n = lax.axis_size("train")
    serve_n = lax.axis_size("serve")
    layers, buffer_len, columns = train_weights.shape
    blocks_dev = block_group.shape[1]
    base = (blocks_dev + serve_n - 1) // serve_n
    slots = base + 1
    full = columns // LANES
    rem = columns - full * LANES
    pairs = layers // PAIR
    listed = layers // 2
    pieces = PAIR * base * full + (1 if rem else 0)
    pieces_list = listed * full + (1 if rem else 0)
    rests = max(PAIR * base, listed)
    spots = serve_n * layers
    width = columns * serve_n
    dtype = train_weights.dtype
    dims = (full, rem, columns, serve_n)
    assert SHIFT == BLOCK and buffer_len % BLOCK == 0
    assert rests * rem <= LANES and layers % PAIR == 0 and slots <= layers and pairs > 2

    group_ids = block_group[:, :, 0]
    smem = pl.BlockSpec(memory_space=pltpu.SMEM)
    vmem = pl.BlockSpec(memory_space=pltpu.VMEM)
    anywhere = pl.BlockSpec(memory_space=pl.ANY)
    hbm = pl.BlockSpec(memory_space=pltpu.HBM)
    codes, scales, tail, shared_codes, shared_scale, second, longest = pl.pallas_call(
        functools.partial(move_kernel, dims, base),
        in_specs=[hbm, hbm, hbm],
        out_specs=[vmem, vmem, vmem, vmem, vmem, hbm, hbm],
        out_shape=[
            pltpu.VMEM((layers - PAIR, base, BLOCK, width), dtype),
            pltpu.VMEM((layers - PAIR, slots, width), jnp.float32),
            pltpu.VMEM((serve_n, pieces, BLOCK, LANES), dtype),
            pltpu.VMEM((listed + 1, BLOCK, width), dtype),
            pltpu.VMEM((listed + 1, 1, width), jnp.float32),
            jax.ShapeDtypeStruct((serve_n, 2, pieces_list, BLOCK, LANES), dtype),
            jax.ShapeDtypeStruct((1, 1), jnp.int32),
        ],
        scratch_shapes=[
            pltpu.VMEM((serve_n, pieces_list, BLOCK, LANES), dtype),
            pltpu.VMEM((serve_n, base * full, BLOCK, LANES), dtype),
            pltpu.VMEM((serve_n, pairs - 1, pieces, BLOCK, LANES), dtype),
            pltpu.VMEM((serve_n, RING, pieces, BLOCK, LANES), dtype),
            pltpu.VMEM((PAIR, columns, buffer_len), dtype),
            pltpu.VMEM((buffer_len // BLOCK, BLOCK, columns), dtype),
            pltpu.VMEM((serve_n + 1, rests, BLOCK, LANES), dtype),
            pltpu.VMEM((layers, 2, SHIFT, columns), dtype),
            pltpu.VMEM((layers, 2, SHIFT, columns), dtype),
            pltpu.VMEM((serve_n * layers + 1, BLOCK, columns), dtype),
            pltpu.VMEM((serve_n, 2, pieces_list, BLOCK, LANES), dtype),
            pltpu.VMEM((serve_n, BLOCK, LANES), jnp.float32),
            pltpu.VMEM((serve_n, 1, LANES), jnp.float32),
            pltpu.VMEM((PAIR * base, 1, width), jnp.float32),
            pltpu.VMEM((layers + 8, spots), jnp.int32),
            pltpu.SMEM((layers + 8, spots), jnp.int32),
            pltpu.VMEM((train_n, 8, LANES), jnp.float32),
            pltpu.VMEM((train_n, 2, 8, LANES), jnp.float32),
            pltpu.SMEM((1, 1), jnp.int32),
            pltpu.SMEM((train_n + 1, layers), jnp.int32),
            pltpu.VMEM((layers, blocks_dev), jnp.int32),
            pltpu.SemaphoreType.DMA((PAIR,)),
            pltpu.SemaphoreType.DMA,
            pltpu.SemaphoreType.DMA((2,)),
            pltpu.SemaphoreType.DMA((RING, PAIR)),
            pltpu.SemaphoreType.DMA((TURNS, PAIR)),
            pltpu.SemaphoreType.DMA((2, 2)),
            pltpu.SemaphoreType.DMA((2, 2)),
            pltpu.SemaphoreType.DMA((serve_n.bit_length() - 1,)),
            pltpu.SemaphoreType.DMA((serve_n.bit_length() - 1,)),
            pltpu.SemaphoreType.DMA((2,)),
            pltpu.SemaphoreType.DMA((train_n, 2)),
            pltpu.SemaphoreType.DMA((2,)),
        ],
        compiler_params=pltpu.CompilerParams(
            collective_id=0, has_side_effects=True, vmem_limit_bytes=36 * MIB
        ),
        name="move",
    )(pltpu.with_memory_space_constraint(row_offset.T, pltpu.HBM), group_ids, jnp.swapaxes(train_weights, 1, 2))

    codes_shape = jax.ShapeDtypeStruct((layers, slots, BLOCK, width), dtype)
    scales_shape = jax.ShapeDtypeStruct((layers, slots, width), jnp.float32)
    rest_scratch = [
        pltpu.VMEM((serve_n, BLOCK, LANES), jnp.float32),
        pltpu.VMEM((serve_n, 1, LANES), jnp.float32),
        pltpu.VMEM((layers, LANES), jnp.int32),
        pltpu.SMEM((layers, LANES), jnp.int32),
    ]
    codes_out, scales_out = pl.pallas_call(
        functools.partial(write_kernel, dims, base),
        in_specs=[vmem, anywhere, vmem, vmem, vmem, vmem],
        out_specs=[hbm, hbm],
        out_shape=[codes_shape, pltpu.HBM((layers, slots, width), jnp.float32)],
        scratch_shapes=[
            pltpu.VMEM((layers, slots, width), jnp.float32),
            pltpu.VMEM((PAIR, base, BLOCK, width), dtype),
            pltpu.VMEM((PAIR * base, 1, width), jnp.float32),
            *rest_scratch,
            pltpu.SemaphoreType.DMA((layers + 1,)),
            pltpu.SemaphoreType.DMA((layers,)),
            pltpu.SemaphoreType.DMA,
        ],
        compiler_params=pltpu.CompilerParams(vmem_limit_bytes=10 * MIB),
        name="write",
    )(group_ids, codes, scales, tail, shared_codes, shared_scale)

    def late(state):
        got = lax.all_to_all(second, "serve", split_axis=0, concat_axis=0, tiled=True)
        late_codes, late_scales = pl.pallas_call(
            functools.partial(late_kernel, dims, base),
            in_specs=[vmem, vmem, hbm, hbm],
            out_specs=[hbm, hbm],
            out_shape=[codes_shape, scales_shape],
            input_output_aliases={2: 0, 3: 1},
            scratch_shapes=[
                pltpu.VMEM((BLOCK, width), dtype),
                pltpu.VMEM((1, width), jnp.float32),
                pltpu.VMEM((slots, width), jnp.float32),
                *rest_scratch,
                pltpu.SemaphoreType.DMA,
            ],
            compiler_params=pltpu.CompilerParams(vmem_limit_bytes=6 * MIB),
            name="late",
        )(group_ids, got, state[1], state[2])
        return jnp.zeros((), jnp.int32), late_codes, late_scales

    state = (longest[0, 0], codes_out, scales_out)
    _, codes_out, scales_out = lax.while_loop(lambda now: now[0] > listed, late, state)
    return (
        codes_out.reshape(layers, 1, 1, slots, BLOCK, width),
        scales_out.reshape(layers, 1, 1, slots, width),
    )


def solution(mesh):
    return jax.shard_map(
        shards,
        mesh=mesh,
        in_specs=(P(None, "train", "serve"), P(), P(None, "train", None)),
        out_specs=(
            P(None, "serve", "train", None, None, None),
            P(None, "serve", "train", None, None),
        ),
        check_vma=False,
    )
```

```python
import functools

import jax
import jax.numpy as jnp
from jax import lax
from jax.experimental import pallas as pl
from jax.experimental.pallas import tpu as pltpu
from jax.sharding import PartitionSpec as P

BLOCK = 32
SHIFT = 32
LANES = 128
PAIR = 2
RING = 3
TURNS = 4
MESH = pl.DeviceIdType.MESH
MIB = 1024 * 1024


def turned(values):
    return jnp.transpose(values.astype(jnp.float32))


def partner(me, mask, count):
    out, bit = 0, 1
    while bit < count:
        out = out + ((me // bit + mask // bit) % 2) * bit
        bit *= 2
    return out


def scaled(values):
    values = values.astype(jnp.float32)
    divisor = jnp.maximum(jnp.max(jnp.abs(values), axis=0, keepdims=True), 0.25)
    return values * (1.0 / divisor), divisor


def scale_rest(dims, count, recv, rem_code, rem_scale):
    full, rem, columns, sources = dims
    if rem:
        for s in range(sources):
            rem_code[s], rem_scale[s] = scaled(recv(s, count * full))


def scale_slot(dims, i, recv, rem_code, rem_scale, put_code, put_scale, place=None):
    place = i if place is None else place
    full, rem, columns, sources = dims
    width = columns * sources
    tiles = -(-width // LANES)
    lane = lax.broadcasted_iota(jnp.int32, (BLOCK, LANES), 1)
    lane_row = lax.broadcasted_iota(jnp.int32, (1, LANES), 1)
    parts = [None] * tiles

    def put(tile, low, code, scale):
        if tile >= tiles:
            return
        if parts[tile] is None:
            parts[tile] = (code, scale)
        else:
            before = parts[tile]
            parts[tile] = (jnp.where(lane >= low, code, before[0]), jnp.where(lane_row >= low, scale, before[1]))

    def flush(below):
        for tile in range(below):
            if parts[tile] is not None:
                code, scale = parts[tile]
                end = min(width, (tile + 1) * LANES)
                size = end - tile * LANES
                put_code(tile * LANES, end, code[:, :size])
                put_scale(tile * LANES, end, scale[:, :size])
                parts[tile] = None

    for s in range(sources):
        for t in range(full + (1 if rem else 0)):
            start = s * columns + t * LANES
            size = LANES if t < full else rem
            low = start % LANES
            if t < full:
                code, scale = scaled(recv(s, i * full + t))
                if low:
                    code, scale = pltpu.roll(code, low, 1), pltpu.roll(scale, low, 1)
            else:
                turn = lax.rem(low + LANES - place * rem, LANES)
                code, scale = pltpu.roll(rem_code[s], turn, 1), pltpu.roll(rem_scale[s], turn, 1)
            tile = start // LANES
            put(tile, low, code, scale)
            if low + size > LANES:
                put(tile + 1, 0, code, scale)
            flush((start + size) // LANES)
    flush(tiles)


def move_kernel(
    dims,
    base,
    offset_hbm,
    group_hbm,
    wt_ref,
    codes_ref,
    scale_ref,
    tail_ref,
    shared_codes,
    shared_scale,
    second_ref,
    longest_ref,
    all_ref,
    turned_ref,
    recv_ref,
    send_ref,
    in_ref,
    w_ref,
    rem_ref,
    edge_ref,
    halo_ref,
    over_ref,
    list_ref,
    rem_code,
    rem_scale,
    rows,
    table_ref,
    table_smem,
    length_ref,
    lengths_ref,
    longest_smem,
    offset_ref,
    group_ref,
    in_sem,
    table_sem,
    small_sem,
    send_sem,
    recv_sem,
    halo_send,
    halo_recv,
    list_send,
    list_recv,
    length_send,
    length_recv,
    second_sem,
):
    full, rem, columns, groups = dims
    slots = base + 1
    pairs = recv_ref.shape[1] + 1
    layers = pairs * PAIR
    listed = layers // 2
    blocks = w_ref.shape[0]
    buffer_len = blocks * BLOCK
    rows_dev = buffer_len - 2 * SHIFT
    me = lax.axis_index("serve")
    part = lax.axis_index("train")
    parts_n = lax.axis_size("train")
    half = base * full
    rest = half + (1 if rem else 0)
    ahead = base > 2

    def fetch(layer, sub):
        return pltpu.make_async_copy(wt_ref.at[layer], in_ref.at[sub], in_sem.at[sub])

    def landing(source, pair, sub, final):
        if ahead and isinstance(pair, int) and pair == 0 and sub == 0:
            return turned_ref.at[source]
        return tail_ref.at[source] if final else recv_ref.at[source, pair]

    def message(mask, pair, sub, final, slots_of=None):
        peer = partner(me, mask, groups)
        span = pl.ds(sub * half, rest if sub == PAIR - 1 else half)
        if slots_of is not None:
            span = pl.ds(slots_of[0] * full, (slots_of[1] - slots_of[0]) * full)
        return pltpu.make_async_remote_copy(
            send_ref.at[peer, pair % RING, span],
            landing(me, pair, sub, final).at[span],
            send_sem.at[pair % RING, sub],
            recv_sem.at[pair % TURNS, sub],
            device_id={"serve": peer},
            device_id_type=MESH,
        )

    def arrival(pair, sub, final):
        span = pl.ds(sub * half, rest if sub == PAIR - 1 else half)
        others = pl.ds(0, groups - 1)
        place = tail_ref.at[others, span] if final else recv_ref.at[others, pair, span]
        return pltpu.make_async_copy(place, place, recv_sem.at[pair % TURNS, sub])

    def departure(pair, sub):
        span = pl.ds(sub * half, rest if sub == PAIR - 1 else half)
        place = send_ref.at[pl.ds(0, groups - 1), pair % RING, span]
        return pltpu.make_async_copy(place, place, send_sem.at[pair % RING, sub])

    bits = [1 << n for n in range(groups.bit_length() - 1)]
    orders = [bits[1:], bits[:0:-1]]
    pieces_list = all_ref.shape[1]
    spans = [pl.ds(0, pieces_list // 2), pl.ds(pieces_list // 2, pieces_list - pieces_list // 2)]

    def stage(number):
        for which, order in enumerate(orders):
            if number < 0:
                yield which, 0, 0
                continue
            held = [0]
            for bit in order[:number]:
                held = held + [mask + bit for mask in held]
            for mask in held:
                yield which, order[number], mask

    def list_message(number, which, bit, mask):
        place = all_ref.at[partner(me, mask, groups), spans[which]]
        return pltpu.make_async_remote_copy(
            place,
            place,
            list_send.at[number],
            list_recv.at[number],
            device_id={"serve": partner(me, bit, groups)},
            device_id_type=MESH,
        )

    def lists_passed(number, sem):
        place = all_ref.at[pl.ds(0, 1 << number)]
        return pltpu.make_async_copy(place, place, sem.at[number])

    def edge(layer, side):
        to = part + 1 if side == 0 else part - 1
        return pltpu.make_async_remote_copy(
            edge_ref.at[layer, side],
            halo_ref.at[layer, side],
            halo_send.at[layer % 2, side],
            halo_recv.at[layer % 2, side],
            device_id={"train": to},
            device_id_type=MESH,
        )

    def length_message(turn, side):
        return pltpu.make_async_remote_copy(
            length_ref.at[turn],
            lengths_ref.at[turn, side],
            length_send.at[side],
            length_recv.at[turn, side],
            device_id={"train": part + 1 if side == 0 else part - 1},
            device_id_type=MESH,
        )

    lengths_ref[...] = jnp.zeros(lengths_ref.shape, jnp.float32)
    barrier = pltpu.get_barrier_semaphore()

    def greet(mask, carry):
        pl.semaphore_signal(barrier, inc=1, device_id={"serve": partner(me, mask, groups)}, device_id_type=MESH)
        return carry

    lax.fori_loop(1, groups, greet, 0)

    @pl.when(part > 0)
    def _():
        pl.semaphore_signal(barrier, inc=1, device_id={"train": part - 1}, device_id_type=MESH)

    @pl.when(part < parts_n - 1)
    def _():
        pl.semaphore_signal(barrier, inc=1, device_id={"train": part + 1}, device_id_type=MESH)

    get_group = pltpu.make_async_copy(group_hbm, group_ref, small_sem.at[0])
    get_group.start()
    fetch(0, 0).start()
    get_offset = pltpu.make_async_copy(offset_hbm, offset_ref, small_sem.at[1])
    get_offset.start()
    for sub in range(1, PAIR):
        fetch(sub, sub).start()

    below = (part + parts_n - 1) // parts_n
    above = (2 * parts_n - 2 - part) // parts_n

    row = lax.broadcasted_iota(jnp.int32, (BLOCK, columns), 0)
    lane = lax.broadcasted_iota(jnp.int32, (BLOCK, LANES), 1)
    last = rows_dev - BLOCK

    def transpose_tile(sub, low):
        high = min(low + LANES, buffer_len)
        rows_of = turned(in_ref[sub, :, low:high]).astype(w_ref.dtype)
        w_ref[low // BLOCK : high // BLOCK] = rows_of.reshape((high - low) // BLOCK, BLOCK, columns)

    def joined(group, count):
        tile = rem_ref[group, 0].astype(jnp.float32)
        for i in range(1, count):
            moved = pltpu.roll(rem_ref[group, i].astype(jnp.float32), i * rem, 1)
            tile = jnp.where(lane >= i * rem, moved, tile)
        return tile

    def edge_ends(layer, act):
        @pl.when(part < parts_n - 1)
        def _():
            act(edge(layer, 0))

        @pl.when(part > 0)
        def _():
            act(edge(layer, 1))

    def store_edges(layer, sub):
        fetch(layer, sub).wait()
        low = (buffer_len - 1) // LANES * LANES
        edge_ref[layer, 0] = turned(in_ref[sub, :, low:buffer_len])[-SHIFT:].astype(edge_ref.dtype)
        edge_ref[layer, 1] = turned(in_ref[sub, :, 0:LANES])[:SHIFT].astype(edge_ref.dtype)


    def send_edges(layer, sub):
        store_edges(layer, sub)

        @pl.when(layer >= 2)
        def _():
            edge_ends(layer - 2, lambda copy: copy.wait_send())

        edge_ends(layer, lambda copy: copy.start())

    def turn_layer(pair, sub):
        layer = pair * PAIR + sub
        for low in range(0, buffer_len, LANES):
            transpose_tile(sub, low)

        @pl.when(layer + PAIR < layers)
        def _():
            fetch(layer + PAIR, sub).start()

        w_ref[0] = jnp.zeros((BLOCK, columns), w_ref.dtype)

    def finish_layer(pair, sub):
        layer = pair * PAIR + sub
        base_row = part * rows_dev

        @pl.when(part > 0)
        def _():
            edge(layer, 0).wait_recv()
            first = offset_ref[part, layer] - base_row
            head = jnp.where(row < first, halo_ref[layer, 0].astype(jnp.float32), w_ref[1].astype(jnp.float32))
            w_ref[1] = head.astype(w_ref.dtype)

        @pl.when(part < parts_n - 1)
        def _():
            edge(layer, 1).wait_recv()
            after = offset_ref[part + 1, layer] - base_row
            tail = w_ref[blocks - 2].astype(jnp.float32)
            tail = jnp.where(row + last >= after, halo_ref[layer, 1].astype(jnp.float32), tail)
            w_ref[blocks - 2] = tail.astype(w_ref.dtype)

        def last_slots(group, carry):
            over_ref[layer * groups + group] = w_ref[table_smem[layer, group * layers + base]]
            return carry

        lax.fori_loop(0, groups, last_slots, 0)

    def prepare(pair, sub):
        turn_layer(pair, sub)
        finish_layer(pair, sub)

    def gather(pair, sub, group, out, slots_of=None):
        for k in range(*(slots_of or (0, base))):
            block = w_ref[table_smem[pair * PAIR + sub, group * layers + k]]
            for t in range(full):
                out[(sub * base + k) * full + t] = block[:, t * LANES : (t + 1) * LANES]
            if rem:
                rem_ref[group, sub * base + k, :, 0:rem] = block[:, full * LANES :]
        if rem and sub == PAIR - 1:
            out[PAIR * half] = joined(group, PAIR * base).astype(out.dtype)

    def give(low, high, pair, sub, pack, send, final, slots_of=None):
        def one(mask, carry):
            peer = partner(me, mask, groups)
            if pack:
                gather(pair, sub, peer, send_ref.at[peer, pair % RING], slots_of)
            if send:
                message(mask, pair, sub, final, slots_of).start()
            return carry

        lax.fori_loop(low, high, one, 0)

    def own(pair, sub, final):
        gather(pair, sub, me, landing(me, pair, sub, final))

    def pack_list(entry_of, out):
        for e in range(listed):
            block = over_ref[entry_of(e)]
            for t in range(full):
                out[e * full + t] = block[:, t * LANES : (t + 1) * LANES]
            if rem:
                rem_ref[groups, e, :, 0:rem] = block[:, full * LANES :]
        if rem:
            out[listed * full] = joined(groups, listed).astype(out.dtype)

    def take(pair, final):
        for sub in range(PAIR):
            arrival(pair, sub, final).wait()

    def unpack(pair):
        def recv(s, n):
            return recv_ref[s, pair, n]

        scale_rest(dims, PAIR * base, recv, rem_code, rem_scale)

        def slot(i, carry):
            def put_code(low, high, code):
                codes_ref[pair * PAIR + i // base, i % base, :, low:high] = code.astype(codes_ref.dtype)

            def put_scale(low, high, scale):
                rows[i, :, low:high] = scale

            place = i
            if ahead:
                place = table_smem[layers + 2, me * layers + jnp.minimum(i, base - 1)]
                place = jnp.where((pair == 0) & (i < base), place, i)
            scale_slot(dims, i, recv, rem_code, rem_scale, put_code, put_scale, place)
            return carry

        lax.fori_loop(0, PAIR * base, slot, 0)
        for i in range(PAIR * base):
            scale_ref[pair * PAIR + i // base, i % base : i % base + 1, :] = rows[i]

    def sent(pair):
        for sub in range(PAIR):
            departure(pair, sub).wait()

    def step(pair, carry):
        @pl.when(pair >= RING)
        def _():
            sent(pair - RING)

        for sub in range(PAIR):
            prepare(pair, sub)
            give(2, groups, pair, sub, True, True, False)
            give(1, 2, pair, sub, True, True, False)
            own(pair, sub, False)
            send_edges(pair * PAIR + sub + 1, (sub + 1) % PAIR)

        take(pair - 1, False)
        if ahead:

            @pl.when(pair == 1)
            def _():
                def restore(source, inner):
                    for k in range(base):
                        place = table_smem[layers + 2, me * layers + k]
                        for t in range(full):
                            recv_ref[source, 0, k * full + t] = turned_ref[source, place * full + t]
                    return inner

                lax.fori_loop(0, groups, restore, 0)

        unpack(pair - 1)
        return carry

    get_group.wait()
    spot = lax.broadcasted_iota(jnp.int32, (layers, groups * layers), 1)
    spot_group = jnp.zeros(spot.shape, jnp.int32)
    for g in range(1, groups):
        spot_group = spot_group + jnp.where(spot >= g * layers, 1, 0)
    spot_slot = spot - spot_group * layers
    seen = jnp.zeros(spot.shape, jnp.int32)
    table = jnp.zeros(spot.shape, jnp.int32)
    moved = jnp.zeros((1, groups * layers), jnp.int32)
    for j in range(group_ref.shape[1]):
        mine = group_ref[:, j : j + 1] == spot_group
        table = jnp.where(mine & (seen == spot_slot), j + 1, table)
        moved = jnp.where(mine[0:1, :] & (seen[0:1, :] + 1 == spot_slot[0:1, :]), j + 1, moved)
        seen = jnp.where(mine, seen + 1, seen)
    table_ref[0:layers, :] = table
    if ahead:
        count, k = seen[0:1, :], spot_slot[0:1, :]
        final_block = group_ref.shape[1]
        turns = (group_ref[0:1, final_block - 1 : final_block] == spot_group[0:1, :]) & (count <= base)
        turned_row = jnp.where(k == 0, final_block, jnp.where(k < count, moved, 0))
        table_ref[0:1, :] = jnp.where(turns, turned_row, table[0:1, :])
        position = jnp.where(k == count - 1, 0, jnp.where(k < count, k + 1, k))
        table_ref[layers + 2 : layers + 3, :] = jnp.where(turns, position, k)
    none = layers * groups
    length = jnp.zeros((1, groups * layers), jnp.int32)
    entry = jnp.full(length.shape, none, jnp.int32)
    total = jnp.zeros((1, LANES), jnp.int32)
    shared = jnp.full(total.shape, none, jnp.int32)
    number = lax.broadcasted_iota(jnp.int32, total.shape, 1)
    long = jnp.where(seen == slots, 1, 0)
    for n in range(layers):
        here = long[n : n + 1, :]
        entry = jnp.where((here > 0) & (length == spot_slot[0:1, :]), n * groups + spot_group[0:1, :], entry)
        length = length + here
        for g in range(groups):
            one = jnp.broadcast_to(here[:, g * layers : g * layers + 1], total.shape)
            shared = jnp.where((one > 0) & (total == number), n * groups + g, shared)
            total = total + one
    table_ref[layers : layers + 1, :] = entry
    table_ref[layers + 1 : layers + 2, 0:LANES] = shared
    to_smem = pltpu.make_async_copy(table_ref, table_smem, table_sem)
    to_smem.start()
    most = jnp.broadcast_to(total.astype(jnp.float32), length_ref.shape[1:])
    over_ref[none] = jnp.zeros((BLOCK, columns), over_ref.dtype)

    end = pairs - 1
    store_edges(0, 0)
    turn_layer(0, 0)
    to_smem.wait()
    pl.semaphore_wait(barrier, groups - 1 + below + above)
    edge_ends(0, lambda copy: copy.start())
    get_offset.wait()
    for sub in range(PAIR):
        if sub > 0:
            turn_layer(0, sub)
        if sub == 0 and ahead:
            give(2, groups, 0, sub, True, True, False, (2, base))
            finish_layer(0, sub)
            give(2, groups, 0, sub, True, True, False, (0, 2))
            give(1, 2, 0, sub, True, True, False)
        else:
            finish_layer(0, sub)
            give(2, groups, 0, sub, True, True, False)
            give(1, 2, 0, sub, True, True, False)
        own(0, sub, False)
        send_edges(sub + 1, (sub + 1) % PAIR)
    lax.fori_loop(1, end, step, 0)

    if end >= RING:
        sent(end - RING)
    for sub in range(PAIR):
        prepare(end, sub)
        give(1, groups, end, sub, True, False, True)
        own(end, sub, True)
        if sub < PAIR - 1:
            send_edges(end * PAIR + sub + 1, sub + 1)
    pack_list(lambda e: table_smem[layers + 1, e], all_ref.at[me])
    high = len(bits) - 1
    for copy in stage(0):
        list_message(0, *copy).start()
    for which in range(2):
        list_message(high, which, 1, 0).start()
    for sub in range(PAIR - 1):
        give(2, groups, end, sub, False, True, True)
        give(1, 2, end, sub, False, True, True)

    def second(group, carry):
        for which in range(2):
            pack_list(lambda e: table_smem[layers, group * layers + which * listed + e], list_ref.at[group, which])
        return carry

    lax.fori_loop(0, groups, second, 0)
    keep = pltpu.make_async_copy(list_ref, second_ref, second_sem.at[0])
    keep.start()
    for n in range(2):
        edge_ends(layers - 1 - n, lambda copy: copy.wait_send())

    def to_neighbours(turn, act):
        @pl.when(part < parts_n - 1)
        def _():
            act(length_message(turn, 0))

        @pl.when(part > 0)
        def _():
            act(length_message(turn, 1))

    def from_neighbours(turn):
        @pl.when(part > 0)
        def _():
            length_message(turn, 0).wait_recv()

        @pl.when(part < parts_n - 1)
        def _():
            length_message(turn, 1).wait_recv()

    for turn in range(parts_n - 1):
        length_ref[turn] = most
        to_neighbours(turn, lambda copy: copy.start())
        from_neighbours(turn)
        for side in range(2):
            most = jnp.maximum(most, lengths_ref[turn, side])
        to_neighbours(turn, lambda copy: copy.wait_send())
    longest_smem[0, 0] = jnp.max(most).astype(jnp.int32)
    tell = pltpu.make_async_copy(longest_smem, longest_ref, second_sem.at[1])
    tell.start()

    take(end - 1, False)
    unpack(end - 1)
    for number in range(1, high + 1):
        lists_passed(number - 1, list_recv).wait()
        if number < high:
            for copy in stage(number):
                list_message(number, *copy).start()
        for which, bit, mask in stage(number - 1):
            list_message(high, which, 1, bit + mask).start()
        if number == 1:
            give(groups * 3 // 4, groups, end, PAIR - 1, False, True, True)
            give(1, groups * 3 // 4, end, PAIR - 1, False, True, True)
    lists_passed(high, list_recv).wait()

    def recv(s, n):
        return all_ref[s, n]

    scale_rest(dims, listed, recv, rem_code, rem_scale)

    def listed_slot(e, carry):
        def put_code(low, high, code):
            shared_codes[e, :, low:high] = code.astype(shared_codes.dtype)

        def put_scale(low, high, scale):
            shared_scale[e, :, low:high] = scale

        scale_slot(dims, e, recv, rem_code, rem_scale, put_code, put_scale)
        return carry

    lax.fori_loop(0, listed, listed_slot, 0)
    shared_codes[listed] = jnp.zeros(shared_codes.shape[1:], shared_codes.dtype)
    shared_scale[listed] = jnp.zeros(shared_scale.shape[1:], jnp.float32)

    keep.wait()
    tell.wait()
    for number in range(high + 1):
        lists_passed(number, list_send).wait()
    for pair in range(max(0, end - RING + 1), end + 1):
        sent(pair)
    take(end, True)


def list_places(group_ref, place_ref, slots, groups, shared):
    layers = group_ref.shape[0]
    me = lax.axis_index("serve")
    count = jnp.sum(jnp.where(group_ref[...] == me, 1, 0), axis=1, keepdims=True)
    ahead = jnp.zeros((layers, 1), jnp.int32)
    every = jnp.where(count == slots, 1, 0)
    if shared:
        every = jnp.zeros((layers, 1), jnp.int32)
        for g in range(groups):
            filled = jnp.sum(jnp.where(group_ref[...] == g, 1, 0), axis=1, keepdims=True)
            one = jnp.where(filled == slots, 1, 0)
            ahead = ahead + jnp.where(g < me, one, 0)
            every = every + one
    length = jnp.zeros((1, 1), jnp.int32)
    for n in range(layers):
        place = jnp.where(count[n : n + 1, :] == slots, length + ahead[n : n + 1, :], layers * groups)
        place_ref[n : n + 1, :] = jnp.broadcast_to(place, (1, place_ref.shape[1]))
        length = length + every[n : n + 1, :]
    return count


def write_kernel(
    dims,
    base,
    group_ref,
    codes_ref,
    scale_ref,
    tail_ref,
    shared_codes,
    shared_scale,
    codes_out,
    scale_out,
    scales,
    codes,
    rows,
    rem_code,
    rem_scale,
    place_ref,
    place_smem,
    sems,
    last_sems,
    place_sem,
):
    groups = dims[3]
    layers = scale_out.shape[0]
    done = layers - PAIR
    listed = layers // 2
    copies = [pltpu.make_async_copy(codes_ref.at[n], codes_out.at[n, pl.ds(0, base)], sems.at[n]) for n in range(done)]
    for copy in copies:
        copy.start()
    count = list_places(group_ref, place_ref, base + 1, groups, True)
    to_smem = pltpu.make_async_copy(place_ref, place_smem, place_sem)
    to_smem.start()

    def recv(s, n):
        return tail_ref[s, n]

    scale_rest(dims, PAIR * base, recv, rem_code, rem_scale)

    def last_pair(sub):
        def slot(k, carry):
            def put_code(low, high, code):
                codes[sub, k, :, low:high] = code.astype(codes.dtype)

            def put_scale(low, high, scale):
                rows[sub * base + k, :, low:high] = scale

            scale_slot(dims, sub * base + k, recv, rem_code, rem_scale, put_code, put_scale)
            return carry

        lax.fori_loop(0, base, slot, 0)
        copies.append(pltpu.make_async_copy(codes.at[sub], codes_out.at[done + sub, pl.ds(0, base)], sems.at[done + sub]))
        copies[-1].start()

    last_pair(0)
    to_smem.wait()
    places = [jnp.minimum(place_smem[n, 0], listed) for n in range(layers)]
    for n in range(layers):
        copies.append(pltpu.make_async_copy(shared_codes.at[places[n]], codes_out.at[n, base], last_sems.at[n]))
        copies[-1].start()
    for sub in range(1, PAIR):
        last_pair(sub)
    slot = lax.broadcasted_iota(jnp.int32, scales.shape[1:], 0)
    for sub in range(PAIR):
        for k in range(base):
            scales[done + sub, k : k + 1, :] = rows[sub * base + k]
    for n in range(layers):
        scale = scale_ref[n] if n < done else scales[n]
        scale = jnp.where(slot < count[n : n + 1, :], scale, 0.0)
        scales[n] = jnp.where(slot < base, scale, jnp.broadcast_to(shared_scale[places[n]], scale.shape))
    copies.append(pltpu.make_async_copy(scales, scale_out, sems.at[layers]))
    copies[-1].start()
    for copy in copies:
        copy.wait()


def late_kernel(
    dims,
    base,
    group_ref,
    got_ref,
    codes_in,
    scale_in,
    codes_out,
    scale_out,
    extra,
    extra_scale,
    scales,
    rem_code,
    rem_scale,
    place_ref,
    place_smem,
    sem,
):
    del codes_in, scale_in
    full, rem, columns, groups = dims
    layers = codes_out.shape[0]
    listed = layers // 2
    list_places(group_ref, place_ref, base + 1, groups, False)
    to_smem = pltpu.make_async_copy(place_ref, place_smem, sem)
    to_smem.start()
    to_smem.wait()
    slot = lax.broadcasted_iota(jnp.int32, scales.shape, 0)
    for which in range(2):

        def recv(s, n, which=which):
            return got_ref[s, which, n]

        scale_rest(dims, listed, recv, rem_code, rem_scale)

        def last_slot(layer, carry, which=which, recv=recv):
            place = place_smem[layer, 0] - which * listed

            @pl.when((place >= 0) & (place < listed))
            def _():
                def put_code(low, high, code):
                    extra[:, low:high] = code.astype(extra.dtype)

                def put_scale(low, high, scale):
                    extra_scale[:, low:high] = scale

                scale_slot(dims, place, recv, rem_code, rem_scale, put_code, put_scale)
                pltpu.sync_copy(extra, codes_out.at[layer, base])
                pltpu.sync_copy(scale_out.at[layer], scales)
                scales[...] = jnp.where(slot < base, scales[...], jnp.broadcast_to(extra_scale[...], scales.shape))
                pltpu.sync_copy(scales, scale_out.at[layer])

            return carry

        lax.fori_loop(0, layers, last_slot, 0)


def shards(train_weights, row_offset, block_group):
    train_n = lax.axis_size("train")
    serve_n = lax.axis_size("serve")
    layers, buffer_len, columns = train_weights.shape
    blocks_dev = block_group.shape[1]
    base = (blocks_dev + serve_n - 1) // serve_n
    slots = base + 1
    full = columns // LANES
    rem = columns - full * LANES
    pairs = layers // PAIR
    listed = layers // 2
    pieces = PAIR * base * full + (1 if rem else 0)
    pieces_list = listed * full + (1 if rem else 0)
    rests = max(PAIR * base, listed)
    spots = serve_n * layers
    width = columns * serve_n
    dtype = train_weights.dtype
    dims = (full, rem, columns, serve_n)
    assert SHIFT == BLOCK and buffer_len % BLOCK == 0
    assert rests * rem <= LANES and layers % PAIR == 0 and slots <= layers and pairs > 2

    group_ids = block_group[:, :, 0]
    smem = pl.BlockSpec(memory_space=pltpu.SMEM)
    vmem = pl.BlockSpec(memory_space=pltpu.VMEM)
    anywhere = pl.BlockSpec(memory_space=pl.ANY)
    hbm = pl.BlockSpec(memory_space=pltpu.HBM)
    codes, scales, tail, shared_codes, shared_scale, second, longest = pl.pallas_call(
        functools.partial(move_kernel, dims, base),
        in_specs=[hbm, hbm, hbm],
        out_specs=[vmem, vmem, vmem, vmem, vmem, hbm, hbm],
        out_shape=[
            pltpu.VMEM((layers - PAIR, base, BLOCK, width), dtype),
            pltpu.VMEM((layers - PAIR, slots, width), jnp.float32),
            pltpu.VMEM((serve_n, pieces, BLOCK, LANES), dtype),
            pltpu.VMEM((listed + 1, BLOCK, width), dtype),
            pltpu.VMEM((listed + 1, 1, width), jnp.float32),
            jax.ShapeDtypeStruct((serve_n, 2, pieces_list, BLOCK, LANES), dtype),
            jax.ShapeDtypeStruct((1, 1), jnp.int32),
        ],
        scratch_shapes=[
            pltpu.VMEM((serve_n, pieces_list, BLOCK, LANES), dtype),
            pltpu.VMEM((serve_n, base * full, BLOCK, LANES), dtype),
            pltpu.VMEM((serve_n, pairs - 1, pieces, BLOCK, LANES), dtype),
            pltpu.VMEM((serve_n, RING, pieces, BLOCK, LANES), dtype),
            pltpu.VMEM((PAIR, columns, buffer_len), dtype),
            pltpu.VMEM((buffer_len // BLOCK, BLOCK, columns), dtype),
            pltpu.VMEM((serve_n + 1, rests, BLOCK, LANES), dtype),
            pltpu.VMEM((layers, 2, SHIFT, columns), dtype),
            pltpu.VMEM((layers, 2, SHIFT, columns), dtype),
            pltpu.VMEM((serve_n * layers + 1, BLOCK, columns), dtype),
            pltpu.VMEM((serve_n, 2, pieces_list, BLOCK, LANES), dtype),
            pltpu.VMEM((serve_n, BLOCK, LANES), jnp.float32),
            pltpu.VMEM((serve_n, 1, LANES), jnp.float32),
            pltpu.VMEM((PAIR * base, 1, width), jnp.float32),
            pltpu.VMEM((layers + 8, spots), jnp.int32),
            pltpu.SMEM((layers + 8, spots), jnp.int32),
            pltpu.VMEM((train_n, 8, LANES), jnp.float32),
            pltpu.VMEM((train_n, 2, 8, LANES), jnp.float32),
            pltpu.SMEM((1, 1), jnp.int32),
            pltpu.SMEM((train_n + 1, layers), jnp.int32),
            pltpu.VMEM((layers, blocks_dev), jnp.int32),
            pltpu.SemaphoreType.DMA((PAIR,)),
            pltpu.SemaphoreType.DMA,
            pltpu.SemaphoreType.DMA((2,)),
            pltpu.SemaphoreType.DMA((RING, PAIR)),
            pltpu.SemaphoreType.DMA((TURNS, PAIR)),
            pltpu.SemaphoreType.DMA((2, 2)),
            pltpu.SemaphoreType.DMA((2, 2)),
            pltpu.SemaphoreType.DMA((serve_n.bit_length() - 1,)),
            pltpu.SemaphoreType.DMA((serve_n.bit_length() - 1,)),
            pltpu.SemaphoreType.DMA((2,)),
            pltpu.SemaphoreType.DMA((train_n, 2)),
            pltpu.SemaphoreType.DMA((2,)),
        ],
        compiler_params=pltpu.CompilerParams(
            collective_id=0, has_side_effects=True, vmem_limit_bytes=36 * MIB
        ),
        name="move",
    )(pltpu.with_memory_space_constraint(row_offset.T, pltpu.HBM), group_ids, jnp.swapaxes(train_weights, 1, 2))

    codes_shape = jax.ShapeDtypeStruct((layers, slots, BLOCK, width), dtype)
    scales_shape = jax.ShapeDtypeStruct((layers, slots, width), jnp.float32)
    rest_scratch = [
        pltpu.VMEM((serve_n, BLOCK, LANES), jnp.float32),
        pltpu.VMEM((serve_n, 1, LANES), jnp.float32),
        pltpu.VMEM((layers, LANES), jnp.int32),
        pltpu.SMEM((layers, LANES), jnp.int32),
    ]
    codes_out, scales_out = pl.pallas_call(
        functools.partial(write_kernel, dims, base),
        in_specs=[vmem, anywhere, vmem, vmem, vmem, vmem],
        out_specs=[hbm, hbm],
        out_shape=[codes_shape, pltpu.HBM((layers, slots, width), jnp.float32)],
        scratch_shapes=[
            pltpu.VMEM((layers, slots, width), jnp.float32),
            pltpu.VMEM((PAIR, base, BLOCK, width), dtype),
            pltpu.VMEM((PAIR * base, 1, width), jnp.float32),
            *rest_scratch,
            pltpu.SemaphoreType.DMA((layers + 1,)),
            pltpu.SemaphoreType.DMA((layers,)),
            pltpu.SemaphoreType.DMA,
        ],
        compiler_params=pltpu.CompilerParams(vmem_limit_bytes=10 * MIB),
        name="write",
    )(group_ids, codes, scales, tail, shared_codes, shared_scale)

    def late(state):
        got = lax.all_to_all(second, "serve", split_axis=0, concat_axis=0, tiled=True)
        late_codes, late_scales = pl.pallas_call(
            functools.partial(late_kernel, dims, base),
            in_specs=[vmem, vmem, hbm, hbm],
            out_specs=[hbm, hbm],
            out_shape=[codes_shape, scales_shape],
            input_output_aliases={2: 0, 3: 1},
            scratch_shapes=[
                pltpu.VMEM((BLOCK, width), dtype),
                pltpu.VMEM((1, width), jnp.float32),
                pltpu.VMEM((slots, width), jnp.float32),
                *rest_scratch,
                pltpu.SemaphoreType.DMA,
            ],
            compiler_params=pltpu.CompilerParams(vmem_limit_bytes=6 * MIB),
            name="late",
        )(group_ids, got, state[1], state[2])
        return jnp.zeros((), jnp.int32), late_codes, late_scales

    state = (longest[0, 0], codes_out, scales_out)
    _, codes_out, scales_out = lax.while_loop(lambda now: now[0] > listed, late, state)
    return (
        codes_out.reshape(layers, 1, 1, slots, BLOCK, width),
        scales_out.reshape(layers, 1, 1, slots, width),
    )


def solution(mesh):
    return jax.shard_map(
        shards,
        mesh=mesh,
        in_specs=(P(None, "train", "serve"), P(), P(None, "train", None)),
        out_specs=(
            P(None, "serve", "train", None, None, None),
            P(None, "serve", "train", None, None),
        ),
        check_vma=False,
    )
```

```python
import functools

import jax
import jax.numpy as jnp
from jax import lax
from jax.experimental import pallas as pl
from jax.experimental.pallas import tpu as pltpu
from jax.sharding import PartitionSpec as P

BLOCK = 32
SHIFT = 32
LANES = 128
PAIR = 2
RING = 3
TURNS = 4
MESH = pl.DeviceIdType.MESH
MIB = 1024 * 1024


def turned(values):
    return jnp.transpose(values.astype(jnp.float32))


def partner(me, mask, count):
    out, bit = 0, 1
    while bit < count:
        out = out + ((me // bit + mask // bit) % 2) * bit
        bit *= 2
    return out


def scaled(values):
    values = values.astype(jnp.float32)
    divisor = jnp.maximum(jnp.max(jnp.abs(values), axis=0, keepdims=True), 0.25)
    return values * (1.0 / divisor), divisor


def scale_rest(dims, count, recv, rem_code, rem_scale):
    full, rem, columns, sources = dims
    if rem:
        for s in range(sources):
            rem_code[s], rem_scale[s] = scaled(recv(s, count * full))


def scale_slot(dims, i, recv, rem_code, rem_scale, put_code, put_scale, place=None):
    place = i if place is None else place
    full, rem, columns, sources = dims
    width = columns * sources
    tiles = -(-width // LANES)
    lane = lax.broadcasted_iota(jnp.int32, (BLOCK, LANES), 1)
    lane_row = lax.broadcasted_iota(jnp.int32, (1, LANES), 1)
    parts = [None] * tiles

    def put(tile, low, code, scale):
        if tile >= tiles:
            return
        if parts[tile] is None:
            parts[tile] = (code, scale)
        else:
            before = parts[tile]
            parts[tile] = (jnp.where(lane >= low, code, before[0]), jnp.where(lane_row >= low, scale, before[1]))

    def flush(below):
        for tile in range(below):
            if parts[tile] is not None:
                code, scale = parts[tile]
                end = min(width, (tile + 1) * LANES)
                size = end - tile * LANES
                put_code(tile * LANES, end, code[:, :size])
                put_scale(tile * LANES, end, scale[:, :size])
                parts[tile] = None

    for s in range(sources):
        for t in range(full + (1 if rem else 0)):
            start = s * columns + t * LANES
            size = LANES if t < full else rem
            low = start % LANES
            if t < full:
                code, scale = scaled(recv(s, i * full + t))
                if low:
                    code, scale = pltpu.roll(code, low, 1), pltpu.roll(scale, low, 1)
            else:
                turn = lax.rem(low + LANES - place * rem, LANES)
                code, scale = pltpu.roll(rem_code[s], turn, 1), pltpu.roll(rem_scale[s], turn, 1)
            tile = start // LANES
            put(tile, low, code, scale)
            if low + size > LANES:
                put(tile + 1, 0, code, scale)
            flush((start + size) // LANES)
    flush(tiles)


def move_kernel(
    dims,
    base,
    offset_hbm,
    group_hbm,
    wt_ref,
    codes_ref,
    scale_ref,
    tail_ref,
    shared_codes,
    shared_scale,
    second_ref,
    longest_ref,
    all_ref,
    turned_ref,
    recv_ref,
    send_ref,
    in_ref,
    w_ref,
    rem_ref,
    edge_ref,
    halo_ref,
    over_ref,
    list_ref,
    rem_code,
    rem_scale,
    rows,
    table_ref,
    table_smem,
    length_ref,
    lengths_ref,
    longest_smem,
    offset_ref,
    group_ref,
    in_sem,
    table_sem,
    small_sem,
    send_sem,
    recv_sem,
    halo_send,
    halo_recv,
    list_send,
    list_recv,
    length_send,
    length_recv,
    second_sem,
):
    full, rem, columns, groups = dims
    slots = base + 1
    pairs = recv_ref.shape[1] + 1
    layers = pairs * PAIR
    listed = layers // 2
    blocks = w_ref.shape[0]
    buffer_len = blocks * BLOCK
    rows_dev = buffer_len - 2 * SHIFT
    me = lax.axis_index("serve")
    part = lax.axis_index("train")
    parts_n = lax.axis_size("train")
    half = base * full
    rest = half + (1 if rem else 0)
    ahead = base > 2

    def fetch(layer, sub):
        return pltpu.make_async_copy(wt_ref.at[layer], in_ref.at[sub], in_sem.at[sub])

    def landing(source, pair, sub, final):
        if ahead and isinstance(pair, int) and pair == 0 and sub == 0:
            return turned_ref.at[source]
        return tail_ref.at[source] if final else recv_ref.at[source, pair]

    def message(mask, pair, sub, final, slots_of=None):
        peer = partner(me, mask, groups)
        span = pl.ds(sub * half, rest if sub == PAIR - 1 else half)
        if slots_of is not None:
            span = pl.ds(slots_of[0] * full, (slots_of[1] - slots_of[0]) * full)
        return pltpu.make_async_remote_copy(
            send_ref.at[peer, pair % RING, span],
            landing(me, pair, sub, final).at[span],
            send_sem.at[pair % RING, sub],
            recv_sem.at[pair % TURNS, sub],
            device_id={"serve": peer},
            device_id_type=MESH,
        )

    def arrival(pair, sub, final):
        span = pl.ds(sub * half, rest if sub == PAIR - 1 else half)
        others = pl.ds(0, groups - 1)
        place = tail_ref.at[others, span] if final else recv_ref.at[others, pair, span]
        return pltpu.make_async_copy(place, place, recv_sem.at[pair % TURNS, sub])

    def departure(pair, sub):
        span = pl.ds(sub * half, rest if sub == PAIR - 1 else half)
        place = send_ref.at[pl.ds(0, groups - 1), pair % RING, span]
        return pltpu.make_async_copy(place, place, send_sem.at[pair % RING, sub])

    bits = [1 << n for n in range(groups.bit_length() - 1)]
    orders = [bits[1:], bits[:0:-1]]
    pieces_list = all_ref.shape[1]
    spans = [pl.ds(0, pieces_list // 2), pl.ds(pieces_list // 2, pieces_list - pieces_list // 2)]

    def stage(number):
        for which, order in enumerate(orders):
            if number < 0:
                yield which, 0, 0
                continue
            held = [0]
            for bit in order[:number]:
                held = held + [mask + bit for mask in held]
            for mask in held:
                yield which, order[number], mask

    def list_message(number, which, bit, mask):
        place = all_ref.at[partner(me, mask, groups), spans[which]]
        return pltpu.make_async_remote_copy(
            place,
            place,
            list_send.at[number],
            list_recv.at[number],
            device_id={"serve": partner(me, bit, groups)},
            device_id_type=MESH,
        )

    def lists_passed(number, sem):
        place = all_ref.at[pl.ds(0, 1 << number)]
        return pltpu.make_async_copy(place, place, sem.at[number])

    def edge(layer, side):
        to = part + 1 if side == 0 else part - 1
        return pltpu.make_async_remote_copy(
            edge_ref.at[layer, side],
            halo_ref.at[layer, side],
            halo_send.at[layer % 2, side],
            halo_recv.at[layer % 2, side],
            device_id={"train": to},
            device_id_type=MESH,
        )

    def length_message(turn, side):
        return pltpu.make_async_remote_copy(
            length_ref.at[turn],
            lengths_ref.at[turn, side],
            length_send.at[side],
            length_recv.at[turn, side],
            device_id={"train": part + 1 if side == 0 else part - 1},
            device_id_type=MESH,
        )

    lengths_ref[...] = jnp.zeros(lengths_ref.shape, jnp.float32)
    barrier = pltpu.get_barrier_semaphore()

    def greet(mask, carry):
        pl.semaphore_signal(barrier, inc=1, device_id={"serve": partner(me, mask, groups)}, device_id_type=MESH)
        return carry

    lax.fori_loop(1, groups, greet, 0)

    @pl.when(part > 0)
    def _():
        pl.semaphore_signal(barrier, inc=1, device_id={"train": part - 1}, device_id_type=MESH)

    @pl.when(part < parts_n - 1)
    def _():
        pl.semaphore_signal(barrier, inc=1, device_id={"train": part + 1}, device_id_type=MESH)

    get_group = pltpu.make_async_copy(group_hbm, group_ref, small_sem.at[0])
    get_group.start()
    fetch(0, 0).start()
    get_offset = pltpu.make_async_copy(offset_hbm, offset_ref, small_sem.at[1])
    get_offset.start()
    for sub in range(1, PAIR):
        fetch(sub, sub).start()

    below = (part + parts_n - 1) // parts_n
    above = (2 * parts_n - 2 - part) // parts_n

    row = lax.broadcasted_iota(jnp.int32, (BLOCK, columns), 0)
    lane = lax.broadcasted_iota(jnp.int32, (BLOCK, LANES), 1)
    last = rows_dev - BLOCK

    def transpose_tile(sub, low):
        high = min(low + LANES, buffer_len)
        rows_of = turned(in_ref[sub, :, low:high]).astype(w_ref.dtype)
        w_ref[low // BLOCK : high // BLOCK] = rows_of.reshape((high - low) // BLOCK, BLOCK, columns)

    def joined(group, count):
        tile = rem_ref[group, 0].astype(jnp.float32)
        for i in range(1, count):
            moved = pltpu.roll(rem_ref[group, i].astype(jnp.float32), i * rem, 1)
            tile = jnp.where(lane >= i * rem, moved, tile)
        return tile

    def edge_ends(layer, act):
        @pl.when(part < parts_n - 1)
        def _():
            act(edge(layer, 0))

        @pl.when(part > 0)
        def _():
            act(edge(layer, 1))

    def store_edges(layer, sub):
        fetch(layer, sub).wait()
        low = (buffer_len - 1) // LANES * LANES
        edge_ref[layer, 0] = turned(in_ref[sub, :, low:buffer_len])[-SHIFT:].astype(edge_ref.dtype)
        edge_ref[layer, 1] = turned(in_ref[sub, :, 0:LANES])[:SHIFT].astype(edge_ref.dtype)


    def send_edges(layer, sub):
        store_edges(layer, sub)

        @pl.when(layer >= 2)
        def _():
            edge_ends(layer - 2, lambda copy: copy.wait_send())

        edge_ends(layer, lambda copy: copy.start())

    def turn_layer(pair, sub):
        layer = pair * PAIR + sub
        for low in range(0, buffer_len, LANES):
            transpose_tile(sub, low)

        @pl.when(layer + PAIR < layers)
        def _():
            fetch(layer + PAIR, sub).start()

        w_ref[0] = jnp.zeros((BLOCK, columns), w_ref.dtype)

    def finish_layer(pair, sub):
        layer = pair * PAIR + sub
        base_row = part * rows_dev

        @pl.when(part > 0)
        def _():
            edge(layer, 0).wait_recv()
            first = offset_ref[part, layer] - base_row
            head = jnp.where(row < first, halo_ref[layer, 0].astype(jnp.float32), w_ref[1].astype(jnp.float32))
            w_ref[1] = head.astype(w_ref.dtype)

        @pl.when(part < parts_n - 1)
        def _():
            edge(layer, 1).wait_recv()
            after = offset_ref[part + 1, layer] - base_row
            tail = w_ref[blocks - 2].astype(jnp.float32)
            tail = jnp.where(row + last >= after, halo_ref[layer, 1].astype(jnp.float32), tail)
            w_ref[blocks - 2] = tail.astype(w_ref.dtype)

        def last_slots(group, carry):
            over_ref[layer * groups + group] = w_ref[table_smem[layer, group * layers + base]]
            return carry

        lax.fori_loop(0, groups, last_slots, 0)

    def prepare(pair, sub):
        turn_layer(pair, sub)
        finish_layer(pair, sub)

    def gather(pair, sub, group, out, slots_of=None):
        for k in range(*(slots_of or (0, base))):
            block = w_ref[table_smem[pair * PAIR + sub, group * layers + k]]
            for t in range(full):
                out[(sub * base + k) * full + t] = block[:, t * LANES : (t + 1) * LANES]
            if rem:
                rem_ref[group, sub * base + k, :, 0:rem] = block[:, full * LANES :]
        if rem and sub == PAIR - 1:
            out[PAIR * half] = joined(group, PAIR * base).astype(out.dtype)

    def give(low, high, pair, sub, pack, send, final, slots_of=None):
        def one(mask, carry):
            peer = partner(me, mask, groups)
            if pack:
                gather(pair, sub, peer, send_ref.at[peer, pair % RING], slots_of)
            if send:
                message(mask, pair, sub, final, slots_of).start()
            return carry

        lax.fori_loop(low, high, one, 0)

    def own(pair, sub, final):
        gather(pair, sub, me, landing(me, pair, sub, final))

    def pack_list(entry_of, out):
        for e in range(listed):
            block = over_ref[entry_of(e)]
            for t in range(full):
                out[e * full + t] = block[:, t * LANES : (t + 1) * LANES]
            if rem:
                rem_ref[groups, e, :, 0:rem] = block[:, full * LANES :]
        if rem:
            out[listed * full] = joined(groups, listed).astype(out.dtype)

    def take(pair, final):
        for sub in range(PAIR):
            arrival(pair, sub, final).wait()

    def unpack(pair):
        def recv(s, n):
            return recv_ref[s, pair, n]

        scale_rest(dims, PAIR * base, recv, rem_code, rem_scale)

        def slot(i, carry):
            def put_code(low, high, code):
                codes_ref[pair * PAIR + i // base, i % base, :, low:high] = code.astype(codes_ref.dtype)

            def put_scale(low, high, scale):
                rows[i, :, low:high] = scale

            place = i
            if ahead:
                place = table_smem[layers + 2, me * layers + jnp.minimum(i, base - 1)]
                place = jnp.where((pair == 0) & (i < base), place, i)
            scale_slot(dims, i, recv, rem_code, rem_scale, put_code, put_scale, place)
            return carry

        lax.fori_loop(0, PAIR * base, slot, 0)
        for i in range(PAIR * base):
            scale_ref[pair * PAIR + i // base, i % base : i % base + 1, :] = rows[i]

    def sent(pair):
        for sub in range(PAIR):
            departure(pair, sub).wait()

    def step(pair, carry):
        @pl.when(pair >= RING)
        def _():
            sent(pair - RING)

        for sub in range(PAIR):
            prepare(pair, sub)
            give(2, groups, pair, sub, True, True, False)
            give(1, 2, pair, sub, True, True, False)
            own(pair, sub, False)
            send_edges(pair * PAIR + sub + 1, (sub + 1) % PAIR)

        take(pair - 1, False)
        if ahead:

            @pl.when(pair == 1)
            def _():
                def restore(source, inner):
                    for k in range(base):
                        place = table_smem[layers + 2, me * layers + k]
                        for t in range(full):
                            recv_ref[source, 0, k * full + t] = turned_ref[source, place * full + t]
                    return inner

                lax.fori_loop(0, groups, restore, 0)

        unpack(pair - 1)
        return carry

    get_group.wait()
    spot = lax.broadcasted_iota(jnp.int32, (layers, groups * layers), 1)
    spot_group = jnp.zeros(spot.shape, jnp.int32)
    for g in range(1, groups):
        spot_group = spot_group + jnp.where(spot >= g * layers, 1, 0)
    spot_slot = spot - spot_group * layers
    seen = jnp.zeros(spot.shape, jnp.int32)
    table = jnp.zeros(spot.shape, jnp.int32)
    moved = jnp.zeros((1, groups * layers), jnp.int32)
    for j in range(group_ref.shape[1]):
        mine = group_ref[:, j : j + 1] == spot_group
        table = jnp.where(mine & (seen == spot_slot), j + 1, table)
        moved = jnp.where(mine[0:1, :] & (seen[0:1, :] + 1 == spot_slot[0:1, :]), j + 1, moved)
        seen = jnp.where(mine, seen + 1, seen)
    table_ref[0:layers, :] = table
    if ahead:
        count, k = seen[0:1, :], spot_slot[0:1, :]
        final_block = group_ref.shape[1]
        turns = (group_ref[0:1, final_block - 1 : final_block] == spot_group[0:1, :]) & (count <= base)
        turned_row = jnp.where(k == 0, final_block, jnp.where(k < count, moved, 0))
        table_ref[0:1, :] = jnp.where(turns, turned_row, table[0:1, :])
        position = jnp.where(k == count - 1, 0, jnp.where(k < count, k + 1, k))
        table_ref[layers + 2 : layers + 3, :] = jnp.where(turns, position, k)
    none = layers * groups
    length = jnp.zeros((1, groups * layers), jnp.int32)
    entry = jnp.full(length.shape, none, jnp.int32)
    total = jnp.zeros((1, LANES), jnp.int32)
    shared = jnp.full(total.shape, none, jnp.int32)
    number = lax.broadcasted_iota(jnp.int32, total.shape, 1)
    long = jnp.where(seen == slots, 1, 0)
    for n in range(layers):
        here = long[n : n + 1, :]
        entry = jnp.where((here > 0) & (length == spot_slot[0:1, :]), n * groups + spot_group[0:1, :], entry)
        length = length + here
        for g in range(groups):
            one = jnp.broadcast_to(here[:, g * layers : g * layers + 1], total.shape)
            shared = jnp.where((one > 0) & (total == number), n * groups + g, shared)
            total = total + one
    table_ref[layers : layers + 1, :] = entry
    table_ref[layers + 1 : layers + 2, 0:LANES] = shared
    to_smem = pltpu.make_async_copy(table_ref, table_smem, table_sem)
    to_smem.start()
    most = jnp.broadcast_to(total.astype(jnp.float32), length_ref.shape[1:])
    over_ref[none] = jnp.zeros((BLOCK, columns), over_ref.dtype)

    end = pairs - 1
    store_edges(0, 0)
    turn_layer(0, 0)
    to_smem.wait()
    pl.semaphore_wait(barrier, groups - 1 + below + above)
    edge_ends(0, lambda copy: copy.start())
    get_offset.wait()
    for sub in range(PAIR):
        if sub > 0:
            turn_layer(0, sub)
        if sub == 0 and ahead:
            give(2, groups, 0, sub, True, True, False, (2, base))
            finish_layer(0, sub)
            give(2, groups, 0, sub, True, True, False, (0, 2))
            give(1, 2, 0, sub, True, True, False)
        else:
            finish_layer(0, sub)
            give(2, groups, 0, sub, True, True, False)
            give(1, 2, 0, sub, True, True, False)
        own(0, sub, False)
        send_edges(sub + 1, (sub + 1) % PAIR)
    lax.fori_loop(1, end, step, 0)

    if end >= RING:
        sent(end - RING)
    for sub in range(PAIR):
        prepare(end, sub)
        give(1, groups, end, sub, True, False, True)
        own(end, sub, True)
        if sub < PAIR - 1:
            send_edges(end * PAIR + sub + 1, sub + 1)
    pack_list(lambda e: table_smem[layers + 1, e], all_ref.at[me])
    high = len(bits) - 1
    for copy in stage(0):
        list_message(0, *copy).start()
    for which in range(2):
        list_message(high, which, 1, 0).start()
    for sub in range(PAIR - 1):
        give(2, groups, end, sub, False, True, True)
        give(1, 2, end, sub, False, True, True)

    def second(group, carry):
        for which in range(2):
            pack_list(lambda e: table_smem[layers, group * layers + which * listed + e], list_ref.at[group, which])
        return carry

    lax.fori_loop(0, groups, second, 0)
    keep = pltpu.make_async_copy(list_ref, second_ref, second_sem.at[0])
    keep.start()
    for n in range(2):
        edge_ends(layers - 1 - n, lambda copy: copy.wait_send())

    def to_neighbours(turn, act):
        @pl.when(part < parts_n - 1)
        def _():
            act(length_message(turn, 0))

        @pl.when(part > 0)
        def _():
            act(length_message(turn, 1))

    def from_neighbours(turn):
        @pl.when(part > 0)
        def _():
            length_message(turn, 0).wait_recv()

        @pl.when(part < parts_n - 1)
        def _():
            length_message(turn, 1).wait_recv()

    for turn in range(parts_n - 1):
        length_ref[turn] = most
        to_neighbours(turn, lambda copy: copy.start())
        from_neighbours(turn)
        for side in range(2):
            most = jnp.maximum(most, lengths_ref[turn, side])
        to_neighbours(turn, lambda copy: copy.wait_send())
    longest_smem[0, 0] = jnp.max(most).astype(jnp.int32)
    tell = pltpu.make_async_copy(longest_smem, longest_ref, second_sem.at[1])
    tell.start()

    take(end - 1, False)
    unpack(end - 1)
    for number in range(1, high + 1):
        lists_passed(number - 1, list_recv).wait()
        if number < high:
            for copy in stage(number):
                list_message(number, *copy).start()
        for which, bit, mask in stage(number - 1):
            list_message(high, which, 1, bit + mask).start()
        if number == 1:
            give(groups * 3 // 4, groups, end, PAIR - 1, False, True, True)
            give(1, groups * 3 // 4, end, PAIR - 1, False, True, True)
    lists_passed(high, list_recv).wait()

    def recv(s, n):
        return all_ref[s, n]

    scale_rest(dims, listed, recv, rem_code, rem_scale)

    def listed_slot(e, carry):
        def put_code(low, high, code):
            shared_codes[e, :, low:high] = code.astype(shared_codes.dtype)

        def put_scale(low, high, scale):
            shared_scale[e, :, low:high] = scale

        scale_slot(dims, e, recv, rem_code, rem_scale, put_code, put_scale)
        return carry

    lax.fori_loop(0, listed, listed_slot, 0)
    shared_codes[listed] = jnp.zeros(shared_codes.shape[1:], shared_codes.dtype)
    shared_scale[listed] = jnp.zeros(shared_scale.shape[1:], jnp.float32)

    keep.wait()
    tell.wait()
    for number in range(high + 1):
        lists_passed(number, list_send).wait()
    for pair in range(max(0, end - RING + 1), end + 1):
        sent(pair)
    take(end, True)


def list_places(group_ref, place_ref, slots, groups, shared):
    layers = group_ref.shape[0]
    me = lax.axis_index("serve")
    count = jnp.sum(jnp.where(group_ref[...] == me, 1, 0), axis=1, keepdims=True)
    ahead = jnp.zeros((layers, 1), jnp.int32)
    every = jnp.where(count == slots, 1, 0)
    if shared:
        every = jnp.zeros((layers, 1), jnp.int32)
        for g in range(groups):
            filled = jnp.sum(jnp.where(group_ref[...] == g, 1, 0), axis=1, keepdims=True)
            one = jnp.where(filled == slots, 1, 0)
            ahead = ahead + jnp.where(g < me, one, 0)
            every = every + one
    length = jnp.zeros((1, 1), jnp.int32)
    for n in range(layers):
        place = jnp.where(count[n : n + 1, :] == slots, length + ahead[n : n + 1, :], layers * groups)
        place_ref[n : n + 1, :] = jnp.broadcast_to(place, (1, place_ref.shape[1]))
        length = length + every[n : n + 1, :]
    return count


def write_kernel(
    dims,
    base,
    group_ref,
    codes_ref,
    scale_ref,
    tail_ref,
    shared_codes,
    shared_scale,
    codes_out,
    scale_out,
    scales,
    codes,
    rows,
    rem_code,
    rem_scale,
    place_ref,
    place_smem,
    sems,
    last_sems,
    place_sem,
):
    groups = dims[3]
    layers = scale_out.shape[0]
    done = layers - PAIR
    listed = layers // 2
    copies = [pltpu.make_async_copy(codes_ref.at[n], codes_out.at[n, pl.ds(0, base)], sems.at[n]) for n in range(done)]
    for copy in copies:
        copy.start()
    count = list_places(group_ref, place_ref, base + 1, groups, True)
    to_smem = pltpu.make_async_copy(place_ref, place_smem, place_sem)
    to_smem.start()

    def recv(s, n):
        return tail_ref[s, n]

    scale_rest(dims, PAIR * base, recv, rem_code, rem_scale)

    def last_pair(sub):
        def slot(k, carry):
            def put_code(low, high, code):
                codes[sub, k, :, low:high] = code.astype(codes.dtype)

            def put_scale(low, high, scale):
                rows[sub * base + k, :, low:high] = scale

            scale_slot(dims, sub * base + k, recv, rem_code, rem_scale, put_code, put_scale)
            return carry

        lax.fori_loop(0, base, slot, 0)
        copies.append(pltpu.make_async_copy(codes.at[sub], codes_out.at[done + sub, pl.ds(0, base)], sems.at[done + sub]))
        copies[-1].start()

    last_pair(0)
    to_smem.wait()
    places = [jnp.minimum(place_smem[n, 0], listed) for n in range(layers)]
    for n in range(layers):
        copies.append(pltpu.make_async_copy(shared_codes.at[places[n]], codes_out.at[n, base], last_sems.at[n]))
        copies[-1].start()
    for sub in range(1, PAIR):
        last_pair(sub)
    slot = lax.broadcasted_iota(jnp.int32, scales.shape[1:], 0)
    for sub in range(PAIR):
        for k in range(base):
            scales[done + sub, k : k + 1, :] = rows[sub * base + k]
    for n in range(layers):
        scale = scale_ref[n] if n < done else scales[n]
        scale = jnp.where(slot < count[n : n + 1, :], scale, 0.0)
        scales[n] = jnp.where(slot < base, scale, jnp.broadcast_to(shared_scale[places[n]], scale.shape))
    copies.append(pltpu.make_async_copy(scales, scale_out, sems.at[layers]))
    copies[-1].start()
    for copy in copies:
        copy.wait()


def late_kernel(
    dims,
    base,
    group_ref,
    got_ref,
    codes_in,
    scale_in,
    codes_out,
    scale_out,
    extra,
    extra_scale,
    scales,
    rem_code,
    rem_scale,
    place_ref,
    place_smem,
    sem,
):
    del codes_in, scale_in
    full, rem, columns, groups = dims
    layers = codes_out.shape[0]
    listed = layers // 2
    list_places(group_ref, place_ref, base + 1, groups, False)
    to_smem = pltpu.make_async_copy(place_ref, place_smem, sem)
    to_smem.start()
    to_smem.wait()
    slot = lax.broadcasted_iota(jnp.int32, scales.shape, 0)
    for which in range(2):

        def recv(s, n, which=which):
            return got_ref[s, which, n]

        scale_rest(dims, listed, recv, rem_code, rem_scale)

        def last_slot(layer, carry, which=which, recv=recv):
            place = place_smem[layer, 0] - which * listed

            @pl.when((place >= 0) & (place < listed))
            def _():
                def put_code(low, high, code):
                    extra[:, low:high] = code.astype(extra.dtype)

                def put_scale(low, high, scale):
                    extra_scale[:, low:high] = scale

                scale_slot(dims, place, recv, rem_code, rem_scale, put_code, put_scale)
                pltpu.sync_copy(extra, codes_out.at[layer, base])
                pltpu.sync_copy(scale_out.at[layer], scales)
                scales[...] = jnp.where(slot < base, scales[...], jnp.broadcast_to(extra_scale[...], scales.shape))
                pltpu.sync_copy(scales, scale_out.at[layer])

            return carry

        lax.fori_loop(0, layers, last_slot, 0)


def shards(train_weights, row_offset, block_group):
    train_n = lax.axis_size("train")
    serve_n = lax.axis_size("serve")
    layers, buffer_len, columns = train_weights.shape
    blocks_dev = block_group.shape[1]
    base = (blocks_dev + serve_n - 1) // serve_n
    slots = base + 1
    full = columns // LANES
    rem = columns - full * LANES
    pairs = layers // PAIR
    listed = layers // 2
    pieces = PAIR * base * full + (1 if rem else 0)
    pieces_list = listed * full + (1 if rem else 0)
    rests = max(PAIR * base, listed)
    spots = serve_n * layers
    width = columns * serve_n
    dtype = train_weights.dtype
    dims = (full, rem, columns, serve_n)
    assert SHIFT == BLOCK and buffer_len % BLOCK == 0
    assert rests * rem <= LANES and layers % PAIR == 0 and slots <= layers and pairs > 2

    group_ids = block_group[:, :, 0]
    smem = pl.BlockSpec(memory_space=pltpu.SMEM)
    vmem = pl.BlockSpec(memory_space=pltpu.VMEM)
    anywhere = pl.BlockSpec(memory_space=pl.ANY)
    hbm = pl.BlockSpec(memory_space=pltpu.HBM)
    codes, scales, tail, shared_codes, shared_scale, second, longest = pl.pallas_call(
        functools.partial(move_kernel, dims, base),
        in_specs=[hbm, hbm, hbm],
        out_specs=[vmem, vmem, vmem, vmem, vmem, hbm, hbm],
        out_shape=[
            pltpu.VMEM((layers - PAIR, base, BLOCK, width), dtype),
            pltpu.VMEM((layers - PAIR, slots, width), jnp.float32),
            pltpu.VMEM((serve_n, pieces, BLOCK, LANES), dtype),
            pltpu.VMEM((listed + 1, BLOCK, width), dtype),
            pltpu.VMEM((listed + 1, 1, width), jnp.float32),
            jax.ShapeDtypeStruct((serve_n, 2, pieces_list, BLOCK, LANES), dtype),
            jax.ShapeDtypeStruct((1, 1), jnp.int32),
        ],
        scratch_shapes=[
            pltpu.VMEM((serve_n, pieces_list, BLOCK, LANES), dtype),
            pltpu.VMEM((serve_n, base * full, BLOCK, LANES), dtype),
            pltpu.VMEM((serve_n, pairs - 1, pieces, BLOCK, LANES), dtype),
            pltpu.VMEM((serve_n, RING, pieces, BLOCK, LANES), dtype),
            pltpu.VMEM((PAIR, columns, buffer_len), dtype),
            pltpu.VMEM((buffer_len // BLOCK, BLOCK, columns), dtype),
            pltpu.VMEM((serve_n + 1, rests, BLOCK, LANES), dtype),
            pltpu.VMEM((layers, 2, SHIFT, columns), dtype),
            pltpu.VMEM((layers, 2, SHIFT, columns), dtype),
            pltpu.VMEM((serve_n * layers + 1, BLOCK, columns), dtype),
            pltpu.VMEM((serve_n, 2, pieces_list, BLOCK, LANES), dtype),
            pltpu.VMEM((serve_n, BLOCK, LANES), jnp.float32),
            pltpu.VMEM((serve_n, 1, LANES), jnp.float32),
            pltpu.VMEM((PAIR * base, 1, width), jnp.float32),
            pltpu.VMEM((layers + 8, spots), jnp.int32),
            pltpu.SMEM((layers + 8, spots), jnp.int32),
            pltpu.VMEM((train_n, 8, LANES), jnp.float32),
            pltpu.VMEM((train_n, 2, 8, LANES), jnp.float32),
            pltpu.SMEM((1, 1), jnp.int32),
            pltpu.SMEM((train_n + 1, layers), jnp.int32),
            pltpu.VMEM((layers, blocks_dev), jnp.int32),
            pltpu.SemaphoreType.DMA((PAIR,)),
            pltpu.SemaphoreType.DMA,
            pltpu.SemaphoreType.DMA((2,)),
            pltpu.SemaphoreType.DMA((RING, PAIR)),
            pltpu.SemaphoreType.DMA((TURNS, PAIR)),
            pltpu.SemaphoreType.DMA((2, 2)),
            pltpu.SemaphoreType.DMA((2, 2)),
            pltpu.SemaphoreType.DMA((serve_n.bit_length() - 1,)),
            pltpu.SemaphoreType.DMA((serve_n.bit_length() - 1,)),
            pltpu.SemaphoreType.DMA((2,)),
            pltpu.SemaphoreType.DMA((train_n, 2)),
            pltpu.SemaphoreType.DMA((2,)),
        ],
        compiler_params=pltpu.CompilerParams(
            collective_id=0, has_side_effects=True, vmem_limit_bytes=36 * MIB
        ),
        name="move",
    )(pltpu.with_memory_space_constraint(row_offset.T, pltpu.HBM), group_ids, jnp.swapaxes(train_weights, 1, 2))

    codes_shape = jax.ShapeDtypeStruct((layers, slots, BLOCK, width), dtype)
    scales_shape = jax.ShapeDtypeStruct((layers, slots, width), jnp.float32)
    rest_scratch = [
        pltpu.VMEM((serve_n, BLOCK, LANES), jnp.float32),
        pltpu.VMEM((serve_n, 1, LANES), jnp.float32),
        pltpu.VMEM((layers, LANES), jnp.int32),
        pltpu.SMEM((layers, LANES), jnp.int32),
    ]
    codes_out, scales_out = pl.pallas_call(
        functools.partial(write_kernel, dims, base),
        in_specs=[vmem, anywhere, vmem, vmem, vmem, vmem],
        out_specs=[hbm, hbm],
        out_shape=[codes_shape, pltpu.HBM((layers, slots, width), jnp.float32)],
        scratch_shapes=[
            pltpu.VMEM((layers, slots, width), jnp.float32),
            pltpu.VMEM((PAIR, base, BLOCK, width), dtype),
            pltpu.VMEM((PAIR * base, 1, width), jnp.float32),
            *rest_scratch,
            pltpu.SemaphoreType.DMA((layers + 1,)),
            pltpu.SemaphoreType.DMA((layers,)),
            pltpu.SemaphoreType.DMA,
        ],
        compiler_params=pltpu.CompilerParams(vmem_limit_bytes=10 * MIB),
        name="write",
    )(group_ids, codes, scales, tail, shared_codes, shared_scale)

    def late(state):
        got = lax.all_to_all(second, "serve", split_axis=0, concat_axis=0, tiled=True)
        late_codes, late_scales = pl.pallas_call(
            functools.partial(late_kernel, dims, base),
            in_specs=[vmem, vmem, hbm, hbm],
            out_specs=[hbm, hbm],
            out_shape=[codes_shape, scales_shape],
            input_output_aliases={2: 0, 3: 1},
            scratch_shapes=[
                pltpu.VMEM((BLOCK, width), dtype),
                pltpu.VMEM((1, width), jnp.float32),
                pltpu.VMEM((slots, width), jnp.float32),
                *rest_scratch,
                pltpu.SemaphoreType.DMA,
            ],
            compiler_params=pltpu.CompilerParams(vmem_limit_bytes=6 * MIB),
            name="late",
        )(group_ids, got, state[1], state[2])
        return jnp.zeros((), jnp.int32), late_codes, late_scales

    codes_out, scales_out = lax.cond(
        longest[0, 0] > listed, lambda c, z: late((0, c, z))[1:], lambda c, z: (c, z), codes_out, scales_out
    )
    return (
        codes_out.reshape(layers, 1, 1, slots, BLOCK, width),
        scales_out.reshape(layers, 1, 1, slots, width),
    )


def solution(mesh):
    return jax.shard_map(
        shards,
        mesh=mesh,
        in_specs=(P(None, "train", "serve"), P(), P(None, "train", None)),
        out_specs=(
            P(None, "serve", "train", None, None, None),
            P(None, "serve", "train", None, None),
        ),
        check_vma=False,
    )
```
